32 devices in a mesh: dp: 4 (over y, x), bins: 8 (over z, core).
Axes of the slice: x: 2, y: 2, z: 4, core: 2. Of those that a mesh axis runs over, the one named last changes fastest.
Arguments:
- activations: bfloat16 [64, 1024, 768], P('dp', 'bins'), may hold values from -16 to 16
- shift_bins: int32 [64], P('dp'), may hold values from -3 to 3, as said below
- reverse_flags: int32 [64], P('dp'), may hold values from 0 to 1
- gain_one: bfloat16 [768], P('bins'), may hold values from 0.5 to 1.5
- bias_one: bfloat16 [768], P('bins'), may hold values from -3 to 3
- conv_weight: bfloat16 [3, 768, 384], P(None, 'bins'), may hold values from -0.125 to 0.125
- gain_two: bfloat16 [384], P('bins'), may hold values from 0.5 to 1.5
- bias_two: bfloat16 [384], P('bins'), may hold values from -3 to 3
- proj_weight: bfloat16 [384, 768], P(None, 'bins'), may hold values from -0.3125 to 0.3125
- proj_bias: bfloat16 [768], P('bins'), may hold values from -2 to 2
- cotangent: bfloat16 [64, 1024, 768], P('dp', 'bins'), may hold values from -6 to 6
Outputs:
- output: bfloat16 [64, 1024, 768], P('dp', 'bins')
- grad_activations: bfloat16 [64, 1024, 768], P('dp', 'bins')
- grad_gain_one: float32 [768], P(('dp', 'bins'))
- grad_bias_one: float32 [768], P(('dp', 'bins'))
- grad_conv_weight: float32 [3, 768, 384], P(None, ('dp', 'bins'))
- grad_gain_two: float32 [384], P('bins')
- grad_bias_two: float32 [384], P('bins')
- grad_proj_weight: float32 [384, 768], P(None, ('dp', 'bins'))
- grad_proj_bias: float32 [768], P(('dp', 'bins'))
The draws below stay inside these ranges and needn't reach their ends.
Inputs may be any that keep to these rules, and one draw needn't show every extreme that they name: `shift_bins`: both 3 and -3 occur in every draw.
All inputs are finite; a program needn't handle non-finite values.
Results may differ from the reference program's by a relative error of at most 0.0067.
Values may be sent and summed in bfloat16 or wider, within the bound.
A program may use at most 128 MiB of HBM per device.

```python
import jax
import jax.numpy as jnp
from jax import lax

C = 768
F = 384
KERNEL_TAPS = 3
DILATION_BINS = 8
SHIFT = 3
MICRO = 4
MB_DEV = 4
SEQS = 64
SEQUENCE_BINS = 1024
N_DP = 4


def draw_activations(key, part):
    subkeys = jax.random.split(key, 4)
    normal_part = jax.random.normal(subkeys[0], (SEQS, SEQUENCE_BINS, C), jnp.float32)
    row_scale = jnp.exp(jax.random.uniform(subkeys[1], (SEQS, SEQUENCE_BINS, 1), jnp.float32, -1.15, 1.15))
    chan_scale = jnp.exp(jax.random.uniform(subkeys[2], (1, 1, C), jnp.float32, -1.15, 1.15))
    chan_mean = 0.5 * jax.random.normal(subkeys[3], (1, 1, C), jnp.float32)
    position = jnp.arange(SEQUENCE_BINS, dtype=jnp.float32) / SEQUENCE_BINS
    sequence_pos = jnp.arange(SEQS, dtype=jnp.float32) / SEQS
    rising = jnp.exp(1.1 * position)[None, :, None] * jnp.exp(0.5 * sequence_pos)[:, None, None]
    values = normal_part * row_scale * chan_scale * rising * 0.5 + chan_mean
    return jnp.clip(values, -16.0, 16.0).astype(jnp.bfloat16)


def draw_shift_bins(key, part):
    subkeys = jax.random.split(key, 3)
    values = jax.random.randint(subkeys[0], (SEQS,), -SHIFT, SHIFT + 1, dtype=jnp.int32)
    first_pick = jax.random.randint(subkeys[1], (), 0, SEQS, dtype=jnp.int32)
    second_pick = (first_pick + jax.random.randint(subkeys[2], (), 1, SEQS, dtype=jnp.int32)) % SEQS
    values = values.at[first_pick].set(SHIFT)
    return values.at[second_pick].set(-SHIFT)


def touch_ends(array, stream_key, least, top_value):
    longest = array.shape.index(max(array.shape))
    spots = []
    for shift in (0, 1):
        where = [jax.random.randint(jax.random.fold_in(stream_key, axis), (), 0, length) for axis, length in enumerate(array.shape)]
        where[longest] = (where[longest] + shift) % array.shape[longest]
        spots.append(tuple(where))
    return array.at[spots[0]].set(least).at[spots[1]].set(top_value)


def block_levels(own_key, shape, pieces, low, high):
    level = 1.0
    for axis_at, shards_of in pieces:
        draws = jax.random.uniform(jax.random.fold_in(jax.random.fold_in(own_key, 6), axis_at), (shards_of,), jnp.float32, low / len(pieces), high / len(pieces))
        level = level * jnp.repeat(jnp.exp(draws), shape[axis_at] // shards_of).reshape((-1,) + (1,) * (len(shape) - 1 - axis_at))
    return level


def normal_values(key, extent, scale, bound, pieces=(), kind=jnp.bfloat16):
    entries = jax.random.normal(key, extent, jnp.float32) * scale
    if len(pieces) > 0:
        entries = block_levels(key, extent, pieces, -0.22, 0.18) * entries
    return jnp.clip(entries, min=-bound, max=bound).astype(kind)


def setup_inputs(seed: int = 0) -> dict:
    seeds = jax.random.split(jax.random.key(seed), 12)
    return {
        "activations": draw_activations(jax.random.fold_in(seeds[11], 71), 0),
        "shift_bins": draw_shift_bins(jax.random.fold_in(seeds[11], 71), 0),
        "reverse_flags": touch_ends(jax.random.randint(seeds[2], (SEQS,), 0, 2), jax.random.fold_in(seeds[2], 1), 0, 1).astype(jnp.int32),
        "gain_one": jnp.clip(1.0 + 0.1 * jax.random.normal(seeds[3], (C,), jnp.float32), 0.5, 1.5).astype(jnp.bfloat16),
        "bias_one": normal_values(seeds[4], (C,), 0.5, 3.0, ((0, 8),)),
        "conv_weight": normal_values(seeds[5], (KERNEL_TAPS, C, F), (KERNEL_TAPS * C) ** -0.5, 0.125, ((1, 8),)),
        "gain_two": jnp.clip(1.0 + 0.1 * jax.random.normal(seeds[6], (F,), jnp.float32), 0.5, 1.5).astype(jnp.bfloat16),
        "bias_two": normal_values(seeds[7], (F,), 0.5, 3.0, ((0, 8),)),
        "proj_weight": normal_values(seeds[8], (F, C), F ** -0.5, 0.3125, ((1, 8),)),
        "proj_bias": normal_values(seeds[9], (C,), 0.3, 2.0, ((0, 8),)),
        "cotangent": normal_values(seeds[10], (SEQS, SEQUENCE_BINS, C), 1.0, 6.0, ((0, 4), (1, 8))),
    }


EPSILON = 1e-05

@jax.custom_vjp
def low(v):
    return lax.optimization_barrier(v.astype(jnp.bfloat16)).astype(jnp.float32)

@jax.custom_vjp
def low_back(v):
    return v

def low_keep(v):
    return (low(v), None)

def low_pass(kept, grad):
    return (grad,)

def back_keep(v):
    return (v, None)

def back_low(kept, grad):
    return (low(grad),)
low.defvjp(low_keep, low_pass)
low_back.defvjp(back_keep, back_low)

def move_rows(inputs, shift_bins, reverse_flags):
    position = jnp.arange(SEQUENCE_BINS, dtype=jnp.int32)[None, :]
    plain_source = position - shift_bins[:, None]
    mirror_source = SEQUENCE_BINS - 1 - position - shift_bins[:, None]
    source = jnp.where(reverse_flags[:, None] > 0, mirror_source, plain_source)
    inside = (source >= 0) & (source < SEQUENCE_BINS)
    clamped = jnp.clip(source, 0, SEQUENCE_BINS - 1).astype(jnp.int32)
    picked = jnp.take_along_axis(inputs, clamped[:, :, None], axis=1)
    return jnp.where(inside[:, :, None], picked, 0.0)

def norm_apply(values, gain, bias):
    mean_all = lax.optimization_barrier(jnp.mean(values, axis=(0, 1)))
    variance = lax.optimization_barrier(jnp.mean(values * values, axis=(0, 1))) - mean_all * mean_all
    return (values - mean_all) * lax.rsqrt(variance + EPSILON) * gain + bias

def block_forward(inputs, gain_one, bias_one, conv_weight, gain_two, bias_two, proj_weight, proj_bias, shift_bins, reverse_flags):
    moved = move_rows(inputs, shift_bins, reverse_flags)
    grouped = moved.reshape(N_DP, MICRO, MB_DEV, SEQUENCE_BINS, C).transpose(1, 0, 2, 3, 4)
    results = []
    for micro_index in range(MICRO):
        rows_in = grouped[micro_index].reshape(N_DP * MB_DEV, SEQUENCE_BINS, C)
        first_hidden = low(jax.nn.gelu(norm_apply(rows_in, gain_one, bias_one), approximate=True))
        padded_sequence = jnp.pad(first_hidden, ((0, 0), (DILATION_BINS, DILATION_BINS), (0, 0)))
        conv_out = jnp.zeros((N_DP * MB_DEV, SEQUENCE_BINS, F), jnp.float32)
        for kernel_tap_index in range(KERNEL_TAPS):
            sliding_window = padded_sequence[:, kernel_tap_index * DILATION_BINS:kernel_tap_index * DILATION_BINS + SEQUENCE_BINS]
            conv_out = conv_out + jnp.einsum('nlc,cf->nlf', sliding_window, conv_weight[kernel_tap_index], precision=lax.Precision.HIGHEST)
        conv_out = low_back(conv_out)
        hidden_two = low(jax.nn.gelu(norm_apply(conv_out, gain_two, bias_two), approximate=True))
        branch = jnp.einsum('nlf,fc->nlc', hidden_two, proj_weight, precision=lax.Precision.HIGHEST) + proj_bias
        results.append((rows_in + branch).reshape(N_DP, MB_DEV, SEQUENCE_BINS, C))
    stacked = jnp.stack(results, axis=1)
    return stacked.reshape(N_DP * MICRO * MB_DEV, SEQUENCE_BINS, C)

def reference(activations, shift_bins, reverse_flags, gain_one, bias_one, conv_weight, gain_two, bias_two, proj_weight, proj_bias, cotangent):
    floats = tuple((item.astype(jnp.float32) for item in (activations, gain_one, bias_one, conv_weight, gain_two, bias_two, proj_weight, proj_bias)))

    def forward(inputs, gain_a, bias_a, conv_w, gain_b, bias_b, proj_w, proj_b):
        return block_forward(inputs, gain_a, bias_a, conv_w, gain_b, bias_b, proj_w, proj_b, shift_bins, reverse_flags)
    result, pullback = jax.vjp(forward, *floats)
    gradients = pullback(cotangent.astype(jnp.float32))
    return (result.astype(jnp.bfloat16), gradients[0].astype(jnp.bfloat16), gradients[1], gradients[2], gradients[3], gradients[4], gradients[5], gradients[6], gradients[7])
```

```python
import functools

import jax
import jax.numpy as jnp
from jax import lax
from jax.experimental import pallas as pl
from jax.experimental.pallas import tpu as pltpu
from jax.sharding import PartitionSpec as P

TAPS = 3
DILATION = 8
MICRO = 4
EPSILON = 1e-05
CHUNK = 32
BASE_SLOTS = 8
FIRST_SLOTS = 2
WINDOW = 2
EDGE = 16
VMEM_LIMIT = 60 * 1024 * 1024
MESH = pl.DeviceIdType.MESH
F32 = jnp.float32
BF16 = jnp.bfloat16
ROOT = 0.7978845608028654
CUBE = 0.044715


def vmem():
    return pl.BlockSpec(memory_space=pltpu.VMEM)


def smem():
    return pl.BlockSpec(memory_space=pltpu.SMEM)


def anywhere():
    return pl.BlockSpec(memory_space=pl.ANY)


def matmul(a, b, ca, cb):
    return lax.dot_general(a, b, (((ca,), (cb,)), ((), ())), preferred_element_type=F32)


class Place:
    def __init__(self, dp_count, bin_count):
        self.dp_count, self.bin_count = dp_count, bin_count
        self.chip_count = bin_count // 2
        self.dp = lax.axis_index("dp")
        self.bin = lax.axis_index("bins")
        self.chip = self.bin // 2
        self.core = lax.rem(self.bin, 2)

    def barrier(self):
        semaphore = pltpu.get_barrier_semaphore()
        for apart in range(1, self.bin_count):
            other = (self.dp, lax.rem(self.bin + apart, self.bin_count))
            pl.semaphore_signal(semaphore, inc=1, device_id=other, device_id_type=MESH)
        for apart in range(1, self.dp_count):
            for core in range(2):
                other = (lax.rem(self.dp + apart, self.dp_count), self.chip * 2 + core)
                pl.semaphore_signal(semaphore, inc=1, device_id=other, device_id_type=MESH)
        pl.semaphore_wait(semaphore, self.bin_count - 1 + 2 * (self.dp_count - 1))


def remote(source, target, sent, landed, device):
    return pltpu.make_async_remote_copy(
        src_ref=source,
        dst_ref=target,
        send_sem=sent,
        recv_sem=landed,
        device_id=device,
        device_id_type=MESH,
    )


class Stream:
    def __init__(self, place, source, target, sent, landed, count):
        self.source, self.target, self.sent, self.landed = source, target, sent, landed
        self.count, self.next = count, 0
        self.device = (place.dp, place.bin_count - 1 - place.bin)

    def piece(self, index):
        return remote(
            self.source.at[index],
            self.target.at[index],
            self.sent.at[index],
            self.landed.at[index],
            self.device,
        )

    def pump(self, pieces=1):
        for _ in range(pieces):
            if self.next >= self.count:
                return
            if self.next >= WINDOW:
                self.piece(self.next - WINDOW).wait_send()
            self.piece(self.next).start()
            self.next += 1

    def loop(self, trips, body, pieces):
        pieces = max(0, min(pieces, self.count - self.next, trips))
        if pieces == 0:
            lax.fori_loop(0, trips, lambda i, carry: (body(i), carry)[1], 0)
            return
        if self.next < WINDOW:
            self.pump(WINDOW - self.next)
            pieces = max(0, min(pieces, self.count - self.next))
        first = self.next
        every = trips // max(pieces, 1)

        def step(i, carry):
            body(i)
            done = lax.div(i, every)

            @pl.when((lax.rem(i, every) == 0) & (done < pieces))
            def _():
                self.piece(first + done - WINDOW).wait_send()
                self.piece(first + done).start()

            return carry

        lax.fori_loop(0, trips, step, 0)
        self.next = first + pieces

    def finish(self):
        self.pump(self.count)
        for index in range(max(0, self.count - WINDOW), self.count):
            self.piece(index).wait_send()
        for index in range(self.count):
            self.piece(index).wait_recv()


class AllReduce:
    def __init__(self, place, mine, near, far, near_sent, near_landed, far_sent, far_landed):
        self.place, self.mine, self.near, self.far = place, mine, near, far
        self.near_count = place.dp_count * 2
        self.me = place.dp * 2 + place.core
        self.near_copies = []
        for apart in range(1, self.near_count):
            to = lax.rem(self.me + apart, self.near_count)
            device = (to // 2, place.chip * 2 + lax.rem(to, 2))
            self.near_copies.append(
                remote(mine, near.at[apart - 1], near_sent.at[apart - 1], near_landed.at[apart - 1], device)
            )
        self.far_copies = []
        for apart in range(1, place.chip_count):
            to = lax.rem(place.chip + apart, place.chip_count)
            device = (place.dp, to * 2 + place.core)
            self.far_copies.append(
                remote(
                    near.at[self.near_count - 1],
                    far.at[apart - 1],
                    far_sent.at[apart - 1],
                    far_landed.at[apart - 1],
                    device,
                )
            )

    def start_near(self):
        for copy in self.near_copies:
            copy.start()

    def finish_near(self):
        for copy in self.near_copies:
            copy.wait()
        count = self.near_count

        total = None
        for member in range(count):
            apart = lax.rem(self.me - member + count, count)
            other = self.near[jnp.maximum(apart - 1, 0)]
            part = jnp.where(apart == 0, self.mine[...], other)
            total = part if total is None else total + part
        self.near[count - 1] = total

    def start_far(self):
        for copy in self.far_copies:
            copy.start()

    def finish_far(self):
        for copy in self.far_copies:
            copy.wait()
        count = self.place.chip_count
        total = None
        for member in range(count):
            apart = lax.rem(self.place.chip - member + count, count)
            part = jnp.where(
                apart == 0, self.near[self.near_count - 1], self.far[jnp.maximum(apart - 1, 0)]
            )
            total = part if total is None else total + part
        return total

    @staticmethod
    def scratch(dp_count, bin_count, rows, width):
        near, far = dp_count * 2, bin_count // 2
        return [
            pltpu.VMEM((rows, width), F32),
            pltpu.VMEM((near, rows, width), F32),
            pltpu.VMEM((far, rows, width), F32),
            pltpu.SemaphoreType.DMA((near,)),
            pltpu.SemaphoreType.DMA((near,)),
            pltpu.SemaphoreType.DMA((far,)),
            pltpu.SemaphoreType.DMA((far,)),
        ]


class Halo:
    def __init__(self, place, to_left, to_right, from_left, from_right, sent, landed):
        self.place, self.from_left, self.from_right = place, from_left, from_right
        count = place.bin_count
        self.right = remote(
            to_right, from_left, sent.at[0], landed.at[0], (place.dp, lax.rem(place.bin + 1, count))
        )
        self.left = remote(
            to_left, from_right, sent.at[1], landed.at[1], (place.dp, lax.rem(place.bin + count - 1, count))
        )
        self.first = place.bin == 0
        self.last = place.bin == count - 1

    def start(self):
        @pl.when(jnp.logical_not(self.last))
        def _():
            self.right.start()

        @pl.when(jnp.logical_not(self.first))
        def _():
            self.left.start()

        @pl.when(self.first)
        def _():
            self.from_left[...] = jnp.zeros_like(self.from_left)

        @pl.when(self.last)
        def _():
            self.from_right[...] = jnp.zeros_like(self.from_right)

    def finish(self):
        @pl.when(jnp.logical_not(self.last))
        def _():
            self.right.wait_send()
            self.left.wait_recv()

        @pl.when(jnp.logical_not(self.first))
        def _():
            self.left.wait_send()
            self.right.wait_recv()


def eighth(values):
    rows, width = values.shape
    return jnp.sum(values.reshape(rows // 8, 8, width), axis=0)


def first_kernel(dims, meta, x, x_edges, cot, shard, params, *rest):
    dp_count, bin_count, seqs, rows, chans, feats, base, first = dims
    (x_low, x_high, weights, totals, stage, extra, landed_cot) = rest[:7]
    (sums, own_stage) = rest[7:9]
    reduce_refs = rest[9:16]
    (halo_sent, halo_landed, one_sent, one_landed, two_sent, two_landed, three_sent, three_landed, local) = rest[16:25]
    cot_sent, cot_landed = rest[25:27]
    place = Place(dp_count, bin_count)
    per_slot = rows // CHUNK
    place.barrier()

    halo = Halo(
        place, x_edges.at[0], x_edges.at[1], x_low, x_high, halo_sent, halo_landed
    )
    halo.start()
    keep = pltpu.make_async_copy(
        shard.at[place.dp], weights.at[place.chip, place.core, place.dp], local.at[0]
    )
    keep.start()
    ones = []
    for apart in range(1, place.chip_count):
        to = lax.rem(place.chip + apart, place.chip_count)
        ones.append(
            remote(
                shard.at[place.dp],
                weights.at[place.chip, place.core, place.dp],
                one_sent.at[apart - 1],
                one_landed.at[apart - 1],
                (place.dp, to * 2 + place.core),
            )
        )
        ones[-1].start()

    def pack(target, slot, piece, origin):
        target[slot * per_slot + piece] = cot[meta[2, origin] * per_slot + piece]

    for slot in range(first):
        for piece in range(per_slot):
            pack(own_stage, slot, piece, slot)
    stream = Stream(place, own_stage, landed_cot, cot_sent, cot_landed, first * per_slot)

    sums[...] = jnp.zeros_like(sums)
    total_bins = rows * bin_count
    row = lax.broadcasted_iota(jnp.int32, (rows, 1), 0) + place.bin * rows

    def statistics(i):
        micro = i // (seqs // MICRO)
        target = row + meta[1, i]
        inside = jnp.where((target >= 0) & (target < total_bins), 1.0, 0.0).astype(F32)
        values = x[i].astype(F32) * inside
        sums[micro] += eighth(values)
        sums[MICRO + micro] += eighth(values * values)

    lax.fori_loop(0, seqs, lambda i, carry: (statistics(i), carry)[1], 0)
    mine = reduce_refs[0]
    mine[0 : 2 * MICRO] = jnp.sum(sums[...], axis=1)
    mine[2 * MICRO : 4 * MICRO] = params[...]
    reduce = AllReduce(place, *reduce_refs)
    reduce.start_near()
    stream.pump(2)

    for slot in range(first, base):
        for piece in range(per_slot):
            pack(stage, slot - first, piece, slot)
    for slot in range(base, seqs):
        for piece in range(per_slot):
            pack(extra, slot - base, piece, slot)

    keep.wait()
    for copy in ones:
        copy.wait()
    twos = []
    for apart in range(1, dp_count):
        to = lax.rem(place.dp + apart, dp_count)
        part = weights.at[:, place.core, place.dp]
        twos.append(
            remote(
                part, part, two_sent.at[apart - 1], two_landed.at[apart - 1], (to, place.bin)
            )
        )
        twos[-1].start()
    reduce.finish_near()
    reduce.start_far()
    stream.pump(2)
    totals[...] = reduce.finish_far()
    stream.pump(2)
    for copy in twos:
        copy.wait()
    half = weights.at[:, place.core]
    three = remote(half, half, three_sent.at[0], three_landed.at[0], (place.dp, place.bin + 1 - 2 * place.core))
    three.start()
    stream.pump(2)
    three.wait()
    halo.finish()
    stream.finish()


def run_first(dims, meta, x, x_edges, cot, shard, params):
    dp_count, bin_count, seqs, rows, chans, feats, base, first = dims
    per_slot = rows // CHUNK
    quarter = chans // bin_count // dp_count
    chips = bin_count // 2
    wshape = (chips, 2, dp_count, TAPS + 1, quarter, feats)
    dma = pltpu.SemaphoreType.DMA
    return pl.pallas_call(
        functools.partial(first_kernel, dims),
        out_shape=(
            jax.ShapeDtypeStruct((seqs, EDGE, chans), BF16),
            jax.ShapeDtypeStruct((seqs, EDGE, chans), BF16),
            jax.ShapeDtypeStruct(wshape, BF16),
            jax.ShapeDtypeStruct((4 * MICRO, chans), F32),
            jax.ShapeDtypeStruct(((base - first) * per_slot, CHUNK, chans), BF16),
            jax.ShapeDtypeStruct(((seqs - base) * per_slot, CHUNK, chans), BF16),
            jax.ShapeDtypeStruct((first * per_slot, CHUNK, chans), BF16),
        ),
        in_specs=[smem(), vmem(), anywhere(), vmem(), anywhere(), vmem()],
        out_specs=(vmem(), vmem(), anywhere(), vmem(), vmem(), vmem(), anywhere()),
        scratch_shapes=[
            pltpu.VMEM((2 * MICRO, 8, chans), F32),
            pltpu.VMEM((first * per_slot, CHUNK, chans), BF16),
            *AllReduce.scratch(dp_count, bin_count, 4 * MICRO, chans),
            dma((2,)),
            dma((2,)),
            dma((chips,)),
            dma((chips,)),
            dma((dp_count,)),
            dma((dp_count,)),
            dma((1,)),
            dma((1,)),
            dma((1,)),
            dma((first * per_slot,)),
            dma((first * per_slot,)),
        ],
        compiler_params=pltpu.CompilerParams(
            collective_id=0, has_side_effects=True, vmem_limit_bytes=VMEM_LIMIT
        ),
        name="first",
    )(meta, x, x_edges, cot, shard, params)


def norm_rows(totals, gains, count, scale_ref, offset_ref, inverse_ref, shift_ref):
    for micro in range(MICRO):
        mean = totals[micro : micro + 1] / count
        second = totals[MICRO + micro : MICRO + micro + 1] / count
        inverse = lax.rsqrt(second - mean * mean + EPSILON)
        scale = inverse * gains[0]
        scale_ref[micro] = scale
        offset_ref[micro] = gains[1] - mean * scale
        if inverse_ref is not None:
            inverse_ref[micro] = inverse
            shift_ref[micro] = -mean * inverse


def gelu(v):
    half = 0.5 * v
    return half + half * jnp.tanh(v * (ROOT + (ROOT * CUBE) * (v * v)))


def gelu_both(v):
    square = v * v
    half = 0.5 * v
    t = jnp.tanh(v * (ROOT + (ROOT * CUBE) * square))
    value = half + half * t
    slope = 0.5 + 0.5 * t + half * (1.0 - t * t) * (ROOT + (3.0 * ROOT * CUBE) * square)
    return value, slope


def forward_kernel(dims, meta, x, x_low, x_high, w, proj, totals, stage, *rest):
    dp_count, bin_count, seqs, rows, chans, feats, base, first = dims
    (moved, conv, out, out_stage, out_extra, landed_cot, totals_two) = rest[:7]
    (scale_one, offset_one, scale_two, offset_two, sums) = rest[7:12]
    reduce_refs = rest[12:19]
    cot_sent, cot_landed = rest[19:21]
    place = Place(dp_count, bin_count)
    per_slot = rows // CHUNK
    pieces = (base - first) * per_slot
    place.barrier()
    stream = Stream(place, stage, landed_cot, cot_sent, cot_landed, pieces)
    stream.pump(WINDOW)
    per_micro = seqs // MICRO
    count = float(per_micro * rows * dp_count * bin_count)
    stats = totals[...]
    params = stats[2 * MICRO :]
    norm_rows(stats, (params[0:1], params[1:2]), count, scale_one, offset_one, None, None)
    proj_bias = params[2:3]
    sums[...] = jnp.zeros_like(sums)

    long_rows = rows + 2 * DILATION
    across = rows + 2 * EDGE
    local_row = lax.broadcasted_iota(jnp.int32, (long_rows, across), 0) - DILATION
    column = lax.broadcasted_iota(jnp.int32, (long_rows, across), 1)
    mask_row = lax.broadcasted_iota(jnp.int32, (long_rows, 1), 0) - DILATION
    total_bins = rows * bin_count

    def up(i):
        micro = i // per_micro
        reverse, shift = meta[0, i], meta[1, i]
        direction = 1 - 2 * reverse
        begin = reverse * (rows - 1)
        pick = jnp.where(column == local_row * direction + (begin - shift + EDGE), 1.0, 0.0).astype(BF16)
        source = jnp.concatenate([x_low[i], x[i], x_high[i]], axis=0)
        shifted = matmul(pick, source, 1, 0)
        moved[i] = shifted[DILATION : DILATION + rows].astype(BF16)
        hidden = gelu(shifted * scale_one[micro] + offset_one[micro])
        where = place.bin * rows + begin + mask_row * direction
        hidden = jnp.where((where >= 0) & (where < total_bins), hidden, 0.0)
        result = None
        for tap in range(TAPS):
            window = hidden[tap * DILATION : tap * DILATION + rows].astype(BF16)
            term = matmul(window, w[tap], 1, 0)
            result = term if result is None else result + term
        conv[i] = result
        sums[micro] += eighth(result)
        sums[MICRO + micro] += eighth(result * result)

    stream.loop(seqs, up, seqs)
    mine = reduce_refs[0]
    mine[...] = jnp.sum(sums[...], axis=1)
    reduce = AllReduce(place, *reduce_refs)
    reduce.start_near()
    stream.pump(1)
    reduce.finish_near()
    reduce.start_far()
    stream.pump(2)
    stats_two = reduce.finish_far()
    totals_two[...] = stats_two
    norm_rows(
        stats_two, (params[3:4, :feats], params[3:4, feats : 2 * feats]), count, scale_two, offset_two, None, None
    )

    def down(i):
        micro = i // per_micro
        hidden = gelu(conv[i] * scale_two[micro] + offset_two[micro]).astype(BF16)
        branch = matmul(hidden, proj[...], 1, 1) + proj_bias
        out[i] = (moved[i].astype(F32) + branch).astype(BF16)

    stream.loop(seqs, down, seqs)
    for slot in range(base):
        origin = meta[2, slot]
        for piece in range(per_slot):
            out_stage[slot * per_slot + piece] = out[origin, piece * CHUNK : (piece + 1) * CHUNK]
    for slot in range(base, seqs):
        origin = meta[2, slot]
        for piece in range(per_slot):
            out_extra[(slot - base) * per_slot + piece] = out[origin, piece * CHUNK : (piece + 1) * CHUNK]
    stream.finish()


def run_forward(dims, meta, x, x_low, x_high, w, proj, totals, stage):
    dp_count, bin_count, seqs, rows, chans, feats, base, first = dims
    per_slot = rows // CHUNK
    pieces = (base - first) * per_slot
    dma = pltpu.SemaphoreType.DMA
    return pl.pallas_call(
        functools.partial(forward_kernel, dims),
        out_shape=(
            jax.ShapeDtypeStruct((seqs, rows, chans), BF16),
            jax.ShapeDtypeStruct((seqs, rows, feats), F32),
            jax.ShapeDtypeStruct((seqs, rows, chans), BF16),
            jax.ShapeDtypeStruct((base * per_slot, CHUNK, chans), BF16),
            jax.ShapeDtypeStruct(((seqs - base) * per_slot, CHUNK, chans), BF16),
            jax.ShapeDtypeStruct((pieces, CHUNK, chans), BF16),
            jax.ShapeDtypeStruct((2 * MICRO, feats), F32),
        ),
        in_specs=[smem(), *[vmem()] * 6, anywhere()],
        out_specs=(*[vmem()] * 5, anywhere(), vmem()),
        scratch_shapes=[
            pltpu.VMEM((MICRO, 1, chans), F32),
            pltpu.VMEM((MICRO, 1, chans), F32),
            pltpu.VMEM((MICRO, 1, feats), F32),
            pltpu.VMEM((MICRO, 1, feats), F32),
            pltpu.VMEM((2 * MICRO, 8, feats), F32),
            *AllReduce.scratch(dp_count, bin_count, 2 * MICRO, feats),
            dma((pieces,)),
            dma((pieces,)),
        ],
        compiler_params=pltpu.CompilerParams(
            collective_id=1, has_side_effects=True, vmem_limit_bytes=VMEM_LIMIT
        ),
        name="forward",
    )(meta, x, x_low, x_high, w, proj, totals, stage)


def backward_kernel(dims, meta, moved, conv, w, proj, totals, totals_two, cot, cot_a, cot_b, cot_c, out_stage, *rest):
    dp_count, bin_count, seqs, rows, chans, feats, base, first = dims
    (grads, low_edge, high_edge, landed_out, sums_two_out, sums_one_out, partial) = rest[:7]
    (cots, scale_one, offset_one, inverse_one, shift_one) = rest[7:12]
    (scale_two, offset_two, inverse_two, shift_two) = rest[12:16]
    (grad_two, grad_one, hidden_all, cotangents_unused, conv_grad, hidden_group, window_group) = rest[16:23]
    (sums_two, sums_one, bias_sum, const_two, const_one) = rest[23:28]
    (send_left, send_right, from_left, from_right, last_left, last_right, last_from_left, last_from_right) = rest[28:36]
    reduce_two = rest[36:43]
    reduce_one = rest[43:50]
    (local, halo_sent, halo_landed, last_sent, last_landed, out_sent, out_landed) = rest[50:57]
    place = Place(dp_count, bin_count)
    per_slot = rows // CHUNK
    per_micro = seqs // MICRO
    loads = [
        pltpu.make_async_copy(cot, cots.at[0:seqs], local.at[0]),
        pltpu.make_async_copy(cot_a, cots.at[seqs : seqs + first], local.at[1]),
        pltpu.make_async_copy(cot_b, cots.at[seqs + first : seqs + base], local.at[2]),
        pltpu.make_async_copy(cot_c, cots.at[seqs + base : 2 * seqs], local.at[3]),
    ]
    for load in loads:
        load.start()
    place.barrier()
    stream = Stream(place, out_stage, landed_out, out_sent, out_landed, base * per_slot)
    stream.pump(WINDOW)
    count = float(per_micro * rows * dp_count * bin_count)
    stats = totals[...]
    params = stats[2 * MICRO :]
    stats_two = totals_two[...]
    norm_rows(stats, (params[0:1], params[1:2]), count, scale_one, offset_one, inverse_one, shift_one)
    norm_rows(
        stats_two,
        (params[3:4, :feats], params[3:4, feats : 2 * feats]),
        count,
        scale_two,
        offset_two,
        inverse_two,
        shift_two,
    )
    sums_two[...] = jnp.zeros_like(sums_two)
    sums_one[...] = jnp.zeros_like(sums_one)
    bias_sum[...] = jnp.zeros_like(bias_sum)
    partial[...] = jnp.zeros_like(partial)
    for load in loads:
        load.wait()

    def head(i):
        micro = i // per_micro
        cotangent = cots[meta[3, i]]
        bias_sum[...] += eighth(cotangent.astype(F32))
        values = conv[i]
        hidden, slope = gelu_both(values * scale_two[micro] + offset_two[micro])
        hidden_all[i] = hidden.astype(BF16)
        grad = matmul(cotangent, proj[...], 1, 0) * slope
        grad_two[i] = grad
        centred = values * inverse_two[micro] + shift_two[micro]
        sums_two[micro] += eighth(grad)
        sums_two[MICRO + micro] += eighth(grad * centred)
        partial[TAPS] += matmul(cotangent, hidden_all[i], 0, 0)

    stream.loop(seqs, head, seqs // 2)
    mine = reduce_two[0]
    mine[0 : 2 * MICRO] = jnp.sum(sums_two[...], axis=1)
    bias_row = jnp.sum(bias_sum[...], axis=0, keepdims=True)
    spare = jnp.zeros((1, feats), F32)
    for part in range(2 * MICRO):
        begin = part * feats
        mine[2 * MICRO + part : 2 * MICRO + part + 1] = bias_row[:, begin : begin + feats] if begin < chans else spare
    reduce = AllReduce(place, *reduce_two)
    reduce.start_near()
    stream.pump(1)
    reduce.finish_near()
    reduce.start_far()
    stream.pump(2)
    back_two = reduce.finish_far()
    sums_two_out[...] = back_two
    for micro in range(MICRO):
        const_two[micro] = back_two[micro : micro + 1] / count
        const_two[MICRO + micro] = back_two[MICRO + micro : MICRO + micro + 1] / count

    def middle(i):
        micro = i // per_micro
        reverse = meta[0, i]
        centred = conv[i] * inverse_two[micro] + shift_two[micro]
        value = scale_two[micro] * (grad_two[i] - const_two[micro] - centred * const_two[MICRO + micro])
        value = value.astype(BF16).astype(F32)
        conv_grad[i] = value
        top, bottom = value[:DILATION], value[rows - DILATION :]
        send_left[i] = jnp.where(reverse > 0, bottom, top)
        send_right[i] = jnp.where(reverse > 0, top, bottom)

    lax.fori_loop(0, seqs, lambda i, carry: (middle(i), carry)[1], 0)
    halo = Halo(place, send_left, send_right, from_left, from_right, halo_sent, halo_landed)
    halo.start()
    stream.pump(2)
    halo.finish()

    def tail(i):
        micro = i // per_micro
        inner = lax.rem(i, per_micro)
        reverse = meta[0, i]
        left, right = from_left[i], from_right[i]
        low = jnp.where(reverse > 0, right, left)
        high = jnp.where(reverse > 0, left, right)
        full = jnp.concatenate([low, conv_grad[i], high], axis=0)
        grad = None
        for tap in range(TAPS):
            begin = (TAPS - 1 - tap) * DILATION
            window = full[begin : begin + rows].astype(BF16)
            window_group[tap, pl.ds(pl.multiple_of(inner * rows, rows), rows)] = window
            term = matmul(window, w[tap], 1, 1)
            grad = term if grad is None else grad + term
        values = moved[i].astype(F32)
        hidden, slope = gelu_both(values * scale_one[micro] + offset_one[micro])
        hidden_group[pl.ds(pl.multiple_of(inner * rows, rows), rows)] = hidden.astype(BF16)
        grad = grad * slope
        grad_one[i] = grad
        centred = values * inverse_one[micro] + shift_one[micro]
        sums_one[micro] += eighth(grad)
        sums_one[MICRO + micro] += eighth(grad * centred)

    for micro in range(MICRO):

        def one(inner, carry, micro=micro):
            tail(micro * per_micro + inner)
            return carry

        stream.loop(per_micro, lambda inner, micro=micro: tail(micro * per_micro + inner), per_micro // 2)
        for tap in range(TAPS):
            partial[tap] += matmul(hidden_group[...], window_group[tap], 0, 0)

    mine = reduce_one[0]
    mine[...] = jnp.sum(sums_one[...], axis=1)
    reduce = AllReduce(place, *reduce_one)
    reduce.start_near()
    stream.pump(1)
    reduce.finish_near()
    reduce.start_far()
    stream.pump(2)
    back_one = reduce.finish_far()
    sums_one_out[...] = back_one
    for micro in range(MICRO):
        const_one[micro] = back_one[micro : micro + 1] / count
        const_one[MICRO + micro] = back_one[MICRO + micro : MICRO + micro + 1] / count

    def end(i):
        micro = i // per_micro
        reverse = meta[0, i]
        centred = moved[i].astype(F32) * inverse_one[micro] + shift_one[micro]
        value = grad_one[i] - const_one[micro] - centred * const_one[MICRO + micro]
        value = cots[meta[3, i]].astype(F32) + scale_one[micro] * value
        grads[i] = value.astype(BF16)
        top, bottom = value[:EDGE].astype(BF16), value[rows - EDGE :].astype(BF16)
        last_left[i] = jnp.where(reverse > 0, bottom, top)
        last_right[i] = jnp.where(reverse > 0, top, bottom)

    stream.loop(seqs, end, seqs // 4)
    last = Halo(place, last_left, last_right, last_from_left, last_from_right, last_sent, last_landed)
    last.start()
    stream.pump(2)
    last.finish()
    low_edge[...] = last_from_left[...]
    high_edge[...] = last_from_right[...]
    stream.finish()


def run_backward(dims, meta, moved, conv, w, proj, totals, totals_two, cot, cot_a, cot_b, cot_c, out_stage):
    dp_count, bin_count, seqs, rows, chans, feats, base, first = dims
    per_slot = rows // CHUNK
    per_micro = seqs // MICRO
    dma = pltpu.SemaphoreType.DMA
    wide = pltpu.VMEM((MICRO, 1, chans), F32)
    narrow = pltpu.VMEM((MICRO, 1, feats), F32)
    return pl.pallas_call(
        functools.partial(backward_kernel, dims),
        out_shape=(
            jax.ShapeDtypeStruct((seqs, rows, chans), BF16),
            jax.ShapeDtypeStruct((seqs, EDGE, chans), BF16),
            jax.ShapeDtypeStruct((seqs, EDGE, chans), BF16),
            jax.ShapeDtypeStruct((base * per_slot, CHUNK, chans), BF16),
            jax.ShapeDtypeStruct((4 * MICRO, feats), F32),
            jax.ShapeDtypeStruct((2 * MICRO, chans), F32),
            jax.ShapeDtypeStruct((TAPS + 1, chans, feats), F32),
        ),
        in_specs=[smem(), *[vmem()] * 6, *[anywhere()] * 5],
        out_specs=(vmem(), vmem(), vmem(), anywhere(), vmem(), vmem(), vmem()),
        scratch_shapes=[
            pltpu.VMEM((2 * seqs, rows, chans), BF16),
            wide,
            wide,
            wide,
            wide,
            narrow,
            narrow,
            narrow,
            narrow,
            pltpu.VMEM((seqs, rows, feats), F32),
            pltpu.VMEM((seqs, rows, chans), F32),
            pltpu.VMEM((seqs, rows, feats), BF16),
            pltpu.VMEM((8, 128), F32),
            pltpu.VMEM((seqs, rows, feats), F32),
            pltpu.VMEM((per_micro * rows, chans), BF16),
            pltpu.VMEM((TAPS, per_micro * rows, feats), BF16),
            pltpu.VMEM((2 * MICRO, 8, feats), F32),
            pltpu.VMEM((2 * MICRO, 8, chans), F32),
            pltpu.VMEM((8, chans), F32),
            pltpu.VMEM((2 * MICRO, 1, feats), F32),
            pltpu.VMEM((2 * MICRO, 1, chans), F32),
            *[pltpu.VMEM((seqs, DILATION, feats), F32)] * 4,
            *[pltpu.VMEM((seqs, EDGE, chans), BF16)] * 4,
            *AllReduce.scratch(dp_count, bin_count, 4 * MICRO, feats),
            *AllReduce.scratch(dp_count, bin_count, 2 * MICRO, chans),
            dma((4,)),
            dma((2,)),
            dma((2,)),
            dma((2,)),
            dma((2,)),
            dma((base * per_slot,)),
            dma((base * per_slot,)),
        ],
        compiler_params=pltpu.CompilerParams(
            collective_id=2, has_side_effects=True, vmem_limit_bytes=VMEM_LIMIT
        ),
        name="backward",
    )(meta, moved, conv, w, proj, totals, totals_two, cot, cot_a, cot_b, cot_c, out_stage)


def last_kernel(rows, meta, grad, left, right, out, near, far, result_out, result_grad):
    i = pl.program_id(0)
    reverse, shift, slot, near_slots = meta[0, i], meta[1, i], meta[4, i], meta[5, i]
    crossed = jnp.where(slot < near_slots, near[0], far[0])
    result_out[0] = jnp.where(reverse > 0, crossed, out[0])
    low = jnp.where(reverse > 0, right[0], left[0])
    high = jnp.where(reverse > 0, left[0], right[0])
    source = jnp.concatenate([low, grad[0], high], axis=0)
    across = rows + 2 * EDGE
    row = lax.broadcasted_iota(jnp.int32, (rows, across), 0)
    column = lax.broadcasted_iota(jnp.int32, (rows, across), 1)
    place = jnp.where(reverse > 0, rows - 1 - row - shift, row + shift) + EDGE
    pick = jnp.where(column == place, 1.0, 0.0).astype(BF16)
    result_grad[0] = matmul(pick, source, 1, 0).astype(BF16)


def run_last(dims, meta, grad, left, right, out, near, far):
    dp_count, bin_count, seqs, rows, chans, feats, base, first = dims
    full = (1, rows, chans)
    edge = (1, EDGE, chans)
    own = lambda i, meta: (i, 0, 0)
    return pl.pallas_call(
        functools.partial(last_kernel, rows),
        out_shape=(
            jax.ShapeDtypeStruct((seqs, rows, chans), BF16),
            jax.ShapeDtypeStruct((seqs, rows, chans), BF16),
        ),
        grid_spec=pltpu.PrefetchScalarGridSpec(
            num_scalar_prefetch=1,
            grid=(seqs,),
            in_specs=[
                pl.BlockSpec(full, own),
                pl.BlockSpec(edge, own),
                pl.BlockSpec(edge, own),
                pl.BlockSpec(full, own),
                pl.BlockSpec(full, lambda i, meta: (jnp.minimum(meta[4, i], base - 1), 0, 0)),
                pl.BlockSpec(full, lambda i, meta: (jnp.maximum(meta[4, i] - base, 0), 0, 0)),
            ],
            out_specs=(pl.BlockSpec(full, own), pl.BlockSpec(full, own)),
        ),
        name="last",
    )(meta, grad, left, right, out, near, far)


def local(
    activations,
    shift_bins,
    reverse_flags,
    gain_one,
    bias_one,
    conv_weight,
    gain_two,
    bias_two,
    proj_weight,
    proj_bias,
    cotangent,
):
    seqs, rows, chans = activations.shape
    feats = conv_weight.shape[2]
    dp_count, bin_count = lax.axis_size("dp"), lax.axis_size("bins")
    dp, bins = lax.axis_index("dp"), lax.axis_index("bins")
    per_slot = rows // CHUNK
    base, first = BASE_SLOTS, FIRST_SLOTS
    dims = (dp_count, bin_count, seqs, rows, chans, feats, base, first)

    reverse = (reverse_flags > 0).astype(jnp.int32)
    index = jnp.arange(seqs, dtype=jnp.int32)
    before = jnp.sum(jnp.where(index[None, :] < index[:, None], reverse[None, :], 0), axis=1)
    slot = jnp.where(reverse > 0, before, 0)
    origin = jnp.sum(
        jnp.where((slot[None, :] == index[:, None]) & (reverse[None, :] > 0), index[None, :], 0), axis=1
    )
    chosen = jnp.where(reverse > 0, seqs + slot, index)
    meta = jnp.stack([reverse, shift_bins, origin, chosen, slot, jnp.full((seqs,), base, jnp.int32)])
    reversed_count = jnp.sum(reverse)

    lane = jnp.arange(chans, dtype=jnp.int32)
    at_home = dp == 0

    def spread(vector):
        size = vector.shape[0]
        width = size * bin_count
        held = jnp.tile(vector.astype(F32), bin_count)
        return jnp.where((jnp.arange(width) // size == bins) & at_home, held, 0.0)

    counts = jnp.where((lane == dp) & (bins == 0), reversed_count.astype(F32), 0.0)
    nothing = jnp.zeros((chans,), F32)
    params = jnp.stack(
        [
            spread(gain_one),
            spread(bias_one),
            spread(proj_bias),
            jnp.concatenate([spread(gain_two), spread(bias_two)]),
            counts,
            nothing,
            nothing,
            nothing,
        ]
    )
    share = chans // bin_count
    quarter = share // dp_count
    shard = jnp.concatenate([conv_weight, proj_weight.T[None]], axis=0)
    shard = shard.reshape(TAPS + 1, dp_count, quarter, feats).transpose(1, 0, 2, 3)
    edges = jnp.stack([activations[:, :EDGE], activations[:, rows - EDGE :]])

    x_low, x_high, weights, totals, stage, cot_extra, cot_a = run_first(
        dims, meta, activations, edges, cotangent.reshape(seqs * per_slot, CHUNK, chans), shard, params
    )
    full = weights.transpose(3, 0, 1, 2, 4, 5).reshape(TAPS + 1, chans, feats)
    w, proj = full[:TAPS], full[TAPS]
    most = jnp.max(totals[3 * MICRO, :dp_count]).astype(jnp.int32)

    moved, conv, out, out_stage, out_extra, cot_b, totals_two = run_forward(
        dims, meta, activations, x_low, x_high, w, proj, totals, stage
    )

    pairs = [(source, bin_count - 1 - source) for source in range(bin_count)]

    def crossing(slots, pair):
        if slots == 0:
            return pair
        held = slots * per_slot
        got = lax.ppermute(jnp.concatenate([item[:held] for item in pair]), "bins", pairs)
        return tuple(
            lax.dynamic_update_slice_in_dim(item, got[k * held : (k + 1) * held], 0, 0)
            for k, item in enumerate(pair)
        )

    extra = lax.switch(
        jnp.clip(most - base, 0, seqs - base),
        [functools.partial(crossing, slots) for slots in range(seqs - base + 1)],
        (cot_extra, out_extra),
    )

    slots_of = lambda item: item.reshape(-1, rows, chans)
    grads, low_edge, high_edge, out_near, back_two, back_one, partial = run_backward(
        dims,
        meta,
        moved,
        conv,
        w,
        proj,
        totals,
        totals_two,
        cotangent,
        slots_of(cot_a),
        slots_of(cot_b),
        slots_of(extra[0]),
        out_stage,
    )
    output, grad_activations = run_last(
        dims, meta, grads, low_edge, high_edge, out, slots_of(out_near), slots_of(extra[1])
    )

    scattered = lax.psum_scatter(partial, ("dp", "bins"), scatter_dimension=1, tiled=True)
    wide = chans // (dp_count * bin_count)
    narrow = feats // bin_count
    wide_at = (dp * bin_count + bins) * wide
    narrow_at = bins * narrow
    bias_sum = back_two[2 * MICRO :].reshape(-1)[:chans]
    cut = lax.dynamic_slice_in_dim
    return (
        output,
        grad_activations,
        cut(jnp.sum(back_one[MICRO:], axis=0), wide_at, wide),
        cut(jnp.sum(back_one[:MICRO], axis=0), wide_at, wide),
        scattered[:TAPS],
        cut(jnp.sum(back_two[MICRO : 2 * MICRO], axis=0), narrow_at, narrow),
        cut(jnp.sum(back_two[:MICRO], axis=0), narrow_at, narrow),
        scattered[TAPS].T,
        cut(bias_sum, wide_at, wide),
    )


def solution(mesh):
    placed = (
        P("dp", "bins", None),
        P("dp"),
        P("dp"),
        P("bins"),
        P("bins"),
        P(None, "bins", None),
        P("bins"),
        P("bins"),
        P(None, "bins"),
        P("bins"),
        P("dp", "bins", None),
    )
    return jax.shard_map(
        local,
        mesh=mesh,
        in_specs=placed,
        out_specs=(
            P("dp", "bins", None),
            P("dp", "bins", None),
            P(("dp", "bins")),
            P(("dp", "bins")),
            P(None, ("dp", "bins"), None),
            P("bins"),
            P("bins"),
            P(None, ("dp", "bins")),
            P(("dp", "bins")),
        ),
        check_vma=False,
    )
```

```python
import functools

import jax
import jax.numpy as jnp
from jax import lax
from jax.experimental import pallas as pl
from jax.experimental.pallas import tpu as pltpu
from jax.sharding import PartitionSpec as P

TAPS = 3
DILATION = 8
MICRO = 4
EPSILON = 1e-05
CHUNK = 32
BASE_SLOTS = 8
PUMPS = (2, 2, 3, 3, 2, 12, 1, 2, 3)
WINDOW = 2
EDGE = 16
VMEM_LIMIT = 60 * 1024 * 1024
MESH = pl.DeviceIdType.MESH
F32 = jnp.float32
BF16 = jnp.bfloat16
ROOT = 0.7978845608028654
CUBE = 0.044715


def vmem():
    return pl.BlockSpec(memory_space=pltpu.VMEM)


def smem():
    return pl.BlockSpec(memory_space=pltpu.SMEM)


def anywhere():
    return pl.BlockSpec(memory_space=pl.ANY)


def matmul(a, b, ca, cb):
    return lax.dot_general(a, b, (((ca,), (cb,)), ((), ())), preferred_element_type=F32)


class Place:
    def __init__(self, dp_count, bin_count):
        self.dp_count, self.bin_count = dp_count, bin_count
        self.chip_count = bin_count // 2
        self.dp = lax.axis_index("dp")
        self.bin = lax.axis_index("bins")
        self.chip = self.bin // 2
        self.core = lax.rem(self.bin, 2)

    def barrier(self):
        semaphore = pltpu.get_barrier_semaphore()
        for apart in range(1, self.bin_count):
            other = (self.dp, lax.rem(self.bin + apart, self.bin_count))
            pl.semaphore_signal(semaphore, inc=1, device_id=other, device_id_type=MESH)
        for apart in range(1, self.dp_count):
            for core in range(2):
                other = (lax.rem(self.dp + apart, self.dp_count), self.chip * 2 + core)
                pl.semaphore_signal(semaphore, inc=1, device_id=other, device_id_type=MESH)
        pl.semaphore_wait(semaphore, self.bin_count - 1 + 2 * (self.dp_count - 1))


def remote(source, target, sent, landed, device):
    return pltpu.make_async_remote_copy(
        src_ref=source,
        dst_ref=target,
        send_sem=sent,
        recv_sem=landed,
        device_id=device,
        device_id_type=MESH,
    )


class Stream:
    def __init__(self, place, source, target, sent, landed, count):
        self.source, self.target, self.sent, self.landed = source, target, sent, landed
        self.count, self.next = count, 0
        self.device = (place.dp, place.bin_count - 1 - place.bin)

    def piece(self, index):
        return remote(
            self.source.at[index],
            self.target.at[index],
            self.sent.at[index],
            self.landed.at[index],
            self.device,
        )

    def pump(self, pieces=1):
        for _ in range(pieces):
            if self.next >= self.count:
                return
            if self.next >= WINDOW:
                self.piece(self.next - WINDOW).wait_send()
            self.piece(self.next).start()
            self.next += 1

    def loop(self, trips, body, pieces):
        pieces = max(0, min(pieces, self.count - self.next, trips))
        if pieces == 0:
            lax.fori_loop(0, trips, lambda i, carry: (body(i), carry)[1], 0)
            return
        if self.next < WINDOW:
            self.pump(WINDOW - self.next)
            pieces = max(0, min(pieces, self.count - self.next))
        first = self.next
        every = trips // max(pieces, 1)

        def step(i, carry):
            body(i)
            done = lax.div(i, every)

            @pl.when((lax.rem(i, every) == 0) & (done < pieces))
            def _():
                self.piece(first + done - WINDOW).wait_send()
                self.piece(first + done).start()

            return carry

        lax.fori_loop(0, trips, step, 0)
        self.next = first + pieces

    def finish(self):
        self.pump(self.count)
        for index in range(max(0, self.count - WINDOW), self.count):
            self.piece(index).wait_send()
        for index in range(self.count):
            self.piece(index).wait_recv()


class AllReduce:
    def __init__(self, place, mine, near, far, near_sent, near_landed, far_sent, far_landed):
        self.place, self.mine, self.near, self.far = place, mine, near, far
        self.near_count = place.dp_count * 2
        self.me = place.dp * 2 + place.core
        self.near_copies = []
        for apart in range(1, self.near_count):
            to = lax.rem(self.me + apart, self.near_count)
            device = (to // 2, place.chip * 2 + lax.rem(to, 2))
            self.near_copies.append(
                remote(mine, near.at[apart - 1], near_sent.at[apart - 1], near_landed.at[apart - 1], device)
            )
        self.far_copies = []
        for apart in range(1, place.chip_count):
            to = lax.rem(place.chip + apart, place.chip_count)
            device = (place.dp, to * 2 + place.core)
            self.far_copies.append(
                remote(
                    near.at[self.near_count - 1],
                    far.at[apart - 1],
                    far_sent.at[apart - 1],
                    far_landed.at[apart - 1],
                    device,
                )
            )

    def start_near(self):
        for copy in self.near_copies:
            copy.start()

    def finish_near(self):
        for copy in self.near_copies:
            copy.wait()
        count = self.near_count

        total = None
        for member in range(count):
            apart = lax.rem(self.me - member + count, count)
            other = self.near[jnp.maximum(apart - 1, 0)]
            part = jnp.where(apart == 0, self.mine[...], other)
            total = part if total is None else total + part
        self.near[count - 1] = total

    def start_far(self):
        for copy in self.far_copies:
            copy.start()

    def finish_far(self):
        for copy in self.far_copies:
            copy.wait()
        count = self.place.chip_count
        total = None
        for member in range(count):
            apart = lax.rem(self.place.chip - member + count, count)
            part = jnp.where(
                apart == 0, self.near[self.near_count - 1], self.far[jnp.maximum(apart - 1, 0)]
            )
            total = part if total is None else total + part
        return total

    @staticmethod
    def scratch(dp_count, bin_count, rows, width):
        near, far = dp_count * 2, bin_count // 2
        return [
            pltpu.VMEM((rows, width), F32),
            pltpu.VMEM((near, rows, width), F32),
            pltpu.VMEM((far, rows, width), F32),
            pltpu.SemaphoreType.DMA((near,)),
            pltpu.SemaphoreType.DMA((near,)),
            pltpu.SemaphoreType.DMA((far,)),
            pltpu.SemaphoreType.DMA((far,)),
        ]


class Halo:
    def __init__(self, place, to_left, to_right, from_left, from_right, sent, landed):
        self.place, self.from_left, self.from_right = place, from_left, from_right
        count = place.bin_count
        self.right = remote(
            to_right, from_left, sent.at[0], landed.at[0], (place.dp, lax.rem(place.bin + 1, count))
        )
        self.left = remote(
            to_left, from_right, sent.at[1], landed.at[1], (place.dp, lax.rem(place.bin + count - 1, count))
        )
        self.first = place.bin == 0
        self.last = place.bin == count - 1

    def start(self):
        @pl.when(jnp.logical_not(self.last))
        def _():
            self.right.start()

        @pl.when(jnp.logical_not(self.first))
        def _():
            self.left.start()

        @pl.when(self.first)
        def _():
            self.from_left[...] = jnp.zeros_like(self.from_left)

        @pl.when(self.last)
        def _():
            self.from_right[...] = jnp.zeros_like(self.from_right)

    def finish(self):
        @pl.when(jnp.logical_not(self.last))
        def _():
            self.right.wait_send()
            self.left.wait_recv()

        @pl.when(jnp.logical_not(self.first))
        def _():
            self.left.wait_send()
            self.right.wait_recv()


def eighth(values):
    rows, width = values.shape
    return jnp.sum(values.reshape(rows // 8, 8, width), axis=0)


def norm_rows(totals, gains, count, scale_ref, offset_ref, inverse_ref, shift_ref):
    for micro in range(MICRO):
        mean = totals[micro : micro + 1] / count
        second = totals[MICRO + micro : MICRO + micro + 1] / count
        inverse = lax.rsqrt(second - mean * mean + EPSILON)
        scale = inverse * gains[0]
        scale_ref[micro] = scale
        offset_ref[micro] = gains[1] - mean * scale
        if inverse_ref is not None:
            inverse_ref[micro] = inverse
            shift_ref[micro] = -mean * inverse


def gelu(v):
    half = 0.5 * v
    return half + half * jnp.tanh(v * (ROOT + (ROOT * CUBE) * (v * v)))


def gelu_both(v):
    square = v * v
    half = 0.5 * v
    t = jnp.tanh(v * (ROOT + (ROOT * CUBE) * square))
    value = half + half * t
    slope = 0.5 + 0.5 * t + half * (1.0 - t * t) * (ROOT + (3.0 * ROOT * CUBE) * square)
    return value, slope


def front_kernel(dims, meta, x_in, cot, shard, vectors, *rest):
    dp_count, bin_count, seqs, rows, chans, feats, base = dims
    (moved_out, conv_out, out_out, out_stage, out_extra, cot_extra, landed_cot, weights_out) = rest[:8]
    (stats_out, params_out, totals_two) = rest[8:11]
    (x, x_low, x_high, to_left, to_right, moved, conv, out, w, stage) = rest[11:21]
    (sums_one, sums, scale_one, offset_one, scale_two, offset_two) = rest[21:27]
    reduce_first = rest[27:34]
    reduce_second = rest[34:41]
    (local, stores, halo_sent, halo_landed, one_sent, one_landed, two_sent, two_landed, three_sent, three_landed) = rest[41:51]
    cot_sent, cot_landed = rest[51:53]
    place = Place(dp_count, bin_count)
    per_slot = rows // CHUNK
    per_micro = seqs // MICRO
    share = chans // bin_count
    group = TAPS + 1
    total_bins = rows * bin_count
    load = pltpu.make_async_copy(x_in, x, local.at[0])
    load.start()
    tap = lax.rem(place.dp, group)
    home = pl.ds(pl.multiple_of(place.bin * share, 8), share)
    keep = pltpu.make_async_copy(shard.at[tap], weights_out.at[tap, home], local.at[1])
    keep.start()
    place.barrier()

    ones = []
    for apart in range(1, place.chip_count):
        to = lax.rem(place.chip + apart, place.chip_count)
        ones.append(
            remote(
                shard.at[tap],
                weights_out.at[tap, home],
                one_sent.at[apart - 1],
                one_landed.at[apart - 1],
                (place.dp, to * 2 + place.core),
            )
        )
        ones[-1].start()
    for slot in range(base):
        origin = meta[2, slot] * per_slot
        for piece in range(per_slot):
            stage[slot * per_slot + piece] = cot[origin + piece]
    stream = Stream(place, stage, landed_cot, cot_sent, cot_landed, base * per_slot)
    stream.pump(WINDOW)
    load.wait()
    to_left[...] = x[:, :EDGE]
    to_right[...] = x[:, rows - EDGE :]
    halo = Halo(place, to_left, to_right, x_low, x_high, halo_sent, halo_landed)
    halo.start()

    sums_one[...] = jnp.zeros_like(sums_one)
    row = lax.broadcasted_iota(jnp.int32, (rows, 1), 0) + place.bin * rows

    def statistics(i):
        micro = i // per_micro
        target = row + meta[1, i]
        inside = jnp.where((target >= 0) & (target < total_bins), 1.0, 0.0).astype(F32)
        values = x[i].astype(F32) * inside
        sums_one[micro] += eighth(values)
        sums_one[MICRO + micro] += eighth(values * values)

    stream.loop(seqs, statistics, PUMPS[0])
    mine = reduce_first[0]
    mine[0 : 2 * MICRO] = jnp.sum(sums_one[...], axis=1)
    mine[2 * MICRO :] = jnp.zeros((bin_count, chans), F32)
    lane = lax.broadcasted_iota(jnp.int32, (1, chans), 1)
    reversed_count = jnp.int32(0)
    for i in range(seqs):
        reversed_count += meta[0, i]
    at_home = jnp.where(place.dp == 0, 1.0, 0.0).astype(F32)
    at_first = jnp.where(place.bin == 0, 1.0, 0.0).astype(F32)
    counts = jnp.where(lane == feats + place.dp, reversed_count.astype(F32) * at_first, 0.0)
    mine[pl.ds(2 * MICRO + place.bin, 1)] = vectors[...] * at_home + counts
    reduce = AllReduce(place, *reduce_first)
    reduce.start_near()
    stream.pump(PUMPS[1])
    for slot in range(base, seqs):
        origin = meta[2, slot] * per_slot
        for piece in range(per_slot):
            cot_extra[(slot - base) * per_slot + piece] = cot[origin + piece]
    reduce.finish_near()
    reduce.start_far()
    keep.wait()
    for copy in ones:
        copy.wait()
    twos = []
    for apart in range(1, group):
        to = (place.dp // group) * group + lax.rem(tap + apart, group)
        for chip in range(place.chip_count):
            part = weights_out.at[tap, pl.ds(pl.multiple_of((chip * 2 + place.core) * share, 8), share)]
            index = (apart - 1) * place.chip_count + chip
            twos.append(remote(part, part, two_sent.at[index], two_landed.at[index], (to, place.bin)))
            twos[-1].start()
    stream.pump(PUMPS[2])
    first = reduce.finish_far()
    stats_out[...] = first[: 2 * MICRO]
    params_out[...] = jnp.zeros_like(params_out)
    begin = 0
    for index, (line, offset, width) in enumerate(
        ((0, 0, share), (1, 0, share), (2, 0, share), (3, 0, share // 2), (3, feats, share // 2))
    ):
        for member in range(bin_count):
            left = offset + member * width
            params_out[line : line + 1, left : left + width] = first[
                2 * MICRO + member : 2 * MICRO + member + 1, begin : begin + width
            ]
        begin += width
    params_out[4:5] = first[2 * MICRO : 2 * MICRO + 1]
    stream.pump(PUMPS[3])
    for copy in twos:
        copy.wait()
    threes = []
    for line in range(group):
        for chip in range(place.chip_count):
            part = weights_out.at[line, pl.ds(pl.multiple_of((chip * 2 + place.core) * share, 8), share)]
            index = line * place.chip_count + chip
            threes.append(
                remote(
                    part,
                    part,
                    three_sent.at[index],
                    three_landed.at[index],
                    (place.dp, place.bin + 1 - 2 * place.core),
                )
            )
            threes[-1].start()
    count = float(per_micro * rows * dp_count * bin_count)
    params = params_out[...]
    norm_rows(first, (params[0:1], params[1:2]), count, scale_one, offset_one, None, None)
    proj_bias = params[2:3]
    sums[...] = jnp.zeros_like(sums)
    stream.pump(PUMPS[4])
    halo.finish()
    for copy in threes:
        copy.wait()
    fetch = pltpu.make_async_copy(weights_out, w, local.at[2])
    fetch.start()
    fetch.wait()

    long_rows = rows + 2 * DILATION
    across = rows + 2 * EDGE
    local_row = lax.broadcasted_iota(jnp.int32, (long_rows, across), 0) - DILATION
    column = lax.broadcasted_iota(jnp.int32, (long_rows, across), 1)
    mask_row = lax.broadcasted_iota(jnp.int32, (long_rows, 1), 0) - DILATION

    def up(i):
        micro = i // per_micro
        reverse, shift = meta[0, i], meta[1, i]
        direction = 1 - 2 * reverse
        begin = reverse * (rows - 1)
        pick = jnp.where(column == local_row * direction + (begin - shift + EDGE), 1.0, 0.0).astype(BF16)
        source = jnp.concatenate([x_low[i], x[i], x_high[i]], axis=0)
        shifted = matmul(pick, source, 1, 0)
        moved[i] = shifted[DILATION : DILATION + rows].astype(BF16)
        pltpu.make_async_copy(moved.at[i], moved_out.at[i], stores.at[0]).start()
        hidden = gelu(shifted * scale_one[micro] + offset_one[micro])
        where = place.bin * rows + begin + mask_row * direction
        hidden = jnp.where((where >= 0) & (where < total_bins), hidden, 0.0)
        result = None
        for tap in range(TAPS):
            window = hidden[tap * DILATION : tap * DILATION + rows].astype(BF16)
            term = matmul(window, w[tap], 1, 0)
            result = term if result is None else result + term
        conv[i] = result
        pltpu.make_async_copy(conv.at[i], conv_out.at[i], stores.at[1]).start()
        sums[micro] += eighth(result)
        sums[MICRO + micro] += eighth(result * result)

    stream.loop(seqs, up, PUMPS[5])
    mine = reduce_second[0]
    mine[...] = jnp.sum(sums[...], axis=1)
    reduce = AllReduce(place, *reduce_second)
    reduce.start_near()
    stream.pump(PUMPS[6])
    reduce.finish_near()
    reduce.start_far()
    stream.pump(PUMPS[7])
    stats_two = reduce.finish_far()
    totals_two[...] = stats_two
    norm_rows(
        stats_two, (params[3:4, :feats], params[3:4, feats : 2 * feats]), count, scale_two, offset_two, None, None
    )

    def down(i):
        micro = i // per_micro
        hidden = gelu(conv[i] * scale_two[micro] + offset_two[micro]).astype(BF16)
        branch = matmul(hidden, w[TAPS], 1, 1) + proj_bias
        out[i] = (moved[i].astype(F32) + branch).astype(BF16)
        pltpu.make_async_copy(out.at[i], out_out.at[i], stores.at[2]).start()

    stream.loop(seqs, down, PUMPS[8])
    for slot in range(base):
        origin = meta[2, slot]
        for piece in range(per_slot):
            out_stage[slot * per_slot + piece] = out[origin, piece * CHUNK : (piece + 1) * CHUNK]
    for slot in range(base, seqs):
        origin = meta[2, slot]
        for piece in range(per_slot):
            out_extra[(slot - base) * per_slot + piece] = out[origin, piece * CHUNK : (piece + 1) * CHUNK]
    pltpu.make_async_copy(moved, moved_out, stores.at[0]).wait()
    pltpu.make_async_copy(conv, conv_out, stores.at[1]).wait()
    pltpu.make_async_copy(out, out_out, stores.at[2]).wait()
    stream.finish()


def run_front(dims, meta, x, cot, shard, vectors):
    dp_count, bin_count, seqs, rows, chans, feats, base = dims
    per_slot = rows // CHUNK
    chips = bin_count // 2
    group = TAPS + 1
    dma = pltpu.SemaphoreType.DMA
    big = (seqs, rows, chans)
    packed = jax.ShapeDtypeStruct((base * per_slot, CHUNK, chans), BF16)
    spare = jax.ShapeDtypeStruct(((seqs - base) * per_slot, CHUNK, chans), BF16)
    edge = pltpu.VMEM((seqs, EDGE, chans), BF16)
    return pl.pallas_call(
        functools.partial(front_kernel, dims),
        out_shape=(
            jax.ShapeDtypeStruct(big, BF16),
            jax.ShapeDtypeStruct((seqs, rows, feats), F32),
            jax.ShapeDtypeStruct(big, BF16),
            packed,
            spare,
            spare,
            packed,
            jax.ShapeDtypeStruct((group, chans, feats), BF16),
            jax.ShapeDtypeStruct((2 * MICRO, chans), F32),
            jax.ShapeDtypeStruct((8, chans), F32),
            jax.ShapeDtypeStruct((2 * MICRO, feats), F32),
        ),
        in_specs=[smem(), anywhere(), vmem(), anywhere(), vmem()],
        out_specs=(*[anywhere()] * 3, *[vmem()] * 3, anywhere(), anywhere(), *[vmem()] * 3),
        scratch_shapes=[
            pltpu.VMEM(big, BF16),
            edge,
            edge,
            edge,
            edge,
            pltpu.VMEM(big, BF16),
            pltpu.VMEM((seqs, rows, feats), F32),
            pltpu.VMEM(big, BF16),
            pltpu.VMEM((group, chans, feats), BF16),
            pltpu.VMEM((base * per_slot, CHUNK, chans), BF16),
            pltpu.VMEM((2 * MICRO, 8, chans), F32),
            pltpu.VMEM((2 * MICRO, 8, feats), F32),
            pltpu.VMEM((MICRO, 1, chans), F32),
            pltpu.VMEM((MICRO, 1, chans), F32),
            pltpu.VMEM((MICRO, 1, feats), F32),
            pltpu.VMEM((MICRO, 1, feats), F32),
            *AllReduce.scratch(dp_count, bin_count, 2 * MICRO + bin_count, chans),
            *AllReduce.scratch(dp_count, bin_count, 2 * MICRO, feats),
            dma((3,)),
            dma((3,)),
            dma((2,)),
            dma((2,)),
            dma((chips,)),
            dma((chips,)),
            dma((TAPS * chips,)),
            dma((TAPS * chips,)),
            dma((group * chips,)),
            dma((group * chips,)),
            dma((base * per_slot,)),
            dma((base * per_slot,)),
        ],
        compiler_params=pltpu.CompilerParams(
            collective_id=1, has_side_effects=True, vmem_limit_bytes=VMEM_LIMIT
        ),
        name="front",
    )(meta, x, cot, shard, vectors)


def backward_kernel(
    dims, meta, moved, conv, w, stats_one, params_in, totals_two, cot, cot_near, cot_far, out_stage, *rest
):
    dp_count, bin_count, seqs, rows, chans, feats, base = dims
    own_scatter = scatters(dims)
    (grads, low_edge, high_edge, landed_out, sums_two_out, sums_one_out, result) = rest[:7]
    (cots, scale_one, offset_one, inverse_one, shift_one) = rest[7:12]
    (scale_two, offset_two, inverse_two, shift_two) = rest[12:16]
    (grad_two, grad_one, hidden_all, cotangents_unused, conv_grad, hidden_group, window_group) = rest[16:23]
    (sums_two, sums_one, bias_sum, const_two, const_one) = rest[23:28]
    (send_left, send_right, from_left, from_right, last_left, last_right, last_from_left, last_from_right) = rest[28:36]
    reduce_two = rest[36:43]
    reduce_one = rest[43:50]
    (local, halo_sent, halo_landed, last_sent, last_landed, out_sent, out_landed) = rest[50:57]
    partial = result
    if own_scatter:
        (partial, halves, dp_send, dp_got, chip_send, chip_got) = rest[57:63]
        (core_sent, core_landed, dp_sent, dp_landed, chip_sent, chip_landed) = rest[63:69]
    place = Place(dp_count, bin_count)
    per_slot = rows // CHUNK
    per_micro = seqs // MICRO
    loads = [
        pltpu.make_async_copy(cot, cots.at[0:seqs], local.at[0]),
        pltpu.make_async_copy(cot_near, cots.at[seqs : seqs + base], local.at[1]),
        pltpu.make_async_copy(cot_far, cots.at[seqs + base : 2 * seqs], local.at[2]),
    ]
    for load in loads:
        load.start()
    place.barrier()
    stream = Stream(place, out_stage, landed_out, out_sent, out_landed, base * per_slot)
    stream.pump(WINDOW)
    count = float(per_micro * rows * dp_count * bin_count)
    stats = stats_one[...]
    params = params_in[...]
    stats_two = totals_two[...]
    norm_rows(stats, (params[0:1], params[1:2]), count, scale_one, offset_one, inverse_one, shift_one)
    norm_rows(
        stats_two,
        (params[3:4, :feats], params[3:4, feats : 2 * feats]),
        count,
        scale_two,
        offset_two,
        inverse_two,
        shift_two,
    )
    sums_two[...] = jnp.zeros_like(sums_two)
    sums_one[...] = jnp.zeros_like(sums_one)
    bias_sum[...] = jnp.zeros_like(bias_sum)
    partial[...] = jnp.zeros_like(partial)

    def gather(line, term):
        partial[line] += term.reshape(partial.shape[1:])

    for load in loads:
        load.wait()

    def head(i):
        micro = i // per_micro
        cotangent = cots[meta[3, i]]
        bias_sum[...] += eighth(cotangent.astype(F32))
        values = conv[i]
        hidden, slope = gelu_both(values * scale_two[micro] + offset_two[micro])
        hidden_all[i] = hidden.astype(BF16)
        grad = matmul(cotangent, w[TAPS], 1, 0) * slope
        grad_two[i] = grad
        centred = values * inverse_two[micro] + shift_two[micro]
        sums_two[micro] += eighth(grad)
        sums_two[MICRO + micro] += eighth(grad * centred)
        gather(TAPS, matmul(cotangent, hidden_all[i], 0, 0))

    stream.loop(seqs, head, seqs // 2)
    mine = reduce_two[0]
    mine[0 : 2 * MICRO] = jnp.sum(sums_two[...], axis=1)
    bias_row = jnp.sum(bias_sum[...], axis=0, keepdims=True)
    spare = jnp.zeros((1, feats), F32)
    for part in range(2 * MICRO):
        begin = part * feats
        mine[2 * MICRO + part : 2 * MICRO + part + 1] = bias_row[:, begin : begin + feats] if begin < chans else spare
    reduce = AllReduce(place, *reduce_two)
    reduce.start_near()
    stream.pump(1)
    reduce.finish_near()
    reduce.start_far()
    stream.pump(2)
    back_two = reduce.finish_far()
    sums_two_out[...] = back_two
    for micro in range(MICRO):
        const_two[micro] = back_two[micro : micro + 1] / count
        const_two[MICRO + micro] = back_two[MICRO + micro : MICRO + micro + 1] / count

    def middle(i):
        micro = i // per_micro
        reverse = meta[0, i]
        centred = conv[i] * inverse_two[micro] + shift_two[micro]
        value = scale_two[micro] * (grad_two[i] - const_two[micro] - centred * const_two[MICRO + micro])
        value = value.astype(BF16).astype(F32)
        conv_grad[i] = value
        top, bottom = value[:DILATION], value[rows - DILATION :]
        send_left[i] = jnp.where(reverse > 0, bottom, top)
        send_right[i] = jnp.where(reverse > 0, top, bottom)

    lax.fori_loop(0, seqs, lambda i, carry: (middle(i), carry)[1], 0)
    halo = Halo(place, send_left, send_right, from_left, from_right, halo_sent, halo_landed)
    halo.start()
    stream.pump(2)
    halo.finish()

    def tail(i):
        micro = i // per_micro
        inner = lax.rem(i, per_micro)
        reverse = meta[0, i]
        left, right = from_left[i], from_right[i]
        low = jnp.where(reverse > 0, right, left)
        high = jnp.where(reverse > 0, left, right)
        full = jnp.concatenate([low, conv_grad[i], high], axis=0)
        grad = None
        for tap in range(TAPS):
            begin = (TAPS - 1 - tap) * DILATION
            window = full[begin : begin + rows].astype(BF16)
            window_group[tap, pl.ds(pl.multiple_of(inner * rows, rows), rows)] = window
            term = matmul(window, w[tap], 1, 1)
            grad = term if grad is None else grad + term
        values = moved[i].astype(F32)
        hidden, slope = gelu_both(values * scale_one[micro] + offset_one[micro])
        hidden_group[pl.ds(pl.multiple_of(inner * rows, rows), rows)] = hidden.astype(BF16)
        grad = grad * slope
        grad_one[i] = grad
        centred = values * inverse_one[micro] + shift_one[micro]
        sums_one[micro] += eighth(grad)
        sums_one[MICRO + micro] += eighth(grad * centred)

    for micro in range(MICRO):
        stream.loop(per_micro, lambda inner, micro=micro: tail(micro * per_micro + inner), per_micro // 2)
        for tap in range(TAPS):
            gather(tap, matmul(hidden_group[...], window_group[tap], 0, 0))

    mine = reduce_one[0]
    mine[...] = jnp.sum(sums_one[...], axis=1)
    reduce = AllReduce(place, *reduce_one)
    reduce.start_near()
    if own_scatter:
        across = remote(
            partial.at[:, :, :, 1 - place.core],
            halves,
            core_sent.at[0],
            core_landed.at[0],
            (place.dp, place.bin + 1 - 2 * place.core),
        )
        across.start()
    stream.pump(1)
    reduce.finish_near()
    reduce.start_far()
    stream.pump(2)
    if own_scatter:
        across.wait()
        for target in range(dp_count):
            for chip in range(place.chip_count):
                both = partial[:, target, chip, place.core] + halves[:, target, chip]
                halves[:, target, chip] = both
                dp_send[target, chip] = both.reshape(dp_send.shape[2:]).astype(BF16)
        dp_copies = []
        for apart in range(1, dp_count):
            to = lax.rem(place.dp + apart, dp_count)
            dp_copies.append(
                remote(
                    dp_send.at[to],
                    dp_got.at[apart - 1],
                    dp_sent.at[apart - 1],
                    dp_landed.at[apart - 1],
                    (to, place.bin),
                )
            )
            dp_copies[-1].start()
    back_one = reduce.finish_far()
    sums_one_out[...] = back_one
    for micro in range(MICRO):
        const_one[micro] = back_one[micro : micro + 1] / count
        const_one[MICRO + micro] = back_one[MICRO + micro : MICRO + micro + 1] / count

    def end(i):
        micro = i // per_micro
        reverse = meta[0, i]
        centred = moved[i].astype(F32) * inverse_one[micro] + shift_one[micro]
        value = grad_one[i] - const_one[micro] - centred * const_one[MICRO + micro]
        value = cots[meta[3, i]].astype(F32) + scale_one[micro] * value
        grads[i] = value.astype(BF16)
        top, bottom = value[:EDGE].astype(BF16), value[rows - EDGE :].astype(BF16)
        last_left[i] = jnp.where(reverse > 0, bottom, top)
        last_right[i] = jnp.where(reverse > 0, top, bottom)

    stream.loop(seqs, end, seqs // 4)
    last = Halo(place, last_left, last_right, last_from_left, last_from_right, last_sent, last_landed)
    last.start()
    stream.pump(2)
    if own_scatter:
        for copy in dp_copies:
            copy.wait()
        for chip in range(place.chip_count):
            total = halves[:, place.dp, chip].reshape(dp_send.shape[2:])
            for apart in range(1, dp_count):
                total += dp_got[apart - 1, chip].astype(F32)
            chip_send[chip] = total
        chip_copies = []
        for apart in range(1, place.chip_count):
            to = lax.rem(place.chip + apart, place.chip_count)
            chip_copies.append(
                remote(
                    chip_send.at[to],
                    chip_got.at[apart - 1],
                    chip_sent.at[apart - 1],
                    chip_landed.at[apart - 1],
                    (place.dp, to * 2 + place.core),
                )
            )
            chip_copies[-1].start()
    last.finish()
    low_edge[...] = last_from_left[...]
    high_edge[...] = last_from_right[...]
    if own_scatter:
        for copy in chip_copies:
            copy.wait()
        total = chip_send[place.chip]
        for apart in range(1, place.chip_count):
            total += chip_got[apart - 1]
        result[...] = total.reshape(result.shape)
    stream.finish()


def scatters(dims):
    dp_count, bin_count, chans = dims[0], dims[1], dims[4]
    return chans % (dp_count * bin_count * 8) == 0


def run_backward(dims, meta, moved, conv, w, stats_one, params, totals_two, cot, cot_near, cot_far, out_stage):
    dp_count, bin_count, seqs, rows, chans, feats, base = dims
    chips = bin_count // 2
    group = TAPS + 1
    quarter = chans // (dp_count * bin_count)
    own_scatter = scatters(dims)
    per_slot = rows // CHUNK
    per_micro = seqs // MICRO
    dma = pltpu.SemaphoreType.DMA
    wide = pltpu.VMEM((MICRO, 1, chans), F32)
    narrow = pltpu.VMEM((MICRO, 1, feats), F32)
    return pl.pallas_call(
        functools.partial(backward_kernel, dims),
        out_shape=(
            jax.ShapeDtypeStruct((seqs, rows, chans), BF16),
            jax.ShapeDtypeStruct((seqs, EDGE, chans), BF16),
            jax.ShapeDtypeStruct((seqs, EDGE, chans), BF16),
            jax.ShapeDtypeStruct((base * per_slot, CHUNK, chans), BF16),
            jax.ShapeDtypeStruct((4 * MICRO, feats), F32),
            jax.ShapeDtypeStruct((2 * MICRO, chans), F32),
            jax.ShapeDtypeStruct((group, quarter if own_scatter else chans, feats), F32),
        ),
        in_specs=[smem(), *[vmem()] * 6, *[anywhere()] * 4],
        out_specs=(vmem(), vmem(), vmem(), anywhere(), vmem(), vmem(), vmem()),
        scratch_shapes=[
            pltpu.VMEM((2 * seqs, rows, chans), BF16),
            wide,
            wide,
            wide,
            wide,
            narrow,
            narrow,
            narrow,
            narrow,
            pltpu.VMEM((seqs, rows, feats), F32),
            pltpu.VMEM((seqs, rows, chans), F32),
            pltpu.VMEM((seqs, rows, feats), BF16),
            pltpu.VMEM((8, 128), F32),
            pltpu.VMEM((seqs, rows, feats), F32),
            pltpu.VMEM((per_micro * rows, chans), BF16),
            pltpu.VMEM((TAPS, per_micro * rows, feats), BF16),
            pltpu.VMEM((2 * MICRO, 8, feats), F32),
            pltpu.VMEM((2 * MICRO, 8, chans), F32),
            pltpu.VMEM((8, chans), F32),
            pltpu.VMEM((2 * MICRO, 1, feats), F32),
            pltpu.VMEM((2 * MICRO, 1, chans), F32),
            *[pltpu.VMEM((seqs, DILATION, feats), F32)] * 4,
            *[pltpu.VMEM((seqs, EDGE, chans), BF16)] * 4,
            *AllReduce.scratch(dp_count, bin_count, 4 * MICRO, feats),
            *AllReduce.scratch(dp_count, bin_count, 2 * MICRO, chans),
            dma((4,)),
            dma((2,)),
            dma((2,)),
            dma((2,)),
            dma((2,)),
            dma((base * per_slot,)),
            dma((base * per_slot,)),
            *(
                (
                    pltpu.VMEM((group, dp_count, chips, 2, quarter, feats), F32),
                    pltpu.VMEM((group, dp_count, chips, quarter, feats), F32),
                    pltpu.VMEM((dp_count, chips, group * quarter, feats), BF16),
                    pltpu.VMEM((dp_count, chips, group * quarter, feats), BF16),
                    pltpu.VMEM((chips, group * quarter, feats), F32),
                    pltpu.VMEM((chips, group * quarter, feats), F32),
                    dma((1,)),
                    dma((1,)),
                    dma((dp_count,)),
                    dma((dp_count,)),
                    dma((chips,)),
                    dma((chips,)),
                )
                if own_scatter
                else ()
            ),
        ],
        compiler_params=pltpu.CompilerParams(
            collective_id=2, has_side_effects=True, vmem_limit_bytes=VMEM_LIMIT
        ),
        name="backward",
    )(meta, moved, conv, w, stats_one, params, totals_two, cot, cot_near, cot_far, out_stage)


def last_kernel(rows, seqs, base, meta, grad, left, right, out, near, far, result_out, result_grad, held, made, got, put):
    for i in range(seqs):
        reverse, slot = meta[0, i], meta[4, i]

        @pl.when(reverse == 0)
        def _():
            pltpu.make_async_copy(out.at[i], held.at[i], got.at[i]).start()

        @pl.when((reverse > 0) & (slot < base))
        def _():
            pltpu.make_async_copy(near.at[jnp.minimum(slot, base - 1)], held.at[i], got.at[i]).start()

        @pl.when((reverse > 0) & (slot >= base))
        def _():
            pltpu.make_async_copy(far.at[jnp.maximum(slot - base, 0)], held.at[i], got.at[i]).start()

    across = rows + 2 * EDGE
    row = lax.broadcasted_iota(jnp.int32, (rows, across), 0)
    column = lax.broadcasted_iota(jnp.int32, (rows, across), 1)

    def step(i, carry):
        reverse, shift = meta[0, i], meta[1, i]
        low = jnp.where(reverse > 0, right[i], left[i])
        high = jnp.where(reverse > 0, left[i], right[i])
        source = jnp.concatenate([low, grad[i], high], axis=0)
        place = jnp.where(reverse > 0, rows - 1 - row - shift, row + shift) + EDGE
        pick = jnp.where(column == place, 1.0, 0.0).astype(BF16)
        made[i] = matmul(pick, source, 1, 0).astype(BF16)
        pltpu.make_async_copy(made.at[i], result_grad.at[i], put.at[0]).start()
        pltpu.make_async_copy(held.at[i], held.at[i], got.at[i]).wait()
        pltpu.make_async_copy(held.at[i], result_out.at[i], put.at[1]).start()
        return carry

    lax.fori_loop(0, seqs, step, 0)
    pltpu.make_async_copy(made, result_grad, put.at[0]).wait()
    pltpu.make_async_copy(held, result_out, put.at[1]).wait()


def run_last(dims, meta, grad, left, right, out, near, far):
    dp_count, bin_count, seqs, rows, chans, feats, base = dims
    big = (seqs, rows, chans)
    return pl.pallas_call(
        functools.partial(last_kernel, rows, seqs, base),
        out_shape=(jax.ShapeDtypeStruct(big, BF16), jax.ShapeDtypeStruct(big, BF16)),
        in_specs=[smem(), vmem(), vmem(), vmem(), anywhere(), anywhere(), anywhere()],
        out_specs=(anywhere(), anywhere()),
        scratch_shapes=[
            pltpu.VMEM(big, BF16),
            pltpu.VMEM(big, BF16),
            pltpu.SemaphoreType.DMA((seqs,)),
            pltpu.SemaphoreType.DMA((2,)),
        ],
        compiler_params=pltpu.CompilerParams(vmem_limit_bytes=VMEM_LIMIT),
        name="last",
    )(meta, grad, left, right, out, near, far)


def local(
    activations,
    shift_bins,
    reverse_flags,
    gain_one,
    bias_one,
    conv_weight,
    gain_two,
    bias_two,
    proj_weight,
    proj_bias,
    cotangent,
):
    seqs, rows, chans = activations.shape
    feats = conv_weight.shape[2]
    dp_count, bin_count = lax.axis_size("dp"), lax.axis_size("bins")
    dp, bins = lax.axis_index("dp"), lax.axis_index("bins")
    per_slot = rows // CHUNK
    base = BASE_SLOTS
    dims = (dp_count, bin_count, seqs, rows, chans, feats, base)

    reverse = (reverse_flags > 0).astype(jnp.int32)
    index = jnp.arange(seqs, dtype=jnp.int32)
    before = jnp.sum(jnp.where(index[None, :] < index[:, None], reverse[None, :], 0), axis=1)
    slot = jnp.where(reverse > 0, before, 0)
    origin = jnp.sum(
        jnp.where((slot[None, :] == index[:, None]) & (reverse[None, :] > 0), index[None, :], 0), axis=1
    )
    chosen = jnp.where(reverse > 0, seqs + slot, index)
    meta = jnp.stack([reverse, shift_bins, origin, chosen, slot])
    vectors = jnp.concatenate([gain_one, bias_one, proj_bias, gain_two, bias_two]).astype(F32)
    vectors = jnp.pad(vectors, (0, chans - vectors.shape[0]))[None]
    shard = jnp.concatenate([conv_weight, proj_weight.T[None]], axis=0)

    (
        moved,
        conv,
        out,
        out_stage,
        out_extra,
        cot_extra,
        cot_near,
        w,
        stats_one,
        params,
        totals_two,
    ) = run_front(dims, meta, activations, cotangent.reshape(seqs * per_slot, CHUNK, chans), shard, vectors)
    most = jnp.max(params[4, feats : feats + dp_count]).astype(jnp.int32)

    pairs = [(source, bin_count - 1 - source) for source in range(bin_count)]

    def crossing(slots, pair):
        if slots == 0:
            return pair
        held = slots * per_slot
        got = lax.ppermute(jnp.concatenate([item[:held] for item in pair]), "bins", pairs)
        return tuple(
            lax.dynamic_update_slice_in_dim(item, got[k * held : (k + 1) * held], 0, 0)
            for k, item in enumerate(pair)
        )

    extra = lax.switch(
        jnp.clip(most - base, 0, seqs - base),
        [functools.partial(crossing, slots) for slots in range(seqs - base + 1)],
        (cot_extra, out_extra),
    )

    slots_of = lambda item: item.reshape(-1, rows, chans)
    grads, low_edge, high_edge, out_near, back_two, back_one, partial = run_backward(
        dims,
        meta,
        moved,
        conv,
        w,
        stats_one,
        params,
        totals_two,
        cotangent,
        slots_of(cot_near),
        slots_of(extra[0]),
        out_stage,
    )
    output, grad_activations = run_last(
        dims, meta, grads, low_edge, high_edge, out, slots_of(out_near), slots_of(extra[1])
    )

    scattered = partial
    if not scatters(dims):
        scattered = lax.psum_scatter(partial, ("dp", "bins"), scatter_dimension=1, tiled=True)
    wide = chans // (dp_count * bin_count)
    narrow = feats // bin_count
    wide_at = (dp * bin_count + bins) * wide
    narrow_at = bins * narrow
    bias_sum = back_two[2 * MICRO :].reshape(-1)[:chans]
    cut = lax.dynamic_slice_in_dim
    return (
        output,
        grad_activations,
        cut(jnp.sum(back_one[MICRO:], axis=0), wide_at, wide),
        cut(jnp.sum(back_one[:MICRO], axis=0), wide_at, wide),
        scattered[:TAPS],
        cut(jnp.sum(back_two[MICRO : 2 * MICRO], axis=0), narrow_at, narrow),
        cut(jnp.sum(back_two[:MICRO], axis=0), narrow_at, narrow),
        scattered[TAPS].T,
        cut(bias_sum, wide_at, wide),
    )


def solution(mesh):
    placed = (
        P("dp", "bins", None),
        P("dp"),
        P("dp"),
        P("bins"),
        P("bins"),
        P(None, "bins", None),
        P("bins"),
        P("bins"),
        P(None, "bins"),
        P("bins"),
        P("dp", "bins", None),
    )
    return jax.shard_map(
        local,
        mesh=mesh,
        in_specs=placed,
        out_specs=(
            P("dp", "bins", None),
            P("dp", "bins", None),
            P(("dp", "bins")),
            P(("dp", "bins")),
            P(None, ("dp", "bins"), None),
            P("bins"),
            P("bins"),
            P(None, ("dp", "bins")),
            P(("dp", "bins")),
        ),
        check_vma=False,
    )
```

```python
import functools

import jax
import jax.numpy as jnp
from jax import lax
from jax.experimental import pallas as pl
from jax.experimental.pallas import tpu as pltpu
from jax.sharding import PartitionSpec as P

TAPS = 3
DILATION = 8
MICRO = 4
EPSILON = 1e-05
CHUNK = 32
BASE_SLOTS = 8
PUMPS = (0, 4, 6, 4, 1, 1, 5, 5, 1, 1)
BACK_PUMPS = (2, 3, 4, 3, 5, 3, 4, 3, 3)
WINDOW = 3
EDGE = 16
LAST_EDGE = 8
VMEM_LIMIT = 60 * 1024 * 1024
MESH = pl.DeviceIdType.MESH
F32 = jnp.float32
BF16 = jnp.bfloat16
ROOT = 0.7978845608028654
CUBE = 0.044715


def vmem():
    return pl.BlockSpec(memory_space=pltpu.VMEM)


def smem():
    return pl.BlockSpec(memory_space=pltpu.SMEM)


def anywhere():
    return pl.BlockSpec(memory_space=pl.ANY)


def matmul(a, b, ca, cb):
    return lax.dot_general(a, b, (((ca,), (cb,)), ((), ())), preferred_element_type=F32)


class Place:
    def __init__(self, dp_count, bin_count):
        self.dp_count, self.bin_count = dp_count, bin_count
        self.chip_count = bin_count // 2
        self.dp = lax.axis_index("dp")
        self.bin = lax.axis_index("bins")
        self.chip = self.bin // 2
        self.core = lax.rem(self.bin, 2)

    def barrier(self):
        semaphore = pltpu.get_barrier_semaphore()
        for apart in range(1, self.bin_count):
            other = (self.dp, lax.rem(self.bin + apart, self.bin_count))
            pl.semaphore_signal(semaphore, inc=1, device_id=other, device_id_type=MESH)
        for apart in range(1, self.dp_count):
            for core in range(2):
                other = (lax.rem(self.dp + apart, self.dp_count), self.chip * 2 + core)
                pl.semaphore_signal(semaphore, inc=1, device_id=other, device_id_type=MESH)
        pl.semaphore_wait(semaphore, self.bin_count - 1 + 2 * (self.dp_count - 1))


def remote(source, target, sent, landed, device):
    return pltpu.make_async_remote_copy(
        src_ref=source,
        dst_ref=target,
        send_sem=sent,
        recv_sem=landed,
        device_id=device,
        device_id_type=MESH,
    )


class Stream:
    def __init__(self, place, source, target, sent, landed, count):
        self.source, self.target, self.sent, self.landed = source, target, sent, landed
        self.count, self.next = count, 0
        self.device = (place.dp, place.bin_count - 1 - place.bin)

    def piece(self, index):
        return remote(
            self.source.at[index],
            self.target.at[index],
            self.sent.at[index],
            self.landed.at[index],
            self.device,
        )

    def pump(self, pieces=1):
        for _ in range(pieces):
            if self.next >= self.count:
                return
            if self.next >= WINDOW:
                self.piece(self.next - WINDOW).wait_send()
            self.piece(self.next).start()
            self.next += 1

    def loop(self, trips, body, pieces):
        pieces = max(0, min(pieces, self.count - self.next, trips))
        if pieces == 0:
            lax.fori_loop(0, trips, lambda i, carry: (body(i), carry)[1], 0)
            return
        if self.next < WINDOW:
            self.pump(WINDOW - self.next)
            pieces = max(0, min(pieces, self.count - self.next))
        first = self.next
        every = trips // max(pieces, 1)

        def step(i, carry):
            body(i)
            done = lax.div(i, every)

            @pl.when((lax.rem(i, every) == 0) & (done < pieces))
            def _():
                self.piece(first + done - WINDOW).wait_send()
                self.piece(first + done).start()

            return carry

        lax.fori_loop(0, trips, step, 0)
        self.next = first + pieces

    def finish(self):
        self.pump(self.count)
        for index in range(max(0, self.count - WINDOW), self.count):
            self.piece(index).wait_send()
        for index in range(self.count):
            self.piece(index).wait_recv()


class AllReduce:
    def __init__(self, place, mine, near, far, near_sent, near_landed, far_sent, far_landed):
        self.place, self.mine, self.near, self.far = place, mine, near, far
        self.near_count = place.dp_count * 2
        self.me = place.dp * 2 + place.core
        self.near_copies = []
        for apart in range(1, self.near_count):
            to = lax.rem(self.me + apart, self.near_count)
            device = (to // 2, place.chip * 2 + lax.rem(to, 2))
            self.near_copies.append(
                remote(mine, near.at[apart - 1], near_sent.at[apart - 1], near_landed.at[apart - 1], device)
            )
        self.far_copies = []
        for apart in range(1, place.chip_count):
            to = lax.rem(place.chip + apart, place.chip_count)
            device = (place.dp, to * 2 + place.core)
            self.far_copies.append(
                remote(
                    near.at[self.near_count - 1],
                    far.at[apart - 1],
                    far_sent.at[apart - 1],
                    far_landed.at[apart - 1],
                    device,
                )
            )

    def start_near(self):
        for copy in self.near_copies:
            copy.start()

    def finish_near(self):
        for copy in self.near_copies:
            copy.wait()
        count = self.near_count

        total = None
        for member in range(count):
            apart = lax.rem(self.me - member + count, count)
            other = self.near[jnp.maximum(apart - 1, 0)]
            part = jnp.where(apart == 0, self.mine[...], other)
            total = part if total is None else total + part
        self.near[count - 1] = total

    def start_far(self):
        for copy in self.far_copies:
            copy.start()

    def finish_far(self):
        for copy in self.far_copies:
            copy.wait()
        count = self.place.chip_count
        total = None
        for member in range(count):
            apart = lax.rem(self.place.chip - member + count, count)
            part = jnp.where(
                apart == 0, self.near[self.near_count - 1], self.far[jnp.maximum(apart - 1, 0)]
            )
            total = part if total is None else total + part
        return total

    @staticmethod
    def scratch(dp_count, bin_count, rows, width):
        near, far = dp_count * 2, bin_count // 2
        return [
            pltpu.VMEM((rows, width), F32),
            pltpu.VMEM((near, rows, width), F32),
            pltpu.VMEM((far, rows, width), F32),
            pltpu.SemaphoreType.DMA((near,)),
            pltpu.SemaphoreType.DMA((near,)),
            pltpu.SemaphoreType.DMA((far,)),
            pltpu.SemaphoreType.DMA((far,)),
        ]


class Halo:
    def __init__(self, place, to_left, to_right, from_left, from_right, sent, landed):
        self.place, self.from_left, self.from_right = place, from_left, from_right
        count = place.bin_count
        self.right = remote(
            to_right, from_left, sent.at[0], landed.at[0], (place.dp, lax.rem(place.bin + 1, count))
        )
        self.left = remote(
            to_left, from_right, sent.at[1], landed.at[1], (place.dp, lax.rem(place.bin + count - 1, count))
        )
        self.first = place.bin == 0
        self.last = place.bin == count - 1

    def start(self):
        @pl.when(jnp.logical_not(self.last))
        def _():
            self.right.start()

        @pl.when(jnp.logical_not(self.first))
        def _():
            self.left.start()

        @pl.when(self.first)
        def _():
            self.from_left[...] = jnp.zeros_like(self.from_left)

        @pl.when(self.last)
        def _():
            self.from_right[...] = jnp.zeros_like(self.from_right)

    def finish(self):
        @pl.when(jnp.logical_not(self.last))
        def _():
            self.right.wait_send()
            self.left.wait_recv()

        @pl.when(jnp.logical_not(self.first))
        def _():
            self.left.wait_send()
            self.right.wait_recv()


def eighth(values):
    rows, width = values.shape
    return jnp.sum(values.reshape(rows // 8, 8, width), axis=0)


def norm_rows(totals, gains, count, scale_ref, offset_ref, inverse_ref, shift_ref):
    for micro in range(MICRO):
        mean = totals[micro : micro + 1] / count
        second = totals[MICRO + micro : MICRO + micro + 1] / count
        inverse = lax.rsqrt(second - mean * mean + EPSILON)
        scale = inverse * gains[0]
        scale_ref[micro] = scale
        offset_ref[micro] = gains[1] - mean * scale
        if inverse_ref is not None:
            inverse_ref[micro] = inverse
            shift_ref[micro] = -mean * inverse


def gelu(v):
    half = 0.5 * v
    return half + half * jnp.tanh(v * (ROOT + (ROOT * CUBE) * (v * v)))


def gelu_both(v):
    square = v * v
    p = 0.5 + 0.5 * jnp.tanh(v * (ROOT + (ROOT * CUBE) * square))
    value = v * p
    slope = p + value * (1.0 - p) * ((2.0 * ROOT) + (6.0 * ROOT * CUBE) * square)
    return value, slope


def front_kernel(dims, meta, x_in, cot, shard, vectors, *rest):
    dp_count, bin_count, seqs, rows, chans, feats, base = dims
    (moved_out, conv_out, out_out, out_stage, out_extra, cot_extra, landed_cot, weights_out) = rest[:8]
    (stats_out, params_out, totals_two) = rest[8:11]
    (x, x_low, x_high, hidden_all, moved, conv, out, w, stage) = rest[11:20]
    direct = direct_weights(dims)
    weights = w if direct else weights_out
    (sums_one, sums, scale_one, offset_one, scale_two, offset_two) = rest[20:26]
    reduce_first = rest[26:33]
    reduce_second = rest[33:40]
    (local, stores, halo_sent, halo_landed, one_sent, one_landed, two_sent, two_landed, three_sent, three_landed) = rest[40:50]
    cot_sent, cot_landed = rest[50:52]
    place = Place(dp_count, bin_count)
    per_slot = rows // CHUNK
    per_micro = seqs // MICRO
    share = chans // bin_count
    group = TAPS + 1
    total_bins = rows * bin_count
    load = pltpu.make_async_copy(x_in, x, local.at[0])
    load.start()
    tap = lax.rem(place.dp, group)
    home = pl.ds(pl.multiple_of(place.bin * share, 8), share)
    keep = pltpu.make_async_copy(shard.at[tap], weights.at[tap, home], local.at[1])
    keep.start()
    place.barrier()

    halo = Halo(
        place, x_in.at[:, 0:EDGE], x_in.at[:, rows - EDGE : rows], x_low, x_high, halo_sent, halo_landed
    )
    halo.start()

    ones = []
    for apart in range(1, place.chip_count):
        to = lax.rem(place.chip + apart, place.chip_count)
        ones.append(
            remote(
                shard.at[tap],
                weights.at[tap, home],
                one_sent.at[apart - 1],
                one_landed.at[apart - 1],
                (place.dp, to * 2 + place.core),
            )
        )
        ones[-1].start()
    for slot in range(base):
        origin = meta[2, slot] * per_slot
        for piece in range(per_slot):
            stage[slot * per_slot + piece] = cot[origin + piece]
    stream = Stream(place, stage, landed_cot, cot_sent, cot_landed, base * per_slot)
    load.wait()

    sums_one[...] = jnp.zeros_like(sums_one)
    row = lax.broadcasted_iota(jnp.int32, (rows, 1), 0) + place.bin * rows

    def statistics(i):
        micro = i // per_micro
        target = row + meta[1, i]
        inside = jnp.where((target >= 0) & (target < total_bins), 1.0, 0.0).astype(F32)
        values = x[i].astype(F32) * inside
        sums_one[micro] += eighth(values)
        sums_one[MICRO + micro] += eighth(values * values)

    stream.loop(seqs, statistics, PUMPS[0])
    mine = reduce_first[0]
    mine[0 : 2 * MICRO] = jnp.sum(sums_one[...], axis=1)
    mine[2 * MICRO :] = jnp.zeros((bin_count, chans), F32)
    lane = lax.broadcasted_iota(jnp.int32, (1, chans), 1)
    reversed_count = jnp.int32(0)
    for i in range(seqs):
        reversed_count += meta[0, i]
    at_home = jnp.where(place.dp == 0, 1.0, 0.0).astype(F32)
    at_first = jnp.where(place.bin == 0, 1.0, 0.0).astype(F32)
    counts = jnp.where(lane == feats + place.dp, reversed_count.astype(F32) * at_first, 0.0)
    mine[pl.ds(2 * MICRO + place.bin, 1)] = vectors[...] * at_home + counts
    reduce = AllReduce(place, *reduce_first)
    reduce.start_near()
    keep.wait()
    for copy in ones:
        copy.wait()
    twos = []
    for apart in range(1, group):
        to = (place.dp // group) * group + lax.rem(tap + apart, group)
        for chip in range(place.chip_count):
            part = weights.at[tap, pl.ds(pl.multiple_of((chip * 2 + place.core) * share, 8), share)]
            index = (apart - 1) * place.chip_count + chip
            twos.append(remote(part, part, two_sent.at[index], two_landed.at[index], (to, place.bin)))
            twos[-1].start()
    stream.pump(PUMPS[1])
    for slot in range(base, seqs):
        origin = meta[2, slot] * per_slot
        for piece in range(per_slot):
            cot_extra[(slot - base) * per_slot + piece] = cot[origin + piece]
    reduce.finish_near()
    reduce.start_far()
    stream.pump(PUMPS[2])
    first = reduce.finish_far()
    stats_out[...] = first[: 2 * MICRO]
    params_out[...] = jnp.zeros_like(params_out)
    begin = 0
    for index, (line, offset, width) in enumerate(
        ((0, 0, share), (1, 0, share), (2, 0, share), (3, 0, share // 2), (3, feats, share // 2))
    ):
        for member in range(bin_count):
            left = offset + member * width
            params_out[line : line + 1, left : left + width] = first[
                2 * MICRO + member : 2 * MICRO + member + 1, begin : begin + width
            ]
        begin += width
    params_out[4:5] = first[2 * MICRO : 2 * MICRO + 1]
    count = float(per_micro * rows * dp_count * bin_count)
    params = params_out[...]
    norm_rows(first, (params[0:1], params[1:2]), count, scale_one, offset_one, None, None)
    proj_bias = params[2:3]
    sums[...] = jnp.zeros_like(sums)
    halo.finish()
    stream.pump(PUMPS[3])

    long_rows = rows + 2 * DILATION
    across = rows + 2 * EDGE
    local_row = lax.broadcasted_iota(jnp.int32, (long_rows, across), 0) - DILATION
    column = lax.broadcasted_iota(jnp.int32, (long_rows, across), 1)
    edge_row = lax.broadcasted_iota(jnp.int32, (DILATION, 1), 0)

    def up(i):
        micro = i // per_micro
        reverse, shift = meta[0, i], meta[1, i]
        direction = 1 - 2 * reverse
        begin = reverse * (rows - 1)
        pick = jnp.where(column == local_row * direction + (begin - shift + EDGE), 1.0, 0.0).astype(BF16)
        source = jnp.concatenate([x_low[i], x[i], x_high[i]], axis=0)
        shifted = matmul(pick, source, 1, 0)
        moved[i] = shifted[DILATION : DILATION + rows].astype(BF16)
        pltpu.make_async_copy(moved.at[i], moved_out.at[i], stores.at[0]).start()
        hidden = gelu(shifted * scale_one[micro] + offset_one[micro])
        parts = []
        for top, first_row in ((0, -DILATION), (DILATION + rows, rows)):
            where = place.bin * rows + begin + (edge_row + first_row) * direction
            parts.append(jnp.where((where >= 0) & (where < total_bins), hidden[top : top + DILATION], 0.0))
        hidden = jnp.concatenate([parts[0], hidden[DILATION : DILATION + rows], parts[1]], axis=0)
        hidden_all[i] = hidden.astype(BF16)

    half_way = seqs // 2
    stream.loop(half_way, up, PUMPS[4])
    for copy in twos:
        copy.wait()
    threes = []
    for line in range(group):
        for chip in range(place.chip_count):
            part = weights.at[line, pl.ds(pl.multiple_of((chip * 2 + place.core) * share, 8), share)]
            index = line * place.chip_count + chip
            threes.append(
                remote(
                    part,
                    part,
                    three_sent.at[index],
                    three_landed.at[index],
                    (place.dp, place.bin + 1 - 2 * place.core),
                )
            )
            threes[-1].start()
    stream.loop(half_way, lambda i: up(i + half_way), PUMPS[5])
    for copy in threes:
        copy.wait()
    if direct:
        pltpu.make_async_copy(w, weights_out, local.at[2]).start()
    else:
        pltpu.make_async_copy(weights_out, w, local.at[2]).start()
        pltpu.make_async_copy(weights_out, w, local.at[2]).wait()

    def across_taps(i):
        micro = i // per_micro
        hidden = hidden_all[i]
        result = None
        for tap in range(TAPS):
            term = matmul(hidden, w[tap], 1, 0)[tap * DILATION : tap * DILATION + rows]
            result = term if result is None else result + term
        conv[i] = result
        pltpu.make_async_copy(conv.at[i], conv_out.at[i], stores.at[1]).start()
        sums[micro] += eighth(result)
        sums[MICRO + micro] += eighth(result * result)

    stream.loop(seqs, across_taps, PUMPS[9])
    mine = reduce_second[0]
    mine[...] = jnp.sum(sums[...], axis=1)
    reduce = AllReduce(place, *reduce_second)
    reduce.start_near()
    stream.pump(PUMPS[6])
    reduce.finish_near()
    reduce.start_far()
    stream.pump(PUMPS[7])
    stats_two = reduce.finish_far()
    totals_two[...] = stats_two
    norm_rows(
        stats_two, (params[3:4, :feats], params[3:4, feats : 2 * feats]), count, scale_two, offset_two, None, None
    )

    def down(i):
        micro = i // per_micro
        hidden = gelu(conv[i] * scale_two[micro] + offset_two[micro]).astype(BF16)
        branch = matmul(hidden, w[TAPS], 1, 1) + proj_bias
        out[i] = (moved[i].astype(F32) + branch).astype(BF16)
        pltpu.make_async_copy(out.at[i], out_out.at[i], stores.at[2]).start()

    stream.loop(seqs, down, PUMPS[8])
    for slot in range(base):
        origin = meta[2, slot]
        for piece in range(per_slot):
            out_stage[slot * per_slot + piece] = out[origin, piece * CHUNK : (piece + 1) * CHUNK]
    for slot in range(base, seqs):
        origin = meta[2, slot]
        for piece in range(per_slot):
            out_extra[(slot - base) * per_slot + piece] = out[origin, piece * CHUNK : (piece + 1) * CHUNK]
    if direct:
        pltpu.make_async_copy(w, weights_out, local.at[2]).wait()
    pltpu.make_async_copy(moved, moved_out, stores.at[0]).wait()
    pltpu.make_async_copy(conv, conv_out, stores.at[1]).wait()
    pltpu.make_async_copy(out, out_out, stores.at[2]).wait()
    stream.finish()


def direct_weights(dims):
    return dims[4] // dims[1] % 16 == 0


def run_front(dims, meta, x, cot, shard, vectors):
    dp_count, bin_count, seqs, rows, chans, feats, base = dims
    per_slot = rows // CHUNK
    chips = bin_count // 2
    group = TAPS + 1
    dma = pltpu.SemaphoreType.DMA
    big = (seqs, rows, chans)
    packed = jax.ShapeDtypeStruct((base * per_slot, CHUNK, chans), BF16)
    spare = jax.ShapeDtypeStruct(((seqs - base) * per_slot, CHUNK, chans), BF16)
    edge = pltpu.VMEM((seqs, EDGE, chans), BF16)
    return pl.pallas_call(
        functools.partial(front_kernel, dims),
        out_shape=(
            jax.ShapeDtypeStruct(big, BF16),
            jax.ShapeDtypeStruct((seqs, rows, feats), F32),
            jax.ShapeDtypeStruct(big, BF16),
            packed,
            spare,
            spare,
            packed,
            jax.ShapeDtypeStruct((group, chans, feats), BF16),
            jax.ShapeDtypeStruct((2 * MICRO, chans), F32),
            jax.ShapeDtypeStruct((8, chans), F32),
            jax.ShapeDtypeStruct((2 * MICRO, feats), F32),
        ),
        in_specs=[smem(), anywhere(), vmem(), anywhere(), vmem()],
        out_specs=(*[anywhere()] * 3, *[vmem()] * 3, anywhere(), anywhere(), *[vmem()] * 3),
        scratch_shapes=[
            pltpu.VMEM(big, BF16),
            edge,
            edge,
            pltpu.VMEM((seqs, rows + 2 * DILATION, chans), BF16),
            pltpu.VMEM(big, BF16),
            pltpu.VMEM((seqs, rows, feats), F32),
            pltpu.VMEM(big, BF16),
            pltpu.VMEM((group, chans, feats), BF16),
            pltpu.VMEM((base * per_slot, CHUNK, chans), BF16),
            pltpu.VMEM((2 * MICRO, 8, chans), F32),
            pltpu.VMEM((2 * MICRO, 8, feats), F32),
            pltpu.VMEM((MICRO, 1, chans), F32),
            pltpu.VMEM((MICRO, 1, chans), F32),
            pltpu.VMEM((MICRO, 1, feats), F32),
            pltpu.VMEM((MICRO, 1, feats), F32),
            *AllReduce.scratch(dp_count, bin_count, 2 * MICRO + bin_count, chans),
            *AllReduce.scratch(dp_count, bin_count, 2 * MICRO, feats),
            dma((3,)),
            dma((3,)),
            dma((2,)),
            dma((2,)),
            dma((chips,)),
            dma((chips,)),
            dma((TAPS * chips,)),
            dma((TAPS * chips,)),
            dma((group * chips,)),
            dma((group * chips,)),
            dma((base * per_slot,)),
            dma((base * per_slot,)),
        ],
        compiler_params=pltpu.CompilerParams(
            collective_id=1, has_side_effects=True, vmem_limit_bytes=VMEM_LIMIT
        ),
        name="front",
    )(meta, x, cot, shard, vectors)


class Scatter:
    def __init__(self, place, first, lines, partial, result, halves, dp_send, dp_got, chip_send, chip_got, *semaphores):
        self.place, self.lines = place, pl.ds(first, lines)
        self.partial, self.result, self.halves = partial, result, halves
        self.dp_send, self.dp_got, self.chip_send, self.chip_got = dp_send, dp_got, chip_send, chip_got
        core_sent, core_landed, dp_sent, dp_landed, chip_sent, chip_landed = semaphores
        self.core = remote(
            partial.at[self.lines, :, :, 1 - place.core],
            halves,
            core_sent.at[0],
            core_landed.at[0],
            (place.dp, place.bin + 1 - 2 * place.core),
        )
        self.dp_copies, self.chip_copies = [], []
        for apart in range(1, place.dp_count):
            to = lax.rem(place.dp + apart, place.dp_count)
            self.dp_copies.append(
                remote(
                    dp_send.at[to],
                    dp_got.at[apart - 1],
                    dp_sent.at[apart - 1],
                    dp_landed.at[apart - 1],
                    (to, place.bin),
                )
            )
        for apart in range(1, place.chip_count):
            to = lax.rem(place.chip + apart, place.chip_count)
            self.chip_copies.append(
                remote(
                    chip_send.at[to],
                    chip_got.at[apart - 1],
                    chip_sent.at[apart - 1],
                    chip_landed.at[apart - 1],
                    (place.dp, to * 2 + place.core),
                )
            )

    def start_core(self):
        self.core.start()

    def core_to_dp(self):
        self.core.wait()
        for target in range(self.place.dp_count):
            for chip in range(self.place.chip_count):
                both = self.partial[self.lines, target, chip, self.place.core] + self.halves[:, target, chip]
                self.halves[:, target, chip] = both
                self.dp_send[target, chip] = both.reshape(self.dp_send.shape[2:]).astype(BF16)
        for copy in self.dp_copies:
            copy.start()

    def dp_to_chip(self):
        for copy in self.dp_copies:
            copy.wait()
        for chip in range(self.place.chip_count):
            total = self.halves[:, self.place.dp, chip].reshape(self.dp_send.shape[2:])
            for apart in range(1, self.place.dp_count):
                total += self.dp_got[apart - 1, chip].astype(F32)
            self.halves[:, 0, chip] = total.reshape(self.halves[:, 0, chip].shape)
            self.chip_send[chip] = total.astype(BF16)
        for copy in self.chip_copies:
            copy.start()

    def finish(self):
        for copy in self.chip_copies:
            copy.wait()
        total = self.halves[:, 0, self.place.chip]
        for apart in range(1, self.place.chip_count):
            total += self.chip_got[apart - 1].astype(F32).reshape(total.shape)
        self.result[self.lines] = total

    @staticmethod
    def scratch(dims, lines):
        dp_count, bin_count, seqs, rows, chans, feats, base = dims
        chips, dma = bin_count // 2, pltpu.SemaphoreType.DMA
        quarter = chans // (dp_count * bin_count)
        return [
            pltpu.VMEM((lines, dp_count, chips, quarter, feats), F32),
            pltpu.VMEM((dp_count, chips, lines * quarter, feats), BF16),
            pltpu.VMEM((dp_count, chips, lines * quarter, feats), BF16),
            pltpu.VMEM((chips, lines * quarter, feats), BF16),
            pltpu.VMEM((chips, lines * quarter, feats), BF16),
            dma((1,)),
            dma((1,)),
            dma((dp_count,)),
            dma((dp_count,)),
            dma((chips,)),
            dma((chips,)),
        ]


def scatters(dims):
    dp_count, bin_count, chans = dims[0], dims[1], dims[4]
    return chans % (dp_count * bin_count * 8) == 0


def backward_kernel(
    dims, meta, moved_in, conv_in, w_in, stats_one, params_in, totals_two, cot, cot_near, cot_far, out_stage, *rest
):
    dp_count, bin_count, seqs, rows, chans, feats, base = dims
    own_scatter = scatters(dims)
    (grads, low_edge, high_edge, landed_out, sums_two_out, sums_one_out, result) = rest[:7]
    (cots, moved, conv, w, chosen) = rest[7:12]
    (scale_one, offset_one, inverse_one, shift_one, scale_two, offset_two, inverse_two, shift_two) = rest[12:20]
    (grad_two, grad_one, hidden_two, hidden_one, windows) = rest[20:25]
    (sums_two, sums_one, bias_sum, line_two, rest_two, line_one, rest_one) = rest[25:32]
    (send_left, send_right, from_left, from_right, last_left, last_right, last_from_left, last_from_right) = rest[32:40]
    reduce_two = rest[40:47]
    reduce_one = rest[47:54]
    (local, halo_sent, halo_landed, last_sent, last_landed, out_sent, out_landed) = rest[54:61]
    partial = result
    place = Place(dp_count, bin_count)
    per_slot = rows // CHUNK
    per_micro = seqs // MICRO
    loads = [
        pltpu.make_async_copy(conv_in, conv, local.at[0]),
        pltpu.make_async_copy(w_in, w, local.at[1]),
        pltpu.make_async_copy(cot, cots.at[0:seqs], local.at[2]),
        pltpu.make_async_copy(cot_near, cots.at[seqs : seqs + base], local.at[3]),
        pltpu.make_async_copy(cot_far, cots.at[seqs + base : 2 * seqs], local.at[4]),
        pltpu.make_async_copy(moved_in, moved, local.at[5]),
    ]
    for load in loads:
        load.start()
    if own_scatter:
        partial = rest[61]
        proj_scatter = Scatter(place, TAPS, 1, partial, result, *rest[62:73])
        conv_scatter = Scatter(place, 0, TAPS, partial, result, *rest[73:84])
    place.barrier()
    stream = Stream(place, out_stage, landed_out, out_sent, out_landed, base * per_slot)
    stream.pump(WINDOW)
    count = float(per_micro * rows * dp_count * bin_count)
    params = params_in[...]
    norm_rows(stats_one[...], (params[0:1], params[1:2]), count, scale_one, offset_one, inverse_one, shift_one)
    norm_rows(
        totals_two[...],
        (params[3:4, :feats], params[3:4, feats : 2 * feats]),
        count,
        scale_two,
        offset_two,
        inverse_two,
        shift_two,
    )
    sums_two[...] = jnp.zeros_like(sums_two)
    sums_one[...] = jnp.zeros_like(sums_one)
    bias_sum[...] = jnp.zeros_like(bias_sum)
    for load in loads[:5]:
        load.wait()

    def head(i):
        micro = i // per_micro
        inner = pl.ds(pl.multiple_of(lax.rem(i, per_micro) * rows, rows), rows)
        cotangent = cots[meta[3, i]]
        chosen[micro, inner] = cotangent
        bias_sum[...] += eighth(cotangent.astype(F32))
        values = conv[i]
        hidden, slope = gelu_both(values * scale_two[micro] + offset_two[micro])
        hidden_two[micro, inner] = hidden.astype(BF16)
        grad = matmul(cotangent, w[TAPS], 1, 0) * slope
        grad_two[i] = grad
        sums_two[micro] += eighth(grad)
        sums_two[MICRO + micro] += eighth(grad * values)

    stream.loop(seqs, head, BACK_PUMPS[0])
    mine = reduce_two[0]
    mine[0 : 2 * MICRO] = jnp.sum(sums_two[...], axis=1)
    bias_row = jnp.sum(bias_sum[...], axis=0, keepdims=True)
    spare = jnp.zeros((1, feats), F32)
    for part in range(2 * MICRO):
        begin = part * feats
        mine[2 * MICRO + part : 2 * MICRO + part + 1] = bias_row[:, begin : begin + feats] if begin < chans else spare
    reduce = AllReduce(place, *reduce_two)
    reduce.start_near()
    stream.pump(BACK_PUMPS[1])

    def weigh(line, terms):
        total = None
        for left, right in terms:
            term = matmul(left, right, 0, 0)
            total = term if total is None else total + term
        partial[line] = total.reshape(partial.shape[1:])

    def proj_terms(micros):
        return [(chosen[micro], hidden_two[micro]) for micro in micros]

    reduce.finish_near()
    reduce.start_far()
    weigh(TAPS, proj_terms(range(MICRO)))
    if own_scatter:
        proj_scatter.start_core()
    stream.pump(BACK_PUMPS[2])
    back_two = reduce.finish_far()

    def lines(back, scale, inverse, shift, line, remainder, out):
        for micro in range(MICRO):
            plain = back[micro : micro + 1]
            centred = inverse[micro] * back[MICRO + micro : MICRO + micro + 1] + shift[micro] * plain
            out[micro : micro + 1] = plain
            out[MICRO + micro : MICRO + micro + 1] = centred
            line[micro] = -scale[micro] * inverse[micro] * (centred / count)
            remainder[micro] = -scale[micro] * (plain / count + shift[micro] * (centred / count))

    lines(back_two, scale_two, inverse_two, shift_two, line_two, rest_two, sums_two_out)
    sums_two_out[2 * MICRO :] = back_two[2 * MICRO :]

    def conv_gradient(i, begin, size):
        micro = i // per_micro
        span = slice(begin, begin + size)
        value = scale_two[micro] * grad_two[i, span] + line_two[micro] * conv[i, span] + rest_two[micro]
        return value.astype(BF16).astype(F32)

    def edges(i):
        reverse = meta[0, i]
        top, bottom = conv_gradient(i, 0, DILATION), conv_gradient(i, rows - DILATION, DILATION)
        send_left[i] = jnp.where(reverse > 0, bottom, top)
        send_right[i] = jnp.where(reverse > 0, top, bottom)

    lax.fori_loop(0, seqs, lambda i, carry: (edges(i), carry)[1], 0)
    halo = Halo(place, send_left, send_right, from_left, from_right, halo_sent, halo_landed)
    halo.start()
    if own_scatter:
        proj_scatter.core_to_dp()
    stream.pump(BACK_PUMPS[3])
    loads[5].wait()
    halo.finish()

    def tail(i):
        micro = i // per_micro
        inner = pl.ds(pl.multiple_of(lax.rem(i, per_micro) * rows, rows), rows)
        reverse = meta[0, i]
        left, right = from_left[i], from_right[i]
        low = jnp.where(reverse > 0, right, left)
        high = jnp.where(reverse > 0, left, right)
        full = jnp.concatenate([low, conv_gradient(i, 0, rows), high], axis=0)
        grad = None
        for tap in range(TAPS):
            begin = (TAPS - 1 - tap) * DILATION
            window = full[begin : begin + rows].astype(BF16)
            windows[micro, inner, tap * feats : (tap + 1) * feats] = window
            term = matmul(window, w[tap], 1, 1)
            grad = term if grad is None else grad + term
        values = moved[i].astype(F32)
        hidden, slope = gelu_both(values * scale_one[micro] + offset_one[micro])
        hidden_one[micro, inner] = hidden.astype(BF16)
        grad = grad * slope
        grad_one[i] = grad
        sums_one[micro] += eighth(grad)
        sums_one[MICRO + micro] += eighth(grad * values)

    stream.loop(seqs, tail, BACK_PUMPS[4])
    mine = reduce_one[0]
    mine[...] = jnp.sum(sums_one[...], axis=1)
    reduce = AllReduce(place, *reduce_one)
    reduce.start_near()
    if own_scatter:
        proj_scatter.dp_to_chip()
    stream.pump(BACK_PUMPS[5])

    def conv_weigh(micros, add):
        total = None
        for micro in micros:
            term = matmul(hidden_one[micro], windows[micro], 0, 0)
            total = term if total is None else total + term
        for tap in range(TAPS):
            part = total[:, tap * feats : (tap + 1) * feats].reshape(partial.shape[1:])
            partial[tap] = partial[tap] + part if add else part

    conv_weigh(range(MICRO // 2), False)
    reduce.finish_near()
    reduce.start_far()
    conv_weigh(range(MICRO // 2, MICRO), True)
    if own_scatter:
        conv_scatter.start_core()
    stream.pump(BACK_PUMPS[6])
    back_one = reduce.finish_far()
    lines(back_one, scale_one, inverse_one, shift_one, line_one, rest_one, sums_one_out)
    if own_scatter:
        conv_scatter.core_to_dp()
        proj_scatter.finish()

    def end(i):
        micro = i // per_micro
        inner = pl.ds(pl.multiple_of(lax.rem(i, per_micro) * rows, rows), rows)
        reverse = meta[0, i]
        value = scale_one[micro] * grad_one[i] + line_one[micro] * moved[i].astype(F32) + rest_one[micro]
        value = chosen[micro, inner].astype(F32) + value
        grads[i] = value.astype(BF16)
        top, bottom = value[:LAST_EDGE].astype(BF16), value[rows - LAST_EDGE :].astype(BF16)
        last_left[i] = jnp.where(reverse > 0, bottom, top)
        last_right[i] = jnp.where(reverse > 0, top, bottom)

    stream.loop(seqs, end, BACK_PUMPS[7])
    last = Halo(place, last_left, last_right, last_from_left, last_from_right, last_sent, last_landed)
    last.start()
    stream.pump(BACK_PUMPS[8])
    if own_scatter:
        conv_scatter.dp_to_chip()
    last.finish()
    low_edge[...] = last_from_left[...]
    high_edge[...] = last_from_right[...]
    if own_scatter:
        conv_scatter.finish()
    stream.finish()


def run_backward(dims, meta, moved, conv, w, stats_one, params, totals_two, cot, cot_near, cot_far, out_stage):
    dp_count, bin_count, seqs, rows, chans, feats, base = dims
    chips = bin_count // 2
    group = TAPS + 1
    quarter = chans // (dp_count * bin_count)
    own_scatter = scatters(dims)
    per_slot = rows // CHUNK
    held = seqs // MICRO * rows
    dma = pltpu.SemaphoreType.DMA
    wide = pltpu.VMEM((MICRO, 1, chans), F32)
    narrow = pltpu.VMEM((MICRO, 1, feats), F32)
    edge = jax.ShapeDtypeStruct((seqs, LAST_EDGE, chans), BF16)
    return pl.pallas_call(
        functools.partial(backward_kernel, dims),
        out_shape=(
            jax.ShapeDtypeStruct((seqs, rows, chans), BF16),
            edge,
            edge,
            jax.ShapeDtypeStruct((base * per_slot, CHUNK, chans), BF16),
            jax.ShapeDtypeStruct((4 * MICRO, feats), F32),
            jax.ShapeDtypeStruct((2 * MICRO, chans), F32),
            jax.ShapeDtypeStruct((group, quarter if own_scatter else chans, feats), F32),
        ),
        in_specs=[smem(), *[anywhere()] * 3, *[vmem()] * 3, *[anywhere()] * 4],
        out_specs=(vmem(), vmem(), vmem(), anywhere(), vmem(), vmem(), vmem()),
        scratch_shapes=[
            pltpu.VMEM((2 * seqs, rows, chans), BF16),
            pltpu.VMEM((seqs, rows, chans), BF16),
            pltpu.VMEM((seqs, rows, feats), F32),
            pltpu.VMEM((group, chans, feats), BF16),
            pltpu.VMEM((MICRO, held, chans), BF16),
            *[wide] * 4,
            *[narrow] * 4,
            pltpu.VMEM((seqs, rows, feats), F32),
            pltpu.VMEM((seqs, rows, chans), F32),
            pltpu.VMEM((MICRO, held, feats), BF16),
            pltpu.VMEM((MICRO, held, chans), BF16),
            pltpu.VMEM((MICRO, held, TAPS * feats), BF16),
            pltpu.VMEM((2 * MICRO, 8, feats), F32),
            pltpu.VMEM((2 * MICRO, 8, chans), F32),
            pltpu.VMEM((8, chans), F32),
            narrow,
            narrow,
            wide,
            wide,
            *[pltpu.VMEM((seqs, DILATION, feats), F32)] * 4,
            *[pltpu.VMEM((seqs, LAST_EDGE, chans), BF16)] * 4,
            *AllReduce.scratch(dp_count, bin_count, 4 * MICRO, feats),
            *AllReduce.scratch(dp_count, bin_count, 2 * MICRO, chans),
            dma((6,)),
            dma((2,)),
            dma((2,)),
            dma((2,)),
            dma((2,)),
            dma((base * per_slot,)),
            dma((base * per_slot,)),
            *(
                (
                    pltpu.VMEM((group, dp_count, chips, 2, quarter, feats), F32),
                    *Scatter.scratch(dims, 1),
                    *Scatter.scratch(dims, TAPS),
                )
                if own_scatter
                else ()
            ),
        ],
        compiler_params=pltpu.CompilerParams(
            collective_id=2, has_side_effects=True, vmem_limit_bytes=VMEM_LIMIT
        ),
        name="backward",
    )(meta, moved, conv, w, stats_one, params, totals_two, cot, cot_near, cot_far, out_stage)


def last_kernel(rows, seqs, base, meta, grad, left, right, out, near, far, result_out, result_grad, held, made, got, put):
    for i in range(seqs):
        reverse, slot = meta[0, i], meta[4, i]

        @pl.when(reverse == 0)
        def _():
            pltpu.make_async_copy(out.at[i], held.at[i], got.at[i]).start()

        @pl.when((reverse > 0) & (slot < base))
        def _():
            pltpu.make_async_copy(near.at[jnp.minimum(slot, base - 1)], held.at[i], got.at[i]).start()

        @pl.when((reverse > 0) & (slot >= base))
        def _():
            pltpu.make_async_copy(far.at[jnp.maximum(slot - base, 0)], held.at[i], got.at[i]).start()

    across = rows + 2 * LAST_EDGE
    row = lax.broadcasted_iota(jnp.int32, (rows, across), 0)
    column = lax.broadcasted_iota(jnp.int32, (rows, across), 1)

    def step(i, carry):
        reverse, shift = meta[0, i], meta[1, i]
        low = jnp.where(reverse > 0, right[i], left[i])
        high = jnp.where(reverse > 0, left[i], right[i])
        source = jnp.concatenate([low, grad[i], high], axis=0)
        place = jnp.where(reverse > 0, rows - 1 - row - shift, row + shift) + LAST_EDGE
        pick = jnp.where(column == place, 1.0, 0.0).astype(BF16)
        made[i] = matmul(pick, source, 1, 0).astype(BF16)
        pltpu.make_async_copy(made.at[i], result_grad.at[i], put.at[0]).start()
        pltpu.make_async_copy(held.at[i], held.at[i], got.at[i]).wait()
        pltpu.make_async_copy(held.at[i], result_out.at[i], put.at[1]).start()
        return carry

    lax.fori_loop(0, seqs, step, 0)
    pltpu.make_async_copy(made, result_grad, put.at[0]).wait()
    pltpu.make_async_copy(held, result_out, put.at[1]).wait()


def run_last(dims, meta, grad, left, right, out, near, far):
    dp_count, bin_count, seqs, rows, chans, feats, base = dims
    big = (seqs, rows, chans)
    return pl.pallas_call(
        functools.partial(last_kernel, rows, seqs, base),
        out_shape=(jax.ShapeDtypeStruct(big, BF16), jax.ShapeDtypeStruct(big, BF16)),
        in_specs=[smem(), vmem(), vmem(), vmem(), anywhere(), anywhere(), anywhere()],
        out_specs=(anywhere(), anywhere()),
        scratch_shapes=[
            pltpu.VMEM(big, BF16),
            pltpu.VMEM(big, BF16),
            pltpu.SemaphoreType.DMA((seqs,)),
            pltpu.SemaphoreType.DMA((2,)),
        ],
        compiler_params=pltpu.CompilerParams(vmem_limit_bytes=VMEM_LIMIT),
        name="last",
    )(meta, grad, left, right, out, near, far)


def local(
    activations,
    shift_bins,
    reverse_flags,
    gain_one,
    bias_one,
    conv_weight,
    gain_two,
    bias_two,
    proj_weight,
    proj_bias,
    cotangent,
):
    seqs, rows, chans = activations.shape
    feats = conv_weight.shape[2]
    dp_count, bin_count = lax.axis_size("dp"), lax.axis_size("bins")
    dp, bins = lax.axis_index("dp"), lax.axis_index("bins")
    per_slot = rows // CHUNK
    base = BASE_SLOTS
    dims = (dp_count, bin_count, seqs, rows, chans, feats, base)

    reverse = (reverse_flags > 0).astype(jnp.int32)
    index = jnp.arange(seqs, dtype=jnp.int32)
    before = jnp.sum(jnp.where(index[None, :] < index[:, None], reverse[None, :], 0), axis=1)
    slot = jnp.where(reverse > 0, before, 0)
    origin = jnp.sum(
        jnp.where((slot[None, :] == index[:, None]) & (reverse[None, :] > 0), index[None, :], 0), axis=1
    )
    chosen = jnp.where(reverse > 0, seqs + slot, index)
    meta = jnp.stack([reverse, shift_bins, origin, chosen, slot])
    vectors = jnp.concatenate([gain_one, bias_one, proj_bias, gain_two, bias_two]).astype(F32)
    vectors = jnp.pad(vectors, (0, chans - vectors.shape[0]))[None]
    shard = jnp.concatenate([conv_weight, proj_weight.T[None]], axis=0)

    (
        moved,
        conv,
        out,
        out_stage,
        out_extra,
        cot_extra,
        cot_near,
        w,
        stats_one,
        params,
        totals_two,
    ) = run_front(dims, meta, activations, cotangent.reshape(seqs * per_slot, CHUNK, chans), shard, vectors)
    most = jnp.max(params[4, feats : feats + dp_count]).astype(jnp.int32)

    pairs = [(source, bin_count - 1 - source) for source in range(bin_count)]

    def crossing(slots, pair):
        if slots == 0:
            return pair
        held = slots * per_slot
        got = lax.ppermute(jnp.concatenate([item[:held] for item in pair]), "bins", pairs)
        return tuple(
            lax.dynamic_update_slice_in_dim(item, got[k * held : (k + 1) * held], 0, 0)
            for k, item in enumerate(pair)
        )

    extra = lax.switch(
        jnp.clip(most - base, 0, seqs - base),
        [functools.partial(crossing, slots) for slots in range(seqs - base + 1)],
        (cot_extra, out_extra),
    )

    slots_of = lambda item: item.reshape(-1, rows, chans)
    grads, low_edge, high_edge, out_near, back_two, back_one, partial = run_backward(
        dims,
        meta,
        moved,
        conv,
        w,
        stats_one,
        params,
        totals_two,
        cotangent,
        slots_of(cot_near),
        slots_of(extra[0]),
        out_stage,
    )
    output, grad_activations = run_last(
        dims, meta, grads, low_edge, high_edge, out, slots_of(out_near), slots_of(extra[1])
    )

    scattered = partial
    if not scatters(dims):
        scattered = lax.psum_scatter(partial, ("dp", "bins"), scatter_dimension=1, tiled=True)
    wide = chans // (dp_count * bin_count)
    narrow = feats // bin_count
    wide_at = (dp * bin_count + bins) * wide
    narrow_at = bins * narrow
    bias_sum = back_two[2 * MICRO :].reshape(-1)[:chans]
    cut = lax.dynamic_slice_in_dim
    return (
        output,
        grad_activations,
        cut(jnp.sum(back_one[MICRO:], axis=0), wide_at, wide),
        cut(jnp.sum(back_one[:MICRO], axis=0), wide_at, wide),
        scattered[:TAPS],
        cut(jnp.sum(back_two[MICRO : 2 * MICRO], axis=0), narrow_at, narrow),
        cut(jnp.sum(back_two[:MICRO], axis=0), narrow_at, narrow),
        scattered[TAPS].T,
        cut(bias_sum, wide_at, wide),
    )


def solution(mesh):
    placed = (
        P("dp", "bins", None),
        P("dp"),
        P("dp"),
        P("bins"),
        P("bins"),
        P(None, "bins", None),
        P("bins"),
        P("bins"),
        P(None, "bins"),
        P("bins"),
        P("dp", "bins", None),
    )
    return jax.shard_map(
        local,
        mesh=mesh,
        in_specs=placed,
        out_specs=(
            P("dp", "bins", None),
            P("dp", "bins", None),
            P(("dp", "bins")),
            P(("dp", "bins")),
            P(None, ("dp", "bins"), None),
            P("bins"),
            P("bins"),
            P(None, ("dp", "bins")),
            P(("dp", "bins")),
        ),
        check_vma=False,
    )
```

```python
import functools

import jax
import jax.numpy as jnp
from jax import lax
from jax.experimental import pallas as pl
from jax.experimental.pallas import tpu as pltpu
from jax.sharding import PartitionSpec as P

TAPS = 3
DILATION = 8
MICRO = 4
EPSILON = 1e-05
CHUNK = 32
BASE_SLOTS = 8
RELAY_SLOTS = 4
PUMPS = (0, 4, 6, 4, 1, 1, 5, 5, 1, 1)
BACK_PUMPS = (2, 3, 4, 3, 5, 3, 4, 3, 3, 1)
WINDOW = 3
EDGE = 16
LAST_EDGE = 8
VMEM_LIMIT = 60 * 1024 * 1024
MESH = pl.DeviceIdType.MESH
F32 = jnp.float32
BF16 = jnp.bfloat16
ROOT = 0.7978845608028654
CUBE = 0.044715


def vmem():
    return pl.BlockSpec(memory_space=pltpu.VMEM)


def smem():
    return pl.BlockSpec(memory_space=pltpu.SMEM)


def anywhere():
    return pl.BlockSpec(memory_space=pl.ANY)


def matmul(a, b, ca, cb):
    return lax.dot_general(a, b, (((ca,), (cb,)), ((), ())), preferred_element_type=F32)


class Place:
    def __init__(self, dp_count, bin_count):
        self.dp_count, self.bin_count = dp_count, bin_count
        self.chip_count = bin_count // 2
        self.dp = lax.axis_index("dp")
        self.bin = lax.axis_index("bins")
        self.chip = self.bin // 2
        self.core = lax.rem(self.bin, 2)

    def barrier(self):
        semaphore = pltpu.get_barrier_semaphore()
        for apart in range(1, self.bin_count):
            other = (self.dp, lax.rem(self.bin + apart, self.bin_count))
            pl.semaphore_signal(semaphore, inc=1, device_id=other, device_id_type=MESH)
        for apart in range(1, self.dp_count):
            for core in range(2):
                other = (lax.rem(self.dp + apart, self.dp_count), self.chip * 2 + core)
                pl.semaphore_signal(semaphore, inc=1, device_id=other, device_id_type=MESH)
        pl.semaphore_wait(semaphore, self.bin_count - 1 + 2 * (self.dp_count - 1))


def remote(source, target, sent, landed, device):
    return pltpu.make_async_remote_copy(
        src_ref=source,
        dst_ref=target,
        send_sem=sent,
        recv_sem=landed,
        device_id=device,
        device_id_type=MESH,
    )


class Stream:
    def __init__(self, place, source, target, sent, landed, count):
        self.source, self.target, self.sent, self.landed = source, target, sent, landed
        self.count, self.next = count, 0
        self.device = (place.dp, place.bin_count - 1 - place.bin)

    def piece(self, index):
        return remote(
            self.source.at[index],
            self.target.at[index],
            self.sent.at[index],
            self.landed.at[index],
            self.device,
        )

    def pump(self, pieces=1):
        for _ in range(pieces):
            if self.next >= self.count:
                return
            if self.next >= WINDOW:
                self.piece(self.next - WINDOW).wait_send()
            self.piece(self.next).start()
            self.next += 1

    def loop(self, trips, body, pieces):
        pieces = max(0, min(pieces, self.count - self.next, trips))
        if pieces == 0:
            lax.fori_loop(0, trips, lambda i, carry: (body(i), carry)[1], 0)
            return
        if self.next < WINDOW:
            self.pump(WINDOW - self.next)
            pieces = max(0, min(pieces, self.count - self.next))
        first = self.next
        every = trips // max(pieces, 1)

        def step(i, carry):
            body(i)
            done = lax.div(i, every)

            @pl.when((lax.rem(i, every) == 0) & (done < pieces))
            def _():
                self.piece(first + done - WINDOW).wait_send()
                self.piece(first + done).start()

            return carry

        lax.fori_loop(0, trips, step, 0)
        self.next = first + pieces

    def finish(self):
        self.pump(self.count)
        for index in range(max(0, self.count - WINDOW), self.count):
            self.piece(index).wait_send()
        for index in range(self.count):
            self.piece(index).wait_recv()


class AllReduce:
    def __init__(self, place, mine, near, far, near_sent, near_landed, far_sent, far_landed):
        self.place, self.mine, self.near, self.far = place, mine, near, far
        self.near_count = place.dp_count * 2
        self.me = place.dp * 2 + place.core
        self.near_copies = []
        for apart in range(1, self.near_count):
            to = lax.rem(self.me + apart, self.near_count)
            device = (to // 2, place.chip * 2 + lax.rem(to, 2))
            self.near_copies.append(
                remote(mine, near.at[apart - 1], near_sent.at[apart - 1], near_landed.at[apart - 1], device)
            )
        self.far_copies = []
        for apart in range(1, place.chip_count):
            to = lax.rem(place.chip + apart, place.chip_count)
            device = (place.dp, to * 2 + place.core)
            self.far_copies.append(
                remote(
                    near.at[self.near_count - 1],
                    far.at[apart - 1],
                    far_sent.at[apart - 1],
                    far_landed.at[apart - 1],
                    device,
                )
            )

    def start_near(self):
        for copy in self.near_copies:
            copy.start()

    def finish_near(self):
        for copy in self.near_copies:
            copy.wait()
        count = self.near_count

        total = None
        for member in range(count):
            apart = lax.rem(self.me - member + count, count)
            other = self.near[jnp.maximum(apart - 1, 0)]
            part = jnp.where(apart == 0, self.mine[...], other)
            total = part if total is None else total + part
        self.near[count - 1] = total

    def start_far(self):
        for copy in self.far_copies:
            copy.start()

    def finish_far(self):
        for copy in self.far_copies:
            copy.wait()
        count = self.place.chip_count
        total = None
        for member in range(count):
            apart = lax.rem(self.place.chip - member + count, count)
            part = jnp.where(
                apart == 0, self.near[self.near_count - 1], self.far[jnp.maximum(apart - 1, 0)]
            )
            total = part if total is None else total + part
        return total

    @staticmethod
    def scratch(dp_count, bin_count, rows, width):
        near, far = dp_count * 2, bin_count // 2
        return [
            pltpu.VMEM((rows, width), F32),
            pltpu.VMEM((near, rows, width), F32),
            pltpu.VMEM((far, rows, width), F32),
            pltpu.SemaphoreType.DMA((near,)),
            pltpu.SemaphoreType.DMA((near,)),
            pltpu.SemaphoreType.DMA((far,)),
            pltpu.SemaphoreType.DMA((far,)),
        ]


class Halo:
    def __init__(self, place, to_left, to_right, from_left, from_right, sent, landed):
        self.place, self.from_left, self.from_right = place, from_left, from_right
        count = place.bin_count
        self.right = remote(
            to_right, from_left, sent.at[0], landed.at[0], (place.dp, lax.rem(place.bin + 1, count))
        )
        self.left = remote(
            to_left, from_right, sent.at[1], landed.at[1], (place.dp, lax.rem(place.bin + count - 1, count))
        )
        self.first = place.bin == 0
        self.last = place.bin == count - 1

    def start(self):
        @pl.when(jnp.logical_not(self.last))
        def _():
            self.right.start()

        @pl.when(jnp.logical_not(self.first))
        def _():
            self.left.start()

        @pl.when(self.first)
        def _():
            self.from_left[...] = jnp.zeros_like(self.from_left)

        @pl.when(self.last)
        def _():
            self.from_right[...] = jnp.zeros_like(self.from_right)

    def finish(self):
        @pl.when(jnp.logical_not(self.last))
        def _():
            self.right.wait_send()
            self.left.wait_recv()

        @pl.when(jnp.logical_not(self.first))
        def _():
            self.left.wait_send()
            self.right.wait_recv()


def eighth(values):
    rows, width = values.shape
    return jnp.sum(values.reshape(rows // 8, 8, width), axis=0)


def norm_rows(totals, gains, count, scale_ref, offset_ref, inverse_ref, shift_ref):
    for micro in range(MICRO):
        mean = totals[micro : micro + 1] / count
        second = totals[MICRO + micro : MICRO + micro + 1] / count
        inverse = lax.rsqrt(second - mean * mean + EPSILON)
        scale = inverse * gains[0]
        scale_ref[micro] = scale
        offset_ref[micro] = gains[1] - mean * scale
        if inverse_ref is not None:
            inverse_ref[micro] = inverse
            shift_ref[micro] = -mean * inverse


def gelu(v):
    half = 0.5 * v
    return half + half * jnp.tanh(v * (ROOT + (ROOT * CUBE) * (v * v)))


def gelu_both(v):
    square = v * v
    p = 0.5 + 0.5 * jnp.tanh(v * (ROOT + (ROOT * CUBE) * square))
    value = v * p
    slope = p + value * (1.0 - p) * ((2.0 * ROOT) + (6.0 * ROOT * CUBE) * square)
    return value, slope


def to_columns(place, source, target, own, sent, landed):
    copies = []
    for apart in range(1, place.dp_count):
        to = lax.rem(place.dp + apart, place.dp_count)
        copies.append(
            remote(
                source.at[to], target(place.dp), sent.at[apart - 1], landed.at[apart - 1], (to, place.bin)
            )
        )
        copies[-1].start()
    copies.append(pltpu.make_async_copy(source.at[place.dp], target(place.dp), own))
    copies[-1].start()
    return copies


def front_kernel(dims, flags, shifts, x_in, cot, shard, *rest):
    dp_count, bin_count, seqs, rows, chans, feats, base, relay = dims
    vectors, rest = rest[:5], rest[5:]
    (moved_out, conv_out, out_out, out_stage, out_extra, cot_extra, landed_cot, weights_out) = rest[:8]
    (stats_out, params_out, totals_two) = rest[8:11]
    meta, rest = rest[11], rest[:11] + rest[12:]
    if relay:
        relay_cot, relay_out = rest[11:13]
        rest = rest[:11] + rest[13:]
    (x, x_low, x_high, hidden_all, moved, conv, out, w, stage) = rest[11:20]
    direct = direct_weights(dims)
    weights = w if direct else weights_out
    (sums_one, sums, scale_one, offset_one, scale_two, offset_two) = rest[20:26]
    reduce_first = rest[26:33]
    reduce_second = rest[33:40]
    (local, stores, halo_sent, halo_landed, one_sent, one_landed, two_sent, two_landed, three_sent, three_landed) = rest[40:50]
    cot_sent, cot_landed = rest[50:52]
    place = Place(dp_count, bin_count)
    per_slot = rows // CHUNK
    per_micro = seqs // MICRO
    if relay:
        (over_cot, over_out, relay_own) = rest[52:55]
        (relay_cot_sent, relay_cot_landed, relay_out_sent, relay_out_landed) = rest[55:59]
    share = chans // bin_count
    group = TAPS + 1
    total_bins = rows * bin_count
    load = pltpu.make_async_copy(x_in, x, local.at[0])
    load.start()
    tap = lax.rem(place.dp, group)
    home = pl.ds(pl.multiple_of(place.bin * share, 8), share)
    keep = pltpu.make_async_copy(shard.at[tap], weights.at[tap, home], local.at[1])
    keep.start()
    reversed_count = jnp.int32(0)
    origins = [jnp.int32(0)] * seqs
    for i in range(seqs):
        reverse = jnp.where(flags[i] > 0, 1, 0)
        meta[0, i] = reverse
        meta[1, i] = shifts[i]
        for slot in range(i + 1):
            origins[slot] = jnp.where((reverse > 0) & (reversed_count == slot), i, origins[slot])
        slot = reverse * reversed_count
        meta[3, i] = jnp.where(reverse > 0, seqs + slot, i)
        meta[4, i] = slot
        reversed_count += reverse
    for slot in range(seqs):
        meta[2, slot] = origins[slot]
    place.barrier()

    halo = Halo(
        place, x_in.at[:, 0:EDGE], x_in.at[:, rows - EDGE : rows], x_low, x_high, halo_sent, halo_landed
    )
    halo.start()

    ones = []
    for apart in range(1, place.chip_count):
        to = lax.rem(place.chip + apart, place.chip_count)
        ones.append(
            remote(
                shard.at[tap],
                weights.at[tap, home],
                one_sent.at[apart - 1],
                one_landed.at[apart - 1],
                (place.dp, to * 2 + place.core),
            )
        )
        ones[-1].start()
    for slot in range(base):
        origin = meta[2, slot] * per_slot
        for piece in range(per_slot):
            stage[slot * per_slot + piece] = cot[origin + piece]
    stream = Stream(place, stage, landed_cot, cot_sent, cot_landed, base * per_slot)
    load.wait()

    sums_one[...] = jnp.zeros_like(sums_one)
    row = lax.broadcasted_iota(jnp.int32, (rows, 1), 0) + place.bin * rows

    def statistics(i):
        micro = i // per_micro
        target = row + meta[1, i]
        inside = jnp.where((target >= 0) & (target < total_bins), 1.0, 0.0).astype(F32)
        values = x[i].astype(F32) * inside
        sums_one[micro] += eighth(values)
        sums_one[MICRO + micro] += eighth(values * values)

    stream.loop(seqs, statistics, PUMPS[0])
    mine = reduce_first[0]
    mine[0 : 2 * MICRO] = jnp.sum(sums_one[...], axis=1)
    mine[2 * MICRO :] = jnp.zeros((bin_count, chans), F32)
    lane = lax.broadcasted_iota(jnp.int32, (1, chans), 1)
    at_home = jnp.where(place.dp == 0, 1.0, 0.0).astype(F32)
    at_first = jnp.where(place.bin == 0, 1.0, 0.0).astype(F32)
    counts = jnp.where(lane == feats + place.dp, reversed_count.astype(F32) * at_first, 0.0)
    pieces = [vector[...].astype(F32) for vector in vectors]
    wide = sum(piece.shape[1] for piece in pieces)
    if wide < chans:
        pieces.append(jnp.zeros((1, chans - wide), F32))
    mine[pl.ds(2 * MICRO + place.bin, 1)] = jnp.concatenate(pieces, axis=1) * at_home + counts
    reduce = AllReduce(place, *reduce_first)
    reduce.start_near()
    keep.wait()
    for copy in ones:
        copy.wait()
    twos = []
    for apart in range(1, group):
        to = (place.dp // group) * group + lax.rem(tap + apart, group)
        for chip in range(place.chip_count):
            part = weights.at[tap, pl.ds(pl.multiple_of((chip * 2 + place.core) * share, 8), share)]
            index = (apart - 1) * place.chip_count + chip
            twos.append(remote(part, part, two_sent.at[index], two_landed.at[index], (to, place.bin)))
            twos[-1].start()
    stream.pump(PUMPS[1])
    for slot in range(base, seqs):
        origin = meta[2, slot] * per_slot
        for piece in range(per_slot):
            if slot < base + relay:
                over_cot[piece, slot - base] = cot[origin + piece]
            else:
                cot_extra[(slot - base - relay) * per_slot + piece] = cot[origin + piece]
    reduce.finish_near()
    reduce.start_far()
    relays = []
    if relay:
        relays += to_columns(
            place, over_cot, lambda own: relay_cot.at[own], relay_own.at[0], relay_cot_sent, relay_cot_landed
        )
    stream.pump(PUMPS[2])
    first = reduce.finish_far()
    stats_out[...] = first[: 2 * MICRO]
    params_out[...] = jnp.zeros_like(params_out)
    begin = 0
    for index, (line, offset, width) in enumerate(
        ((0, 0, share), (1, 0, share), (2, 0, share), (3, 0, share // 2), (3, feats, share // 2))
    ):
        for member in range(bin_count):
            left = offset + member * width
            params_out[line : line + 1, left : left + width] = first[
                2 * MICRO + member : 2 * MICRO + member + 1, begin : begin + width
            ]
        begin += width
    params_out[4:5] = first[2 * MICRO : 2 * MICRO + 1]
    count = float(per_micro * rows * dp_count * bin_count)
    params = params_out[...]
    norm_rows(first, (params[0:1], params[1:2]), count, scale_one, offset_one, None, None)
    proj_bias = params[2:3]
    sums[...] = jnp.zeros_like(sums)
    halo.finish()
    stream.pump(PUMPS[3])

    long_rows = rows + 2 * DILATION
    across = rows + 2 * EDGE
    local_row = lax.broadcasted_iota(jnp.int32, (long_rows, across), 0) - DILATION
    column = lax.broadcasted_iota(jnp.int32, (long_rows, across), 1)
    edge_row = lax.broadcasted_iota(jnp.int32, (DILATION, 1), 0)

    def up(i):
        micro = i // per_micro
        reverse, shift = meta[0, i], meta[1, i]
        direction = 1 - 2 * reverse
        begin = reverse * (rows - 1)
        pick = jnp.where(column == local_row * direction + (begin - shift + EDGE), 1.0, 0.0).astype(BF16)
        source = jnp.concatenate([x_low[i], x[i], x_high[i]], axis=0)
        shifted = matmul(pick, source, 1, 0)
        moved[i] = shifted[DILATION : DILATION + rows].astype(BF16)
        pltpu.make_async_copy(moved.at[i], moved_out.at[i], stores.at[0]).start()
        hidden = gelu(shifted * scale_one[micro] + offset_one[micro])
        parts = []
        for top, first_row in ((0, -DILATION), (DILATION + rows, rows)):
            where = place.bin * rows + begin + (edge_row + first_row) * direction
            parts.append(jnp.where((where >= 0) & (where < total_bins), hidden[top : top + DILATION], 0.0))
        hidden = jnp.concatenate([parts[0], hidden[DILATION : DILATION + rows], parts[1]], axis=0)
        hidden_all[i] = hidden.astype(BF16)

    half_way = seqs // 2
    stream.loop(half_way, up, PUMPS[4])
    for copy in twos:
        copy.wait()
    threes = []
    for line in range(group):
        for chip in range(place.chip_count):
            part = weights.at[line, pl.ds(pl.multiple_of((chip * 2 + place.core) * share, 8), share)]
            index = line * place.chip_count + chip
            threes.append(
                remote(
                    part,
                    part,
                    three_sent.at[index],
                    three_landed.at[index],
                    (place.dp, place.bin + 1 - 2 * place.core),
                )
            )
            threes[-1].start()
    stream.loop(half_way, lambda i: up(i + half_way), PUMPS[5])
    for copy in threes:
        copy.wait()
    if direct:
        pltpu.make_async_copy(w, weights_out, local.at[2]).start()
    else:
        pltpu.make_async_copy(weights_out, w, local.at[2]).start()
        pltpu.make_async_copy(weights_out, w, local.at[2]).wait()

    def across_taps(i):
        micro = i // per_micro
        hidden = hidden_all[i]
        result = None
        for tap in range(TAPS):
            term = matmul(hidden, w[tap], 1, 0)[tap * DILATION : tap * DILATION + rows]
            result = term if result is None else result + term
        conv[i] = result
        pltpu.make_async_copy(conv.at[i], conv_out.at[i], stores.at[1]).start()
        sums[micro] += eighth(result)
        sums[MICRO + micro] += eighth(result * result)

    stream.loop(seqs, across_taps, PUMPS[9])
    mine = reduce_second[0]
    mine[...] = jnp.sum(sums[...], axis=1)
    reduce = AllReduce(place, *reduce_second)
    reduce.start_near()
    stream.pump(PUMPS[6])
    reduce.finish_near()
    reduce.start_far()
    stream.pump(PUMPS[7])
    stats_two = reduce.finish_far()
    totals_two[...] = stats_two
    norm_rows(
        stats_two, (params[3:4, :feats], params[3:4, feats : 2 * feats]), count, scale_two, offset_two, None, None
    )

    def down(i):
        micro = i // per_micro
        hidden = gelu(conv[i] * scale_two[micro] + offset_two[micro]).astype(BF16)
        branch = matmul(hidden, w[TAPS], 1, 1) + proj_bias
        out[i] = (moved[i].astype(F32) + branch).astype(BF16)
        pltpu.make_async_copy(out.at[i], out_out.at[i], stores.at[2]).start()

    stream.loop(seqs - base, lambda i: down(i + base), 0)
    if relay:
        for slot in range(base, base + relay):
            for piece in range(per_slot):
                over_out[piece, slot - base] = out[meta[2, slot], piece * CHUNK : (piece + 1) * CHUNK]
        relays += to_columns(
            place, over_out, lambda own: relay_out.at[own], relay_own.at[1], relay_out_sent, relay_out_landed
        )
    stream.loop(base, down, PUMPS[8])
    for slot in (*range(base), *range(base + relay, seqs)):
        origin = meta[2, slot]
        for piece in range(per_slot):
            part = out[origin, piece * CHUNK : (piece + 1) * CHUNK]
            if slot < base:
                out_stage[slot * per_slot + piece] = part
            else:
                out_extra[(slot - base - relay) * per_slot + piece] = part
    if direct:
        pltpu.make_async_copy(w, weights_out, local.at[2]).wait()
    pltpu.make_async_copy(moved, moved_out, stores.at[0]).wait()
    pltpu.make_async_copy(conv, conv_out, stores.at[1]).wait()
    pltpu.make_async_copy(out, out_out, stores.at[2]).wait()
    for copy in relays:
        copy.wait()
    stream.finish()


def direct_weights(dims):
    return dims[4] // dims[1] % 16 == 0


def run_front(dims, flags, shifts, x, cot, shard, vectors):
    dp_count, bin_count, seqs, rows, chans, feats, base, relay = dims
    per_slot = rows // CHUNK
    chips = bin_count // 2
    group = TAPS + 1
    dma = pltpu.SemaphoreType.DMA
    big = (seqs, rows, chans)
    packed = jax.ShapeDtypeStruct((base * per_slot, CHUNK, chans), BF16)
    spare = jax.ShapeDtypeStruct(((seqs - base - relay) * per_slot, CHUNK, chans), BF16)
    columns = (dp_count, relay, CHUNK, chans)
    edge = pltpu.VMEM((seqs, EDGE, chans), BF16)
    return pl.pallas_call(
        functools.partial(front_kernel, dims),
        out_shape=(
            jax.ShapeDtypeStruct(big, BF16),
            jax.ShapeDtypeStruct((seqs, rows, feats), F32),
            jax.ShapeDtypeStruct(big, BF16),
            packed,
            spare,
            spare,
            packed,
            jax.ShapeDtypeStruct((group, chans, feats), BF16),
            jax.ShapeDtypeStruct((2 * MICRO, chans), F32),
            jax.ShapeDtypeStruct((8, chans), F32),
            jax.ShapeDtypeStruct((2 * MICRO, feats), F32),
            jax.ShapeDtypeStruct((5, seqs), jnp.int32),
            *([jax.ShapeDtypeStruct(columns, BF16)] * 2 if relay else ()),
        ),
        in_specs=[smem(), smem(), anywhere(), vmem(), anywhere(), *[vmem()] * 5],
        out_specs=(
            *[anywhere()] * 3,
            *[vmem()] * 3,
            anywhere(),
            anywhere(),
            *[vmem()] * 3,
            smem(),
            *([anywhere()] * 2 if relay else ()),
        ),
        scratch_shapes=[
            pltpu.VMEM(big, BF16),
            edge,
            edge,
            pltpu.VMEM((seqs, rows + 2 * DILATION, chans), BF16),
            pltpu.VMEM(big, BF16),
            pltpu.VMEM((seqs, rows, feats), F32),
            pltpu.VMEM(big, BF16),
            pltpu.VMEM((group, chans, feats), BF16),
            pltpu.VMEM((base * per_slot, CHUNK, chans), BF16),
            pltpu.VMEM((2 * MICRO, 8, chans), F32),
            pltpu.VMEM((2 * MICRO, 8, feats), F32),
            pltpu.VMEM((MICRO, 1, chans), F32),
            pltpu.VMEM((MICRO, 1, chans), F32),
            pltpu.VMEM((MICRO, 1, feats), F32),
            pltpu.VMEM((MICRO, 1, feats), F32),
            *AllReduce.scratch(dp_count, bin_count, 2 * MICRO + bin_count, chans),
            *AllReduce.scratch(dp_count, bin_count, 2 * MICRO, feats),
            dma((3,)),
            dma((3,)),
            dma((2,)),
            dma((2,)),
            dma((chips,)),
            dma((chips,)),
            dma((TAPS * chips,)),
            dma((TAPS * chips,)),
            dma((group * chips,)),
            dma((group * chips,)),
            dma((base * per_slot,)),
            dma((base * per_slot,)),
            *([pltpu.VMEM(columns, BF16)] * 2 + [dma((2,))] + [dma((dp_count,))] * 4 if relay else ()),
        ],
        compiler_params=pltpu.CompilerParams(
            collective_id=1, has_side_effects=True, vmem_limit_bytes=VMEM_LIMIT
        ),
        name="front",
    )(flags, shifts, x, cot, shard, *vectors)


def starts(counts, dims):
    base, relay = dims[6:8]
    begin, found = jnp.int32(0), []
    for column in range(dims[0]):
        held = jnp.clip(counts[column] - base, 0, relay)
        found.append((begin, held))
        begin = begin + held
    return found


def choose(dims, counts, choice):
    dp_count, seqs, base, relay = dims[0], dims[2], dims[6], dims[7]
    total, most = jnp.int32(0), jnp.int32(0)
    for column in range(dp_count):
        total = total + jnp.clip(counts[column] - base, 0, relay)
        most = jnp.maximum(most, counts[column])
    every = dp_count * relay
    beyond = jnp.maximum(most - base - relay - 1, 0) * 2 + jnp.where(total > every // 2, 1, 0)
    choice[0] = jnp.where(most > base + relay, every + 1 + beyond, total)


def compact_kernel(dims, params, *rest):
    dp_count, feats, relay = dims[0], dims[5], dims[7]
    (cot, out), rest = rest[: 2 * (relay > 0)] or (None, None), rest[2 * (relay > 0) :]
    counts, choice = rest[:2]
    for column in range(dp_count):
        counts[column] = params[4, feats + column].astype(jnp.int32)
    choose(dims, counts, choice)
    if not relay:
        return
    packed, ready = rest[2:]
    for wait in (False, True):
        for column, (begin, held) in enumerate(starts(counts, dims)):
            for slot in range(relay):

                @pl.when(slot < held)
                def _():
                    for side, source in enumerate((cot, out)):
                        copy = pltpu.make_async_copy(
                            source.at[column, slot],
                            packed.at[2 * jnp.minimum(begin + slot, dp_count * relay - 1) + side],
                            ready.at[(side * dp_count + column) * relay + slot],
                        )
                        copy.wait() if wait else copy.start()


def run_compact(dims, params, *relays):
    dp_count, chans, relay = dims[0], dims[4], dims[7]
    pieces = 2 * dp_count * relay
    return pl.pallas_call(
        functools.partial(compact_kernel, dims),
        out_shape=(
            jax.ShapeDtypeStruct((dp_count,), jnp.int32),
            jax.ShapeDtypeStruct((1,), jnp.int32),
            *([jax.ShapeDtypeStruct((pieces, CHUNK, chans), BF16)] if relay else ()),
        ),
        in_specs=[smem(), *[anywhere()] * len(relays)],
        out_specs=(smem(), smem(), *([vmem()] if relay else ())),
        scratch_shapes=[pltpu.SemaphoreType.DMA((pieces,))] if relay else [],
        name="compact",
    )(params, *relays)


class Scatter:
    def __init__(self, place, first, lines, partial, result, halves, dp_send, dp_got, chip_send, chip_got, *semaphores):
        self.place, self.lines = place, pl.ds(first, lines)
        self.partial, self.result, self.halves = partial, result, halves
        self.dp_send, self.dp_got, self.chip_send, self.chip_got = dp_send, dp_got, chip_send, chip_got
        core_sent, core_landed, dp_sent, dp_landed, chip_sent, chip_landed = semaphores
        self.core = remote(
            partial.at[self.lines, :, :, 1 - place.core],
            halves,
            core_sent.at[0],
            core_landed.at[0],
            (place.dp, place.bin + 1 - 2 * place.core),
        )
        self.dp_copies, self.chip_copies = [], []
        for apart in range(1, place.dp_count):
            to = lax.rem(place.dp + apart, place.dp_count)
            self.dp_copies.append(
                remote(
                    dp_send.at[to],
                    dp_got.at[apart - 1],
                    dp_sent.at[apart - 1],
                    dp_landed.at[apart - 1],
                    (to, place.bin),
                )
            )
        for apart in range(1, place.chip_count):
            to = lax.rem(place.chip + apart, place.chip_count)
            self.chip_copies.append(
                remote(
                    chip_send.at[to],
                    chip_got.at[apart - 1],
                    chip_sent.at[apart - 1],
                    chip_landed.at[apart - 1],
                    (place.dp, to * 2 + place.core),
                )
            )

    def start_core(self):
        self.core.start()

    def core_to_dp(self):
        self.core.wait()
        for target in range(self.place.dp_count):
            for chip in range(self.place.chip_count):
                both = self.partial[self.lines, target, chip, self.place.core] + self.halves[:, target, chip]
                self.halves[:, target, chip] = both
                self.dp_send[target, chip] = both.reshape(self.dp_send.shape[2:]).astype(BF16)
        for copy in self.dp_copies:
            copy.start()

    def dp_to_chip(self):
        for copy in self.dp_copies:
            copy.wait()
        for chip in range(self.place.chip_count):
            total = self.halves[:, self.place.dp, chip].reshape(self.dp_send.shape[2:])
            for apart in range(1, self.place.dp_count):
                total += self.dp_got[apart - 1, chip].astype(F32)
            self.halves[:, 0, chip] = total.reshape(self.halves[:, 0, chip].shape)
            self.chip_send[chip] = total.astype(BF16)
        for copy in self.chip_copies:
            copy.start()

    def finish(self):
        for copy in self.chip_copies:
            copy.wait()
        total = self.halves[:, 0, self.place.chip]
        for apart in range(1, self.place.chip_count):
            total += self.chip_got[apart - 1].astype(F32).reshape(total.shape)
        self.result[self.lines] = total

    @staticmethod
    def scratch(dims, lines):
        dp_count, bin_count, seqs, rows, chans, feats, base, relay = dims
        chips, dma = bin_count // 2, pltpu.SemaphoreType.DMA
        quarter = chans // (dp_count * bin_count)
        return [
            pltpu.VMEM((lines, dp_count, chips, quarter, feats), F32),
            pltpu.VMEM((dp_count, chips, lines * quarter, feats), BF16),
            pltpu.VMEM((dp_count, chips, lines * quarter, feats), BF16),
            pltpu.VMEM((chips, lines * quarter, feats), BF16),
            pltpu.VMEM((chips, lines * quarter, feats), BF16),
            dma((1,)),
            dma((1,)),
            dma((dp_count,)),
            dma((dp_count,)),
            dma((chips,)),
            dma((chips,)),
        ]


def scatters(dims):
    dp_count, bin_count, chans = dims[0], dims[1], dims[4]
    return chans % (dp_count * bin_count * 8) == 0


def backward_kernel(
    dims, meta, counts, crossed, moved_in, conv_in, w_in, stats_one, params_in, totals_two, cot, cot_near, cot_far, out_stage, *rest
):
    dp_count, bin_count, seqs, rows, chans, feats, base, relay = dims
    own_scatter = scatters(dims)
    (grads, low_edge, high_edge, landed_out, sums_two_out, sums_one_out, result) = rest[:7]
    if relay:
        landed_relay = rest[7]
        (relayed, home_cot, home_out, relay_own) = rest[-8:-4]
        (relay_cot_sent, relay_cot_landed, relay_out_sent, relay_out_landed) = rest[-4:]
        rest = rest[:7] + rest[8:-8]
    (cots, moved, conv, w, chosen) = rest[7:12]
    (scale_one, offset_one, inverse_one, shift_one, scale_two, offset_two, inverse_two, shift_two) = rest[12:20]
    (grad_two, grad_one, hidden_two, hidden_one, windows) = rest[20:25]
    (sums_two, sums_one, bias_sum, line_two, rest_two, line_one, rest_one) = rest[25:32]
    (send_left, send_right, from_left, from_right, last_left, last_right, last_from_left, last_from_right) = rest[32:40]
    reduce_two = rest[40:47]
    reduce_one = rest[47:54]
    (local, halo_sent, halo_landed, last_sent, last_landed, out_sent, out_landed) = rest[54:61]
    partial = result
    place = Place(dp_count, bin_count)
    per_slot = rows // CHUNK
    per_micro = seqs // MICRO
    loads = [
        pltpu.make_async_copy(conv_in, conv, local.at[0]),
        pltpu.make_async_copy(w_in, w, local.at[1]),
        pltpu.make_async_copy(cot, cots.at[0:seqs], local.at[2]),
        pltpu.make_async_copy(cot_near, cots.at[seqs : seqs + base], local.at[3]),
        pltpu.make_async_copy(cot_far, cots.at[seqs + base + relay : 2 * seqs], local.at[4]),
        pltpu.make_async_copy(moved_in, moved, local.at[5]),
    ]
    for load in loads:
        load.start()
    if own_scatter:
        partial = rest[61]
        proj_scatter = Scatter(place, TAPS, 1, partial, result, *rest[62:73])
        conv_scatter = Scatter(place, 0, TAPS, partial, result, *rest[73:84])
    place.barrier()
    stream = Stream(place, out_stage, landed_out, out_sent, out_landed, base * per_slot)
    stream.pump(WINDOW)
    cot_relays, out_relays = [], []
    if relay:
        for column, (begin, held) in enumerate(starts(counts, dims)):
            for slot in range(relay):
                at = 2 * jnp.minimum(begin + slot, dp_count * relay - 1)
                home_cot[column, slot] = crossed[at]
                home_out[column, slot] = crossed[at + 1]
        spot = lambda own: pl.ds(pl.multiple_of(own * CHUNK, CHUNK), CHUNK)
        cot_relays = to_columns(
            place, home_cot, lambda own: relayed.at[:, spot(own)], relay_own.at[0], relay_cot_sent, relay_cot_landed
        )
    count = float(per_micro * rows * dp_count * bin_count)
    params = params_in[...]
    norm_rows(stats_one[...], (params[0:1], params[1:2]), count, scale_one, offset_one, inverse_one, shift_one)
    norm_rows(
        totals_two[...],
        (params[3:4, :feats], params[3:4, feats : 2 * feats]),
        count,
        scale_two,
        offset_two,
        inverse_two,
        shift_two,
    )
    sums_two[...] = jnp.zeros_like(sums_two)
    sums_one[...] = jnp.zeros_like(sums_one)
    bias_sum[...] = jnp.zeros_like(bias_sum)
    for load in loads[:5]:
        load.wait()

    def head(i, late):
        micro = i // per_micro
        inner = pl.ds(pl.multiple_of(lax.rem(i, per_micro) * rows, rows), rows)
        cotangent = cots[meta[3, i]]
        if late and relay:
            place_in = meta[4, i] - base
            other = relayed[jnp.clip(place_in, 0, relay - 1)]
            cotangent = jnp.where((meta[0, i] > 0) & (place_in >= 0) & (place_in < relay), other, cotangent)
        chosen[micro, inner] = cotangent
        bias_sum[...] += eighth(cotangent.astype(F32))
        values = conv[i]
        hidden, slope = gelu_both(values * scale_two[micro] + offset_two[micro])
        hidden_two[micro, inner] = hidden.astype(BF16)
        grad = matmul(cotangent, w[TAPS], 1, 0) * slope
        grad_two[i] = grad
        sums_two[micro] += eighth(grad)
        sums_two[MICRO + micro] += eighth(grad * values)

    stream.loop(base, lambda i: head(i, False), BACK_PUMPS[0])
    for copy in cot_relays:
        copy.wait()
    stream.loop(seqs - base, lambda i: head(i + base, True), BACK_PUMPS[9])
    mine = reduce_two[0]
    mine[0 : 2 * MICRO] = jnp.sum(sums_two[...], axis=1)
    bias_row = jnp.sum(bias_sum[...], axis=0, keepdims=True)
    spare = jnp.zeros((1, feats), F32)
    for part in range(2 * MICRO):
        begin = part * feats
        mine[2 * MICRO + part : 2 * MICRO + part + 1] = bias_row[:, begin : begin + feats] if begin < chans else spare
    reduce = AllReduce(place, *reduce_two)
    reduce.start_near()
    stream.pump(BACK_PUMPS[1])

    def weigh(line, terms):
        total = None
        for left, right in terms:
            term = matmul(left, right, 0, 0)
            total = term if total is None else total + term
        partial[line] = total.reshape(partial.shape[1:])

    def proj_terms(micros):
        return [(chosen[micro], hidden_two[micro]) for micro in micros]

    reduce.finish_near()
    reduce.start_far()
    if relay:
        out_relays = to_columns(
            place, home_out, lambda own: landed_relay.at[:, spot(own)], relay_own.at[1], relay_out_sent, relay_out_landed
        )
    weigh(TAPS, proj_terms(range(MICRO)))
    if own_scatter:
        proj_scatter.start_core()
    stream.pump(BACK_PUMPS[2])
    back_two = reduce.finish_far()

    def lines(back, scale, inverse, shift, line, remainder, out):
        for micro in range(MICRO):
            plain = back[micro : micro + 1]
            centred = inverse[micro] * back[MICRO + micro : MICRO + micro + 1] + shift[micro] * plain
            out[micro : micro + 1] = plain
            out[MICRO + micro : MICRO + micro + 1] = centred
            line[micro] = -scale[micro] * inverse[micro] * (centred / count)
            remainder[micro] = -scale[micro] * (plain / count + shift[micro] * (centred / count))

    lines(back_two, scale_two, inverse_two, shift_two, line_two, rest_two, sums_two_out)
    sums_two_out[2 * MICRO :] = back_two[2 * MICRO :]

    def conv_gradient(i, begin, size):
        micro = i // per_micro
        span = slice(begin, begin + size)
        value = scale_two[micro] * grad_two[i, span] + line_two[micro] * conv[i, span] + rest_two[micro]
        return value.astype(BF16).astype(F32)

    def edges(i):
        reverse = meta[0, i]
        top, bottom = conv_gradient(i, 0, DILATION), conv_gradient(i, rows - DILATION, DILATION)
        send_left[i] = jnp.where(reverse > 0, bottom, top)
        send_right[i] = jnp.where(reverse > 0, top, bottom)

    lax.fori_loop(0, seqs, lambda i, carry: (edges(i), carry)[1], 0)
    halo = Halo(place, send_left, send_right, from_left, from_right, halo_sent, halo_landed)
    halo.start()
    if own_scatter:
        proj_scatter.core_to_dp()
    stream.pump(BACK_PUMPS[3])
    loads[5].wait()
    halo.finish()

    def tail(i):
        micro = i // per_micro
        inner = pl.ds(pl.multiple_of(lax.rem(i, per_micro) * rows, rows), rows)
        reverse = meta[0, i]
        left, right = from_left[i], from_right[i]
        low = jnp.where(reverse > 0, right, left)
        high = jnp.where(reverse > 0, left, right)
        full = jnp.concatenate([low, conv_gradient(i, 0, rows), high], axis=0)
        grad = None
        for tap in range(TAPS):
            begin = (TAPS - 1 - tap) * DILATION
            window = full[begin : begin + rows].astype(BF16)
            windows[micro, inner, tap * feats : (tap + 1) * feats] = window
            term = matmul(window, w[tap], 1, 1)
            grad = term if grad is None else grad + term
        values = moved[i].astype(F32)
        hidden, slope = gelu_both(values * scale_one[micro] + offset_one[micro])
        hidden_one[micro, inner] = hidden.astype(BF16)
        grad = grad * slope
        grad_one[i] = grad
        sums_one[micro] += eighth(grad)
        sums_one[MICRO + micro] += eighth(grad * values)

    stream.loop(seqs, tail, BACK_PUMPS[4])
    mine = reduce_one[0]
    mine[...] = jnp.sum(sums_one[...], axis=1)
    reduce = AllReduce(place, *reduce_one)
    reduce.start_near()
    if own_scatter:
        proj_scatter.dp_to_chip()
    stream.pump(BACK_PUMPS[5])

    def conv_weigh(micros, add):
        total = None
        for micro in micros:
            term = matmul(hidden_one[micro], windows[micro], 0, 0)
            total = term if total is None else total + term
        for tap in range(TAPS):
            part = total[:, tap * feats : (tap + 1) * feats].reshape(partial.shape[1:])
            partial[tap] = partial[tap] + part if add else part

    conv_weigh(range(MICRO // 2), False)
    reduce.finish_near()
    reduce.start_far()
    conv_weigh(range(MICRO // 2, MICRO), True)
    if own_scatter:
        conv_scatter.start_core()
    stream.pump(BACK_PUMPS[6])
    back_one = reduce.finish_far()
    lines(back_one, scale_one, inverse_one, shift_one, line_one, rest_one, sums_one_out)
    if own_scatter:
        conv_scatter.core_to_dp()
        proj_scatter.finish()

    def end(i):
        micro = i // per_micro
        inner = pl.ds(pl.multiple_of(lax.rem(i, per_micro) * rows, rows), rows)
        reverse = meta[0, i]
        value = scale_one[micro] * grad_one[i] + line_one[micro] * moved[i].astype(F32) + rest_one[micro]
        value = chosen[micro, inner].astype(F32) + value
        grads[i] = value.astype(BF16)
        top, bottom = value[:LAST_EDGE].astype(BF16), value[rows - LAST_EDGE :].astype(BF16)
        last_left[i] = jnp.where(reverse > 0, bottom, top)
        last_right[i] = jnp.where(reverse > 0, top, bottom)

    stream.loop(seqs, end, BACK_PUMPS[7])
    last = Halo(place, last_left, last_right, last_from_left, last_from_right, last_sent, last_landed)
    last.start()
    stream.pump(BACK_PUMPS[8])
    if own_scatter:
        conv_scatter.dp_to_chip()
    last.finish()
    low_edge[...] = last_from_left[...]
    high_edge[...] = last_from_right[...]
    if own_scatter:
        conv_scatter.finish()
    for copy in out_relays:
        copy.wait()
    stream.finish()


def run_backward(dims, meta, counts, crossed, moved, conv, w, stats_one, params, totals_two, cot, cot_near, cot_far, out_stage):
    dp_count, bin_count, seqs, rows, chans, feats, base, relay = dims
    chips = bin_count // 2
    group = TAPS + 1
    quarter = chans // (dp_count * bin_count)
    own_scatter = scatters(dims)
    per_slot = rows // CHUNK
    held = seqs // MICRO * rows
    dma = pltpu.SemaphoreType.DMA
    wide = pltpu.VMEM((MICRO, 1, chans), F32)
    narrow = pltpu.VMEM((MICRO, 1, feats), F32)
    edge = jax.ShapeDtypeStruct((seqs, LAST_EDGE, chans), BF16)
    return pl.pallas_call(
        functools.partial(backward_kernel, dims),
        out_shape=(
            jax.ShapeDtypeStruct((seqs, rows, chans), BF16),
            edge,
            edge,
            jax.ShapeDtypeStruct((base * per_slot, CHUNK, chans), BF16),
            jax.ShapeDtypeStruct((4 * MICRO, feats), F32),
            jax.ShapeDtypeStruct((2 * MICRO, chans), F32),
            jax.ShapeDtypeStruct((group, quarter if own_scatter else chans, feats), F32),
            *([jax.ShapeDtypeStruct((relay, rows, chans), BF16)] if relay else ()),
        ),
        in_specs=[smem(), smem(), vmem(), *[anywhere()] * 3, *[vmem()] * 3, *[anywhere()] * 4],
        out_specs=(vmem(), vmem(), vmem(), anywhere(), vmem(), vmem(), vmem(), *([anywhere()] if relay else ())),
        scratch_shapes=[
            pltpu.VMEM((2 * seqs, rows, chans), BF16),
            pltpu.VMEM((seqs, rows, chans), BF16),
            pltpu.VMEM((seqs, rows, feats), F32),
            pltpu.VMEM((group, chans, feats), BF16),
            pltpu.VMEM((MICRO, held, chans), BF16),
            *[wide] * 4,
            *[narrow] * 4,
            pltpu.VMEM((seqs, rows, feats), F32),
            pltpu.VMEM((seqs, rows, chans), F32),
            pltpu.VMEM((MICRO, held, feats), BF16),
            pltpu.VMEM((MICRO, held, chans), BF16),
            pltpu.VMEM((MICRO, held, TAPS * feats), BF16),
            pltpu.VMEM((2 * MICRO, 8, feats), F32),
            pltpu.VMEM((2 * MICRO, 8, chans), F32),
            pltpu.VMEM((8, chans), F32),
            narrow,
            narrow,
            wide,
            wide,
            *[pltpu.VMEM((seqs, DILATION, feats), F32)] * 4,
            *[pltpu.VMEM((seqs, LAST_EDGE, chans), BF16)] * 4,
            *AllReduce.scratch(dp_count, bin_count, 4 * MICRO, feats),
            *AllReduce.scratch(dp_count, bin_count, 2 * MICRO, chans),
            dma((6,)),
            dma((2,)),
            dma((2,)),
            dma((2,)),
            dma((2,)),
            dma((base * per_slot,)),
            dma((base * per_slot,)),
            *(
                (
                    pltpu.VMEM((group, dp_count, chips, 2, quarter, feats), F32),
                    *Scatter.scratch(dims, 1),
                    *Scatter.scratch(dims, TAPS),
                )
                if own_scatter
                else ()
            ),
            *(
                [pltpu.VMEM((relay, rows, chans), BF16)]
                + [pltpu.VMEM((dp_count, relay, CHUNK, chans), BF16)] * 2
                + [dma((2,))]
                + [dma((dp_count,))] * 4
                if relay
                else ()
            ),
        ],
        compiler_params=pltpu.CompilerParams(
            collective_id=2, has_side_effects=True, vmem_limit_bytes=VMEM_LIMIT
        ),
        name="backward",
    )(meta, counts, crossed, moved, conv, w, stats_one, params, totals_two, cot, cot_near, cot_far, out_stage)


def last_kernel(dims, meta, back_one, back_two, *rest):
    dp_count, bin_count, seqs, rows, chans, feats, base, relay = dims
    own_scatter = scatters(dims)
    partial, rest = (rest[0], rest[1:]) if own_scatter else (None, rest)
    (grad, left, right, out, near), rest = rest[:5], rest[5:]
    relayed, rest = (rest[0], rest[1:]) if relay else (None, rest)
    (far, result_out, result_grad, gain_one, bias_one, gain_two, bias_two, bias_proj) = rest[:8]
    if own_scatter:
        conv_weight, proj_weight = rest[8:10]
        conv_weight[...] = partial[:TAPS]
        proj_weight[...] = partial[TAPS]
    (held, made, got, put) = rest[-4:]
    for i in range(seqs):
        reverse, slot = meta[0, i], meta[4, i]

        @pl.when(reverse == 0)
        def _():
            pltpu.make_async_copy(out.at[i], held.at[i], got.at[i]).start()

        @pl.when((reverse > 0) & (slot < base))
        def _():
            pltpu.make_async_copy(near.at[jnp.minimum(slot, base - 1)], held.at[i], got.at[i]).start()

        if relay:

            @pl.when((reverse > 0) & (slot >= base) & (slot < base + relay))
            def _():
                pltpu.make_async_copy(relayed.at[jnp.clip(slot - base, 0, relay - 1)], held.at[i], got.at[i]).start()

        @pl.when((reverse > 0) & (slot >= base + relay))
        def _():
            pltpu.make_async_copy(far.at[jnp.maximum(slot - base - relay, 0)], held.at[i], got.at[i]).start()

    across = rows + 2 * LAST_EDGE
    row = lax.broadcasted_iota(jnp.int32, (rows, across), 0)
    column = lax.broadcasted_iota(jnp.int32, (rows, across), 1)

    def step(i, carry):
        reverse, shift = meta[0, i], meta[1, i]
        low = jnp.where(reverse > 0, right[i], left[i])
        high = jnp.where(reverse > 0, left[i], right[i])
        source = jnp.concatenate([low, grad[i], high], axis=0)
        place = jnp.where(reverse > 0, rows - 1 - row - shift, row + shift) + LAST_EDGE
        pick = jnp.where(column == place, 1.0, 0.0).astype(BF16)
        made[i] = matmul(pick, source, 1, 0).astype(BF16)
        pltpu.make_async_copy(made.at[i], result_grad.at[i], put.at[0]).start()
        pltpu.make_async_copy(held.at[i], held.at[i], got.at[i]).wait()
        pltpu.make_async_copy(held.at[i], result_out.at[i], put.at[1]).start()
        return carry

    lax.fori_loop(0, seqs, step, 0)
    dp, bins = lax.axis_index("dp"), lax.axis_index("bins")

    def own(values, index, result):
        width, share = values.shape[1], result.shape[1]
        begin = index * share
        result[...] = pltpu.roll(values, lax.rem(width - begin, width), 1)[:, :share]

    def summed(back, begin):
        return jnp.sum(back[begin : begin + MICRO], axis=0, keepdims=True)

    wide, narrow = dp * bin_count + bins, bins
    own(summed(back_one, MICRO), wide, gain_one)
    own(summed(back_one, 0), wide, bias_one)
    own(summed(back_two, MICRO), narrow, gain_two)
    own(summed(back_two, 0), narrow, bias_two)
    bias = jnp.concatenate([back_two[2 * MICRO + k : 2 * MICRO + k + 1] for k in range(chans // feats)], axis=1)
    own(bias, wide, bias_proj)
    pltpu.make_async_copy(made, result_grad, put.at[0]).wait()
    pltpu.make_async_copy(held, result_out, put.at[1]).wait()


def run_last(dims, meta, back_one, back_two, partial, grad, left, right, out, near, relayed, far):
    dp_count, bin_count, seqs, rows, chans, feats, base, relay = dims
    own_scatter = scatters(dims)
    big = jax.ShapeDtypeStruct((seqs, rows, chans), BF16)
    quarter = chans // (dp_count * bin_count)
    wide = jax.ShapeDtypeStruct((1, quarter), F32)
    narrow = jax.ShapeDtypeStruct((1, feats // bin_count), F32)
    weights = (
        jax.ShapeDtypeStruct((TAPS, quarter, feats), F32),
        jax.ShapeDtypeStruct((quarter, feats), F32),
    )
    partials = [partial] if own_scatter else []
    return pl.pallas_call(
        functools.partial(last_kernel, dims),
        out_shape=(big, big, wide, wide, narrow, narrow, wide, *(weights if own_scatter else ())),
        in_specs=[
            smem(),
            *[vmem()] * (5 + len(partials)),
            *[anywhere()] * (3 + len(relayed)),
        ],
        out_specs=(anywhere(), anywhere(), *[vmem()] * (7 if own_scatter else 5)),
        scratch_shapes=[
            pltpu.VMEM(big.shape, BF16),
            pltpu.VMEM(big.shape, BF16),
            pltpu.SemaphoreType.DMA((seqs,)),
            pltpu.SemaphoreType.DMA((2,)),
        ],
        compiler_params=pltpu.CompilerParams(vmem_limit_bytes=VMEM_LIMIT),
        name="last",
    )(meta, back_one, back_two, *partials, grad, left, right, out, near, *relayed, far)


def local(
    activations,
    shift_bins,
    reverse_flags,
    gain_one,
    bias_one,
    conv_weight,
    gain_two,
    bias_two,
    proj_weight,
    proj_bias,
    cotangent,
):
    seqs, rows, chans = activations.shape
    feats = conv_weight.shape[2]
    dp_count, bin_count = lax.axis_size("dp"), lax.axis_size("bins")
    per_slot = rows // CHUNK
    base = BASE_SLOTS
    relay = RELAY_SLOTS if per_slot == dp_count else 0
    dims = (dp_count, bin_count, seqs, rows, chans, feats, base, relay)

    vectors = [vector[None] for vector in (gain_one, bias_one, proj_bias, gain_two, bias_two)]
    shard = jnp.concatenate([conv_weight, proj_weight.T[None]], axis=0)

    (
        moved,
        conv,
        out,
        out_stage,
        out_extra,
        cot_extra,
        cot_near,
        w,
        stats_one,
        params,
        totals_two,
        meta,
        *relays,
    ) = run_front(
        dims,
        reverse_flags,
        shift_bins,
        activations,
        cotangent.reshape(seqs * per_slot, CHUNK, chans),
        shard,
        vectors,
    )
    counts, choice, *packed = run_compact(dims, params, *relays)
    pairs = [(source, bin_count - 1 - source) for source in range(bin_count)]
    direct = seqs - base - relay
    pieces = 2 * dp_count * relay

    def crossing(relayed, slots, packed, pair):
        moving = [packed[: 2 * relayed]] * (relayed > 0)
        moving += [item[: slots * per_slot] for item in pair] * (slots > 0)
        if not moving:
            return packed, *pair
        got = lax.ppermute(jnp.concatenate(moving), "bins", pairs)
        put = lax.dynamic_update_slice_in_dim
        if relayed:
            packed = put(packed, got[: 2 * relayed], 0, 0)
        if slots:
            held = slots * per_slot
            rest = got[2 * relayed :]
            pair = tuple(put(item, rest[k * held : (k + 1) * held], 0, 0) for k, item in enumerate(pair))
        return packed, *pair

    every = pieces // 2
    branches = [functools.partial(crossing, held, 0) for held in range(every + 1)]
    for slots in range(1, direct + 1):
        branches += [functools.partial(crossing, held, slots) for held in (every // 2, every)]
    packed = packed[0] if relay else jnp.zeros((1, CHUNK, chans), BF16)
    crossed, cot_far, out_far = lax.switch(choice[0], branches, packed, (cot_extra, out_extra))

    slots_of = lambda item: item.reshape(-1, rows, chans)
    grads, low_edge, high_edge, out_near, back_two, back_one, partial, *landed = run_backward(
        dims,
        meta,
        counts,
        crossed,
        moved,
        conv,
        w,
        stats_one,
        params,
        totals_two,
        cotangent,
        slots_of(cot_near),
        slots_of(cot_far),
        out_stage,
    )
    output, grad_activations, gain_one, bias_one, gain_two, bias_two, bias_proj, *weights = run_last(
        dims,
        meta,
        back_one,
        back_two,
        partial,
        grads,
        low_edge,
        high_edge,
        out,
        slots_of(out_near),
        landed,
        slots_of(out_far),
    )
    if not weights:
        scattered = lax.psum_scatter(partial, ("dp", "bins"), scatter_dimension=1, tiled=True)
        weights = scattered[:TAPS], scattered[TAPS]
    return (
        output,
        grad_activations,
        gain_one[0],
        bias_one[0],
        weights[0],
        gain_two[0],
        bias_two[0],
        weights[1].T,
        bias_proj[0],
    )


def solution(mesh):
    placed = (
        P("dp", "bins", None),
        P("dp"),
        P("dp"),
        P("bins"),
        P("bins"),
        P(None, "bins", None),
        P("bins"),
        P("bins"),
        P(None, "bins"),
        P("bins"),
        P("dp", "bins", None),
    )
    return jax.shard_map(
        local,
        mesh=mesh,
        in_specs=placed,
        out_specs=(
            P("dp", "bins", None),
            P("dp", "bins", None),
            P(("dp", "bins")),
            P(("dp", "bins")),
            P(None, ("dp", "bins"), None),
            P("bins"),
            P("bins"),
            P(None, ("dp", "bins")),
            P(("dp", "bins")),
        ),
        check_vma=False,
    )
```

```python
import functools

import jax
import jax.numpy as jnp
from jax import lax
from jax.experimental import pallas as pl
from jax.experimental.pallas import tpu as pltpu
from jax.sharding import PartitionSpec as P

TAPS = 3
DILATION = 8
MICRO = 4
EPSILON = 1e-05
CHUNK = 32
BASE_SLOTS = 8
RELAY_SLOTS = 4
PUMPS = (0, 1, 10, 0, 4, 4, 0, 18, 0, 0)
BACK_PUMPS = (2, 1, 3, 5, 6, 1, 4, 2, 32, 2, 3)
WINDOW = 32
EDGE = 16
LAST_EDGE = 8
VMEM_LIMIT = 60 * 1024 * 1024
MESH = pl.DeviceIdType.MESH
F32 = jnp.float32
BF16 = jnp.bfloat16
ROOT = 0.7978845608028654
CUBE = 0.044715


def vmem():
    return pl.BlockSpec(memory_space=pltpu.VMEM)


def smem():
    return pl.BlockSpec(memory_space=pltpu.SMEM)


def anywhere():
    return pl.BlockSpec(memory_space=pl.ANY)


def matmul(a, b, ca, cb):
    return lax.dot_general(a, b, (((ca,), (cb,)), ((), ())), preferred_element_type=F32)


class Place:
    def __init__(self, dp_count, bin_count):
        self.dp_count, self.bin_count = dp_count, bin_count
        self.chip_count = bin_count // 2
        self.dp = lax.axis_index("dp")
        self.bin = lax.axis_index("bins")
        self.chip = self.bin // 2
        self.core = lax.rem(self.bin, 2)

    def barrier(self):
        semaphore = pltpu.get_barrier_semaphore()
        for apart in range(1, self.bin_count):
            other = (self.dp, lax.rem(self.bin + apart, self.bin_count))
            pl.semaphore_signal(semaphore, inc=1, device_id=other, device_id_type=MESH)
        for apart in range(1, self.dp_count):
            for core in range(2):
                other = (lax.rem(self.dp + apart, self.dp_count), self.chip * 2 + core)
                pl.semaphore_signal(semaphore, inc=1, device_id=other, device_id_type=MESH)
        pl.semaphore_wait(semaphore, self.bin_count - 1 + 2 * (self.dp_count - 1))


def remote(source, target, sent, landed, device):
    return pltpu.make_async_remote_copy(
        src_ref=source,
        dst_ref=target,
        send_sem=sent,
        recv_sem=landed,
        device_id=device,
        device_id_type=MESH,
    )


class Stream:
    def __init__(self, place, source, target, sent, landed, count):
        self.source, self.target, self.sent, self.landed = source, target, sent, landed
        self.count, self.next = count, 0
        self.device = (place.dp, place.bin_count - 1 - place.bin)

    def piece(self, index):
        return remote(
            self.source.at[index],
            self.target.at[index],
            self.sent.at[index],
            self.landed.at[index],
            self.device,
        )

    def pump(self, pieces=1):
        for _ in range(pieces):
            if self.next >= self.count:
                return
            if self.next >= WINDOW:
                self.piece(self.next - WINDOW).wait_send()
            self.piece(self.next).start()
            self.next += 1

    def loop(self, trips, body, pieces):
        pieces = max(0, min(pieces, self.count - self.next, trips))
        if pieces == 0 or self.next < WINDOW and self.next + pieces <= WINDOW:
            first, every = self.next, trips // max(pieces, 1)

            def plain(i, carry):
                body(i)
                done = lax.div(i, every)
                if pieces:

                    @pl.when((lax.rem(i, every) == 0) & (done < pieces))
                    def _():
                        self.piece(first + done).start()

                return carry

            lax.fori_loop(0, trips, plain, 0)
            self.next += pieces
            return
        if pieces == 0:
            lax.fori_loop(0, trips, lambda i, carry: (body(i), carry)[1], 0)
            return
        if self.next < WINDOW:
            self.pump(WINDOW - self.next)
            pieces = max(0, min(pieces, self.count - self.next))
        first = self.next
        every = trips // max(pieces, 1)

        def step(i, carry):
            body(i)
            done = lax.div(i, every)

            @pl.when((lax.rem(i, every) == 0) & (done < pieces))
            def _():
                self.piece(first + done - WINDOW).wait_send()
                self.piece(first + done).start()

            return carry

        lax.fori_loop(0, trips, step, 0)
        self.next = first + pieces

    def finish(self):
        self.pump(self.count)
        for index in range(max(0, self.count - WINDOW), self.count):
            self.piece(index).wait_send()
        for index in range(self.count):
            self.piece(index).wait_recv()


class AllReduce:
    def __init__(self, place, mine, near, far, near_sent, near_landed, far_sent, far_landed):
        self.place, self.mine, self.near, self.far = place, mine, near, far
        self.near_count = place.dp_count * 2
        self.me = place.dp * 2 + place.core
        self.near_copies = []
        for apart in range(1, self.near_count):
            to = lax.rem(self.me + apart, self.near_count)
            device = (to // 2, place.chip * 2 + lax.rem(to, 2))
            self.near_copies.append(
                remote(mine, near.at[apart - 1], near_sent.at[apart - 1], near_landed.at[apart - 1], device)
            )
        self.far_copies = []
        for apart in range(1, place.chip_count):
            to = lax.rem(place.chip + apart, place.chip_count)
            device = (place.dp, to * 2 + place.core)
            self.far_copies.append(
                remote(
                    near.at[self.near_count - 1],
                    far.at[apart - 1],
                    far_sent.at[apart - 1],
                    far_landed.at[apart - 1],
                    device,
                )
            )

    def start_near(self):
        for copy in self.near_copies:
            copy.start()

    def finish_near(self):
        for copy in self.near_copies:
            copy.wait()
        count = self.near_count

        total = None
        for member in range(count):
            apart = lax.rem(self.me - member + count, count)
            other = self.near[jnp.maximum(apart - 1, 0)]
            part = jnp.where(apart == 0, self.mine[...], other)
            total = part if total is None else total + part
        self.near[count - 1] = total

    def start_far(self):
        for copy in self.far_copies:
            copy.start()

    def finish_far(self):
        for copy in self.far_copies:
            copy.wait()
        count = self.place.chip_count
        total = None
        for member in range(count):
            apart = lax.rem(self.place.chip - member + count, count)
            part = jnp.where(
                apart == 0, self.near[self.near_count - 1], self.far[jnp.maximum(apart - 1, 0)]
            )
            total = part if total is None else total + part
        return total

    @staticmethod
    def scratch(dp_count, bin_count, rows, width):
        near, far = dp_count * 2, bin_count // 2
        return [
            pltpu.VMEM((rows, width), F32),
            pltpu.VMEM((near, rows, width), F32),
            pltpu.VMEM((far, rows, width), F32),
            pltpu.SemaphoreType.DMA((near,)),
            pltpu.SemaphoreType.DMA((near,)),
            pltpu.SemaphoreType.DMA((far,)),
            pltpu.SemaphoreType.DMA((far,)),
        ]


class Halo:
    def __init__(self, place, to_left, to_right, from_left, from_right, sent, landed):
        self.place, self.from_left, self.from_right = place, from_left, from_right
        count = place.bin_count
        self.right = remote(
            to_right, from_left, sent.at[0], landed.at[0], (place.dp, lax.rem(place.bin + 1, count))
        )
        self.left = remote(
            to_left, from_right, sent.at[1], landed.at[1], (place.dp, lax.rem(place.bin + count - 1, count))
        )
        self.first = place.bin == 0
        self.last = place.bin == count - 1

    def start(self):
        @pl.when(jnp.logical_not(self.last))
        def _():
            self.right.start()

        @pl.when(jnp.logical_not(self.first))
        def _():
            self.left.start()

        @pl.when(self.first)
        def _():
            self.from_left[...] = jnp.zeros_like(self.from_left)

        @pl.when(self.last)
        def _():
            self.from_right[...] = jnp.zeros_like(self.from_right)

    def finish(self):
        @pl.when(jnp.logical_not(self.last))
        def _():
            self.right.wait_send()
            self.left.wait_recv()

        @pl.when(jnp.logical_not(self.first))
        def _():
            self.left.wait_send()
            self.right.wait_recv()


def eighth(values):
    rows, width = values.shape
    return jnp.sum(values.reshape(rows // 8, 8, width), axis=0)


def norm_rows(totals, gains, count, scale_ref, offset_ref, inverse_ref, shift_ref):
    for micro in range(MICRO):
        mean = totals[micro : micro + 1] / count
        second = totals[MICRO + micro : MICRO + micro + 1] / count
        inverse = lax.rsqrt(second - mean * mean + EPSILON)
        scale = inverse * gains[0]
        scale_ref[micro] = scale
        offset_ref[micro] = gains[1] - mean * scale
        if inverse_ref is not None:
            inverse_ref[micro] = inverse
            shift_ref[micro] = -mean * inverse


def gelu(v):
    half = 0.5 * v
    return half + half * jnp.tanh(v * (ROOT + (ROOT * CUBE) * (v * v)))


def gelu_both(v):
    square = v * v
    p = 0.5 + 0.5 * jnp.tanh(v * (ROOT + (ROOT * CUBE) * square))
    value = v * p
    slope = p + value * (1.0 - p) * ((2.0 * ROOT) + (6.0 * ROOT * CUBE) * square)
    return value, slope


def to_columns(place, source, target, own, sent, landed):
    copies = []
    for apart in range(1, place.dp_count):
        to = lax.rem(place.dp + apart, place.dp_count)
        copies.append(
            remote(
                source.at[to], target(place.dp), sent.at[apart - 1], landed.at[apart - 1], (to, place.bin)
            )
        )
        copies[-1].start()
    copies.append(pltpu.make_async_copy(source.at[place.dp], target(place.dp), own))
    copies[-1].start()
    return copies


def front_kernel(dims, flags, shifts, x_in, cot, shard, *rest):
    dp_count, bin_count, seqs, rows, chans, feats, base, relay = dims
    vectors, rest = rest[:5], rest[5:]
    (moved_out, conv_out, out_out, out_stage, out_extra, cot_extra, landed_cot, weights_out) = rest[:8]
    (stats_out, params_out, totals_two) = rest[8:11]
    meta, rest = rest[11], rest[:11] + rest[12:]
    if relay:
        relay_cot, relay_out = rest[11:13]
        rest = rest[:11] + rest[13:]
    (x, x_low, x_high, hidden_all, moved, conv, out, w, stage) = rest[11:20]
    direct = direct_weights(dims)
    weights = w if direct else weights_out
    (sums_one, sums, scale_one, offset_one, scale_two, offset_two) = rest[20:26]
    reduce_first = rest[26:33]
    reduce_second = rest[33:40]
    (local, stores, halo_sent, halo_landed, one_sent, one_landed, two_sent, two_landed, three_sent, three_landed) = rest[40:50]
    cot_sent, cot_landed = rest[50:52]
    (line_out, lines, count_out, count_all, line_sent, line_landed, count_sent, count_landed) = rest[-8:]
    place = Place(dp_count, bin_count)
    per_slot = rows // CHUNK
    per_micro = seqs // MICRO
    if relay:
        (over_cot, over_out, relay_own) = rest[52:55]
        (relay_cot_sent, relay_cot_landed, relay_out_sent, relay_out_landed) = rest[55:59]
    share = chans // bin_count
    group = TAPS + 1
    total_bins = rows * bin_count
    load = pltpu.make_async_copy(x_in, x, local.at[0])
    load.start()
    tap = lax.rem(place.dp, group)
    home = pl.ds(pl.multiple_of(place.bin * share, 8), share)
    keep = pltpu.make_async_copy(shard.at[tap], weights.at[tap, home], local.at[1])
    keep.start()
    reversed_count = jnp.int32(0)
    origins = [jnp.int32(0)] * seqs
    for i in range(seqs):
        reverse = jnp.where(flags[i] > 0, 1, 0)
        meta[0, i] = reverse
        meta[1, i] = shifts[i]
        for slot in range(i + 1):
            origins[slot] = jnp.where((reverse > 0) & (reversed_count == slot), i, origins[slot])
        slot = reverse * reversed_count
        meta[3, i] = jnp.where(reverse > 0, seqs + slot, i)
        meta[4, i] = slot
        reversed_count += reverse
    for slot in range(seqs):
        meta[2, slot] = origins[slot]
    place.barrier()

    ones = []
    for apart in range(1, place.chip_count):
        to = lax.rem(place.chip + apart, place.chip_count)
        ones.append(
            remote(
                shard.at[tap],
                weights.at[tap, home],
                one_sent.at[apart - 1],
                one_landed.at[apart - 1],
                (place.dp, to * 2 + place.core),
            )
        )
        ones[-1].start()
    pieces = [vector[...].astype(F32) for vector in vectors]
    wide = sum(piece.shape[1] for piece in pieces)
    if wide < chans:
        pieces.append(jnp.zeros((1, chans - wide), F32))
    line_out[...] = jnp.concatenate(pieces, axis=1)
    lines[place.bin] = line_out[...]
    count_out[...] = jnp.zeros_like(count_out) + reversed_count.astype(F32)
    count_all[place.dp] = count_out[...]
    smalls = []
    for apart in range(1, bin_count):
        to = lax.rem(place.bin + apart, bin_count)
        smalls.append(
            remote(line_out, lines.at[place.bin], line_sent.at[apart - 1], line_landed.at[apart - 1], (place.dp, to))
        )
    for apart in range(1, dp_count):
        to = lax.rem(place.dp + apart, dp_count)
        smalls.append(
            remote(
                count_out,
                count_all.at[place.dp],
                count_sent.at[apart - 1],
                count_landed.at[apart - 1],
                (to, place.bin),
            )
        )
    for copy in smalls:
        copy.start()
    halo = Halo(
        place, x_in.at[:, 0:EDGE], x_in.at[:, rows - EDGE : rows], x_low, x_high, halo_sent, halo_landed
    )
    halo.start()
    for slot in range(base):
        origin = meta[2, slot] * per_slot
        for piece in range(per_slot):
            stage[slot * per_slot + piece] = cot[origin + piece]
    stream = Stream(place, stage, landed_cot, cot_sent, cot_landed, base * per_slot)
    load.wait()

    sums_one[...] = jnp.zeros_like(sums_one)
    row = lax.broadcasted_iota(jnp.int32, (rows, 1), 0) + place.bin * rows

    def statistics(i):
        micro = i // per_micro
        target = row + meta[1, i]
        inside = jnp.where((target >= 0) & (target < total_bins), 1.0, 0.0).astype(F32)
        values = x[i].astype(F32) * inside
        sums_one[micro] += eighth(values)
        sums_one[MICRO + micro] += eighth(values * values)

    stream.loop(seqs, statistics, PUMPS[0])
    mine = reduce_first[0]
    mine[...] = jnp.sum(sums_one[...], axis=1)
    reduce = AllReduce(place, *reduce_first)
    reduce.start_near()
    keep.wait()
    for copy in ones:
        copy.wait()
    twos = []
    for apart in range(1, group):
        to = (place.dp // group) * group + lax.rem(tap + apart, group)
        for chip in range(place.chip_count):
            part = weights.at[tap, pl.ds(pl.multiple_of((chip * 2 + place.core) * share, 8), share)]
            index = (apart - 1) * place.chip_count + chip
            twos.append(remote(part, part, two_sent.at[index], two_landed.at[index], (to, place.bin)))
            twos[-1].start()
    stream.pump(PUMPS[1])
    for slot in range(base, seqs):
        origin = meta[2, slot] * per_slot
        for piece in range(per_slot):
            if slot < base + relay:
                over_cot[piece, slot - base] = cot[origin + piece]
            else:
                cot_extra[(slot - base - relay) * per_slot + piece] = cot[origin + piece]
    reduce.finish_near()
    reduce.start_far()
    stream.pump(PUMPS[2])
    relays = []
    if relay:
        relays += to_columns(
            place, over_cot, lambda own: relay_cot.at[own], relay_own.at[0], relay_cot_sent, relay_cot_landed
        )
    first = reduce.finish_far()
    stats_out[...] = first
    for copy in smalls:
        copy.wait()
    params_out[...] = jnp.zeros_like(params_out)
    begin = 0
    for index, (line, offset, width) in enumerate(
        ((0, 0, share), (1, 0, share), (2, 0, share), (3, 0, share // 2), (3, feats, share // 2))
    ):
        for member in range(bin_count):
            left = offset + member * width
            params_out[line : line + 1, left : left + width] = lines[member, :, begin : begin + width]
        begin += width
    lane = lax.broadcasted_iota(jnp.int32, (1, chans), 1)
    held = jnp.zeros((1, chans), F32)
    for column in range(dp_count):
        held = jnp.where(lane == feats + column, count_all[column, :, 0:1], held)
    params_out[4:5] = held
    count = float(per_micro * rows * dp_count * bin_count)
    params = params_out[...]
    norm_rows(first, (params[0:1], params[1:2]), count, scale_one, offset_one, None, None)
    proj_bias = params[2:3]
    sums[...] = jnp.zeros_like(sums)
    halo.finish()
    stream.pump(PUMPS[3])

    long_rows = rows + 2 * DILATION
    across = rows + 2 * EDGE
    local_row = lax.broadcasted_iota(jnp.int32, (long_rows, across), 0) - DILATION
    column = lax.broadcasted_iota(jnp.int32, (long_rows, across), 1)
    edge_row = lax.broadcasted_iota(jnp.int32, (DILATION, 1), 0)

    def up(i):
        micro = i // per_micro
        reverse, shift = meta[0, i], meta[1, i]
        direction = 1 - 2 * reverse
        begin = reverse * (rows - 1)
        pick = jnp.where(column == local_row * direction + (begin - shift + EDGE), 1.0, 0.0).astype(BF16)
        source = jnp.concatenate([x_low[i], x[i], x_high[i]], axis=0)
        shifted = matmul(pick, source, 1, 0)
        moved[i] = shifted[DILATION : DILATION + rows].astype(BF16)
        pltpu.make_async_copy(moved.at[i], moved_out.at[i], stores.at[0]).start()
        hidden = gelu(shifted * scale_one[micro] + offset_one[micro])
        parts = []
        for top, first_row in ((0, -DILATION), (DILATION + rows, rows)):
            where = place.bin * rows + begin + (edge_row + first_row) * direction
            parts.append(jnp.where((where >= 0) & (where < total_bins), hidden[top : top + DILATION], 0.0))
        hidden = jnp.concatenate([parts[0], hidden[DILATION : DILATION + rows], parts[1]], axis=0)
        hidden_all[i] = hidden.astype(BF16)

    half_way = seqs // 2
    stream.loop(half_way, up, PUMPS[4])
    for copy in twos:
        copy.wait()
    threes = []
    for line in range(group):
        for chip in range(place.chip_count):
            part = weights.at[line, pl.ds(pl.multiple_of((chip * 2 + place.core) * share, 8), share)]
            index = line * place.chip_count + chip
            threes.append(
                remote(
                    part,
                    part,
                    three_sent.at[index],
                    three_landed.at[index],
                    (place.dp, place.bin + 1 - 2 * place.core),
                )
            )
            threes[-1].start()
    stream.loop(half_way, lambda i: up(i + half_way), PUMPS[5])
    for copy in threes:
        copy.wait()
    if direct:
        pltpu.make_async_copy(w, weights_out, local.at[2]).start()
    else:
        pltpu.make_async_copy(weights_out, w, local.at[2]).start()
        pltpu.make_async_copy(weights_out, w, local.at[2]).wait()

    def across_taps(i):
        micro = i // per_micro
        hidden = hidden_all[i]
        result = None
        for tap in range(TAPS):
            term = matmul(hidden, w[tap], 1, 0)[tap * DILATION : tap * DILATION + rows]
            result = term if result is None else result + term
        conv[i] = result
        pltpu.make_async_copy(conv.at[i], conv_out.at[i], stores.at[1]).start()
        sums[micro] += eighth(result)
        sums[MICRO + micro] += eighth(result * result)

    stream.loop(seqs, across_taps, PUMPS[9])
    mine = reduce_second[0]
    mine[...] = jnp.sum(sums[...], axis=1)
    reduce = AllReduce(place, *reduce_second)
    reduce.start_near()
    stream.pump(PUMPS[6])
    reduce.finish_near()
    reduce.start_far()
    stream.pump(PUMPS[7])
    stats_two = reduce.finish_far()
    totals_two[...] = stats_two
    norm_rows(
        stats_two, (params[3:4, :feats], params[3:4, feats : 2 * feats]), count, scale_two, offset_two, None, None
    )

    def down(i):
        micro = i // per_micro
        hidden = gelu(conv[i] * scale_two[micro] + offset_two[micro]).astype(BF16)
        branch = matmul(hidden, w[TAPS], 1, 1) + proj_bias
        out[i] = (moved[i].astype(F32) + branch).astype(BF16)
        pltpu.make_async_copy(out.at[i], out_out.at[i], stores.at[2]).start()

    stream.loop(seqs - base, lambda i: down(i + base), 0)
    if relay:
        for slot in range(base, base + relay):
            for piece in range(per_slot):
                over_out[piece, slot - base] = out[meta[2, slot], piece * CHUNK : (piece + 1) * CHUNK]
        relays += to_columns(
            place, over_out, lambda own: relay_out.at[own], relay_own.at[1], relay_out_sent, relay_out_landed
        )
    stream.loop(base, down, PUMPS[8])
    for slot in (*range(base), *range(base + relay, seqs)):
        origin = meta[2, slot]
        for piece in range(per_slot):
            part = out[origin, piece * CHUNK : (piece + 1) * CHUNK]
            if slot < base:
                out_stage[slot * per_slot + piece] = part
            else:
                out_extra[(slot - base - relay) * per_slot + piece] = part
    if direct:
        pltpu.make_async_copy(w, weights_out, local.at[2]).wait()
    pltpu.make_async_copy(moved, moved_out, stores.at[0]).wait()
    pltpu.make_async_copy(conv, conv_out, stores.at[1]).wait()
    pltpu.make_async_copy(out, out_out, stores.at[2]).wait()
    for copy in relays:
        copy.wait()
    stream.finish()


def direct_weights(dims):
    return dims[4] // dims[1] % 16 == 0


def run_front(dims, flags, shifts, x, cot, shard, vectors):
    dp_count, bin_count, seqs, rows, chans, feats, base, relay = dims
    per_slot = rows // CHUNK
    chips = bin_count // 2
    group = TAPS + 1
    dma = pltpu.SemaphoreType.DMA
    big = (seqs, rows, chans)
    packed = jax.ShapeDtypeStruct((base * per_slot, CHUNK, chans), BF16)
    spare = jax.ShapeDtypeStruct(((seqs - base - relay) * per_slot, CHUNK, chans), BF16)
    columns = (dp_count, relay, CHUNK, chans)
    edge = pltpu.VMEM((seqs, EDGE, chans), BF16)
    return pl.pallas_call(
        functools.partial(front_kernel, dims),
        out_shape=(
            jax.ShapeDtypeStruct(big, BF16),
            jax.ShapeDtypeStruct((seqs, rows, feats), F32),
            jax.ShapeDtypeStruct(big, BF16),
            packed,
            spare,
            spare,
            packed,
            jax.ShapeDtypeStruct((group, chans, feats), BF16),
            jax.ShapeDtypeStruct((2 * MICRO, chans), F32),
            jax.ShapeDtypeStruct((8, chans), F32),
            jax.ShapeDtypeStruct((2 * MICRO, feats), F32),
            jax.ShapeDtypeStruct((5, seqs), jnp.int32),
            *([jax.ShapeDtypeStruct(columns, BF16)] * 2 if relay else ()),
        ),
        in_specs=[smem(), smem(), anywhere(), vmem(), anywhere(), *[vmem()] * 5],
        out_specs=(
            *[anywhere()] * 3,
            *[vmem()] * 3,
            anywhere(),
            anywhere(),
            *[vmem()] * 3,
            smem(),
            *([anywhere()] * 2 if relay else ()),
        ),
        scratch_shapes=[
            pltpu.VMEM(big, BF16),
            edge,
            edge,
            pltpu.VMEM((seqs, rows + 2 * DILATION, chans), BF16),
            pltpu.VMEM(big, BF16),
            pltpu.VMEM((seqs, rows, feats), F32),
            pltpu.VMEM(big, BF16),
            pltpu.VMEM((group, chans, feats), BF16),
            pltpu.VMEM((base * per_slot, CHUNK, chans), BF16),
            pltpu.VMEM((2 * MICRO, 8, chans), F32),
            pltpu.VMEM((2 * MICRO, 8, feats), F32),
            pltpu.VMEM((MICRO, 1, chans), F32),
            pltpu.VMEM((MICRO, 1, chans), F32),
            pltpu.VMEM((MICRO, 1, feats), F32),
            pltpu.VMEM((MICRO, 1, feats), F32),
            *AllReduce.scratch(dp_count, bin_count, 2 * MICRO, chans),
            *AllReduce.scratch(dp_count, bin_count, 2 * MICRO, feats),
            dma((3,)),
            dma((3,)),
            dma((2,)),
            dma((2,)),
            dma((chips,)),
            dma((chips,)),
            dma((TAPS * chips,)),
            dma((TAPS * chips,)),
            dma((group * chips,)),
            dma((group * chips,)),
            dma((base * per_slot,)),
            dma((base * per_slot,)),
            *([pltpu.VMEM(columns, BF16)] * 2 + [dma((2,))] + [dma((dp_count,))] * 4 if relay else ()),
            pltpu.VMEM((1, chans), F32),
            pltpu.VMEM((bin_count, 1, chans), F32),
            pltpu.VMEM((1, 128), F32),
            pltpu.VMEM((dp_count, 1, 128), F32),
            *[dma((bin_count,))] * 2,
            *[dma((dp_count,))] * 2,
        ],
        compiler_params=pltpu.CompilerParams(
            collective_id=1, has_side_effects=True, vmem_limit_bytes=VMEM_LIMIT
        ),
        name="front",
    )(flags, shifts, x, cot, shard, *vectors)


def starts(counts, dims):
    base, relay = dims[6:8]
    begin, found = jnp.int32(0), []
    for column in range(dims[0]):
        held = jnp.clip(counts[column] - base, 0, relay)
        found.append((begin, held))
        begin = begin + held
    return found


def choose(dims, counts, choice):
    dp_count, seqs, base, relay = dims[0], dims[2], dims[6], dims[7]
    total, most = jnp.int32(0), jnp.int32(0)
    for column in range(dp_count):
        total = total + jnp.clip(counts[column] - base, 0, relay)
        most = jnp.maximum(most, counts[column])
    every = dp_count * relay
    beyond = jnp.maximum(most - base - relay - 1, 0) * 2 + jnp.where(total > every // 2, 1, 0)
    choice[0] = jnp.where(most > base + relay, every + 1 + beyond, total)


def compact_kernel(dims, params, *rest):
    dp_count, feats, relay = dims[0], dims[5], dims[7]
    (cot, out), rest = rest[: 2 * (relay > 0)] or (None, None), rest[2 * (relay > 0) :]
    counts, choice = rest[:2]
    for column in range(dp_count):
        counts[column] = params[4, feats + column].astype(jnp.int32)
    choose(dims, counts, choice)
    if not relay:
        return
    packed, ready = rest[2:]
    for wait in (False, True):
        for column, (begin, held) in enumerate(starts(counts, dims)):
            for slot in range(relay):

                @pl.when(slot < held)
                def _():
                    for side, source in enumerate((cot, out)):
                        copy = pltpu.make_async_copy(
                            source.at[column, slot],
                            packed.at[2 * jnp.minimum(begin + slot, dp_count * relay - 1) + side],
                            ready.at[(side * dp_count + column) * relay + slot],
                        )
                        copy.wait() if wait else copy.start()


def run_compact(dims, params, *relays):
    dp_count, chans, relay = dims[0], dims[4], dims[7]
    pieces = 2 * dp_count * relay
    return pl.pallas_call(
        functools.partial(compact_kernel, dims),
        out_shape=(
            jax.ShapeDtypeStruct((dp_count,), jnp.int32),
            jax.ShapeDtypeStruct((1,), jnp.int32),
            *([jax.ShapeDtypeStruct((pieces, CHUNK, chans), BF16)] if relay else ()),
        ),
        in_specs=[smem(), *[anywhere()] * len(relays)],
        out_specs=(smem(), smem(), *([vmem()] if relay else ())),
        scratch_shapes=[pltpu.SemaphoreType.DMA((pieces,))] if relay else [],
        name="compact",
    )(params, *relays)


class Scatter:
    def __init__(self, place, first, lines, partial, result, halves, dp_send, dp_got, chip_send, chip_got, *semaphores):
        self.place, self.lines = place, pl.ds(first, lines)
        self.partial, self.result, self.halves = partial, result, halves
        self.dp_send, self.dp_got, self.chip_send, self.chip_got = dp_send, dp_got, chip_send, chip_got
        core_sent, core_landed, dp_sent, dp_landed, chip_sent, chip_landed = semaphores
        self.core = remote(
            partial.at[self.lines, :, :, 1 - place.core],
            halves,
            core_sent.at[0],
            core_landed.at[0],
            (place.dp, place.bin + 1 - 2 * place.core),
        )
        self.dp_copies, self.chip_copies = [], []
        for apart in range(1, place.dp_count):
            to = lax.rem(place.dp + apart, place.dp_count)
            self.dp_copies.append(
                remote(
                    dp_send.at[to],
                    dp_got.at[apart - 1],
                    dp_sent.at[apart - 1],
                    dp_landed.at[apart - 1],
                    (to, place.bin),
                )
            )
        for apart in range(1, place.chip_count):
            to = lax.rem(place.chip + apart, place.chip_count)
            self.chip_copies.append(
                remote(
                    chip_send.at[to],
                    chip_got.at[apart - 1],
                    chip_sent.at[apart - 1],
                    chip_landed.at[apart - 1],
                    (place.dp, to * 2 + place.core),
                )
            )

    def start_core(self):
        self.core.start()

    def core_to_dp(self):
        self.core.wait()
        for target in range(self.place.dp_count):
            for chip in range(self.place.chip_count):
                both = self.partial[self.lines, target, chip, self.place.core] + self.halves[:, target, chip]
                self.halves[:, target, chip] = both
                self.dp_send[target, chip] = both.reshape(self.dp_send.shape[2:]).astype(BF16)
        for copy in self.dp_copies:
            copy.start()

    def dp_to_chip(self):
        for copy in self.dp_copies:
            copy.wait()
        for chip in range(self.place.chip_count):
            total = self.halves[:, self.place.dp, chip].reshape(self.dp_send.shape[2:])
            for apart in range(1, self.place.dp_count):
                total += self.dp_got[apart - 1, chip].astype(F32)
            self.halves[:, 0, chip] = total.reshape(self.halves[:, 0, chip].shape)
            self.chip_send[chip] = total.astype(BF16)
        for copy in self.chip_copies:
            copy.start()

    def finish(self):
        for copy in self.chip_copies:
            copy.wait()
        total = self.halves[:, 0, self.place.chip]
        for apart in range(1, self.place.chip_count):
            total += self.chip_got[apart - 1].astype(F32).reshape(total.shape)
        self.result[self.lines] = total

    @staticmethod
    def scratch(dims, lines):
        dp_count, bin_count, seqs, rows, chans, feats, base, relay = dims
        chips, dma = bin_count // 2, pltpu.SemaphoreType.DMA
        quarter = chans // (dp_count * bin_count)
        return [
            pltpu.VMEM((lines, dp_count, chips, quarter, feats), F32),
            pltpu.VMEM((dp_count, chips, lines * quarter, feats), BF16),
            pltpu.VMEM((dp_count, chips, lines * quarter, feats), BF16),
            pltpu.VMEM((chips, lines * quarter, feats), BF16),
            pltpu.VMEM((chips, lines * quarter, feats), BF16),
            dma((1,)),
            dma((1,)),
            dma((dp_count,)),
            dma((dp_count,)),
            dma((chips,)),
            dma((chips,)),
        ]


def scatters(dims):
    dp_count, bin_count, chans = dims[0], dims[1], dims[4]
    return chans % (dp_count * bin_count * 8) == 0


def backward_kernel(
    dims, meta, counts, crossed, moved_in, conv_in, w_in, stats_one, params_in, totals_two, cot, cot_near, cot_far, out_stage, *rest
):
    dp_count, bin_count, seqs, rows, chans, feats, base, relay = dims
    own_scatter = scatters(dims)
    (grads, low_edge, high_edge, landed_out, sums_two_out, sums_one_out, result) = rest[:7]
    if relay:
        landed_relay = rest[7]
        (relayed, home_cot, home_out, relay_own) = rest[-8:-4]
        (relay_cot_sent, relay_cot_landed, relay_out_sent, relay_out_landed) = rest[-4:]
        rest = rest[:7] + rest[8:-8]
    (cots, moved, conv, w, chosen) = rest[7:12]
    (scale_one, offset_one, inverse_one, shift_one, scale_two, offset_two, inverse_two, shift_two) = rest[12:20]
    (grad_two, grad_one, hidden_two, hidden_one, windows) = rest[20:25]
    (sums_two, sums_one, bias_sum, line_two, rest_two, line_one, rest_one) = rest[25:32]
    (send_left, send_right, from_left, from_right, last_left, last_right, last_from_left, last_from_right) = rest[32:40]
    reduce_two = rest[40:47]
    reduce_one = rest[47:54]
    (local, halo_sent, halo_landed, last_sent, last_landed, out_sent, out_landed) = rest[54:61]
    partial = result
    place = Place(dp_count, bin_count)
    per_slot = rows // CHUNK
    per_micro = seqs // MICRO
    loads = [
        pltpu.make_async_copy(conv_in, conv, local.at[0]),
        pltpu.make_async_copy(w_in, w, local.at[1]),
        pltpu.make_async_copy(cot, cots.at[0:seqs], local.at[2]),
        pltpu.make_async_copy(cot_near, cots.at[seqs : seqs + base], local.at[3]),
        pltpu.make_async_copy(cot_far, cots.at[seqs + base + relay : 2 * seqs], local.at[4]),
        pltpu.make_async_copy(moved_in, moved, local.at[5]),
    ]
    for load in loads:
        load.start()
    if own_scatter:
        partial = rest[61]
        proj_scatter = Scatter(place, TAPS, 1, partial, result, *rest[62:73])
        conv_scatter = Scatter(place, 0, TAPS, partial, result, *rest[73:84])
    place.barrier()
    stream = Stream(place, out_stage, landed_out, out_sent, out_landed, base * per_slot)
    stream.pump(BACK_PUMPS[10])
    cot_relays, out_relays = [], []
    if relay:
        for column, (begin, held) in enumerate(starts(counts, dims)):
            for slot in range(relay):
                at = 2 * jnp.minimum(begin + slot, dp_count * relay - 1)
                home_cot[column, slot] = crossed[at]
                home_out[column, slot] = crossed[at + 1]
        spot = lambda own: pl.ds(pl.multiple_of(own * CHUNK, CHUNK), CHUNK)
        cot_relays = to_columns(
            place, home_cot, lambda own: relayed.at[:, spot(own)], relay_own.at[0], relay_cot_sent, relay_cot_landed
        )
    count = float(per_micro * rows * dp_count * bin_count)
    params = params_in[...]
    norm_rows(stats_one[...], (params[0:1], params[1:2]), count, scale_one, offset_one, inverse_one, shift_one)
    norm_rows(
        totals_two[...],
        (params[3:4, :feats], params[3:4, feats : 2 * feats]),
        count,
        scale_two,
        offset_two,
        inverse_two,
        shift_two,
    )
    sums_two[...] = jnp.zeros_like(sums_two)
    sums_one[...] = jnp.zeros_like(sums_one)
    bias_sum[...] = jnp.zeros_like(bias_sum)
    for load in loads[:5]:
        load.wait()

    def head(i, late):
        micro = i // per_micro
        inner = pl.ds(pl.multiple_of(lax.rem(i, per_micro) * rows, rows), rows)
        cotangent = cots[meta[3, i]]
        if late and relay:
            place_in = meta[4, i] - base
            other = relayed[jnp.clip(place_in, 0, relay - 1)]
            cotangent = jnp.where((meta[0, i] > 0) & (place_in >= 0) & (place_in < relay), other, cotangent)
        chosen[micro, inner] = cotangent
        bias_sum[...] += eighth(cotangent.astype(F32))
        values = conv[i]
        hidden, slope = gelu_both(values * scale_two[micro] + offset_two[micro])
        hidden_two[micro, inner] = hidden.astype(BF16)
        grad = matmul(cotangent, w[TAPS], 1, 0) * slope
        grad_two[i] = grad
        sums_two[micro] += eighth(grad)
        sums_two[MICRO + micro] += eighth(grad * values)

    stream.loop(base, lambda i: head(i, False), BACK_PUMPS[0])
    for copy in cot_relays:
        copy.wait()
    stream.loop(seqs - base, lambda i: head(i + base, True), BACK_PUMPS[9])
    mine = reduce_two[0]
    mine[0 : 2 * MICRO] = jnp.sum(sums_two[...], axis=1)
    bias_row = jnp.sum(bias_sum[...], axis=0, keepdims=True)
    spare = jnp.zeros((1, feats), F32)
    for part in range(2 * MICRO):
        begin = part * feats
        mine[2 * MICRO + part : 2 * MICRO + part + 1] = bias_row[:, begin : begin + feats] if begin < chans else spare
    reduce = AllReduce(place, *reduce_two)
    reduce.start_near()
    stream.pump(BACK_PUMPS[1])

    def weigh(line, terms):
        total = None
        for left, right in terms:
            term = matmul(left, right, 0, 0)
            total = term if total is None else total + term
        partial[line] = total.reshape(partial.shape[1:])

    def proj_terms(micros):
        return [(chosen[micro], hidden_two[micro]) for micro in micros]

    reduce.finish_near()
    reduce.start_far()
    stream.pump(BACK_PUMPS[2])
    if relay:
        out_relays = to_columns(
            place, home_out, lambda own: landed_relay.at[:, spot(own)], relay_own.at[1], relay_out_sent, relay_out_landed
        )
    weigh(TAPS, proj_terms(range(MICRO)))
    if own_scatter:
        proj_scatter.start_core()
    back_two = reduce.finish_far()

    def lines(back, scale, inverse, shift, line, remainder, out):
        for micro in range(MICRO):
            plain = back[micro : micro + 1]
            centred = inverse[micro] * back[MICRO + micro : MICRO + micro + 1] + shift[micro] * plain
            out[micro : micro + 1] = plain
            out[MICRO + micro : MICRO + micro + 1] = centred
            line[micro] = -scale[micro] * inverse[micro] * (centred / count)
            remainder[micro] = -scale[micro] * (plain / count + shift[micro] * (centred / count))

    lines(back_two, scale_two, inverse_two, shift_two, line_two, rest_two, sums_two_out)
    sums_two_out[2 * MICRO :] = back_two[2 * MICRO :]

    def conv_gradient(i, begin, size):
        micro = i // per_micro
        span = slice(begin, begin + size)
        value = scale_two[micro] * grad_two[i, span] + line_two[micro] * conv[i, span] + rest_two[micro]
        return value.astype(BF16).astype(F32)

    def edges(i):
        reverse = meta[0, i]
        top, bottom = conv_gradient(i, 0, DILATION), conv_gradient(i, rows - DILATION, DILATION)
        send_left[i] = jnp.where(reverse > 0, bottom, top)
        send_right[i] = jnp.where(reverse > 0, top, bottom)

    lax.fori_loop(0, seqs, lambda i, carry: (edges(i), carry)[1], 0)
    halo = Halo(place, send_left, send_right, from_left, from_right, halo_sent, halo_landed)
    halo.start()
    stream.pump(BACK_PUMPS[3])
    if own_scatter:
        proj_scatter.core_to_dp()
    loads[5].wait()
    halo.finish()

    def tail(i):
        micro = i // per_micro
        inner = pl.ds(pl.multiple_of(lax.rem(i, per_micro) * rows, rows), rows)
        reverse = meta[0, i]
        left, right = from_left[i], from_right[i]
        low = jnp.where(reverse > 0, right, left)
        high = jnp.where(reverse > 0, left, right)
        full = jnp.concatenate([low, conv_gradient(i, 0, rows), high], axis=0)
        grad = None
        for tap in range(TAPS):
            begin = (TAPS - 1 - tap) * DILATION
            window = full[begin : begin + rows].astype(BF16)
            windows[micro, inner, tap * feats : (tap + 1) * feats] = window
            term = matmul(window, w[tap], 1, 1)
            grad = term if grad is None else grad + term
        values = moved[i].astype(F32)
        hidden, slope = gelu_both(values * scale_one[micro] + offset_one[micro])
        hidden_one[micro, inner] = hidden.astype(BF16)
        grad = grad * slope
        grad_one[i] = grad
        sums_one[micro] += eighth(grad)
        sums_one[MICRO + micro] += eighth(grad * values)

    stream.loop(seqs, tail, BACK_PUMPS[4])
    mine = reduce_one[0]
    mine[...] = jnp.sum(sums_one[...], axis=1)
    reduce = AllReduce(place, *reduce_one)
    reduce.start_near()
    if own_scatter:
        proj_scatter.dp_to_chip()
    stream.pump(BACK_PUMPS[5])

    def conv_weigh(micros, add):
        total = None
        for micro in micros:
            term = matmul(hidden_one[micro], windows[micro], 0, 0)
            total = term if total is None else total + term
        for tap in range(TAPS):
            part = total[:, tap * feats : (tap + 1) * feats].reshape(partial.shape[1:])
            partial[tap] = partial[tap] + part if add else part

    conv_weigh(range(MICRO // 2), False)
    reduce.finish_near()
    reduce.start_far()
    stream.pump(BACK_PUMPS[6])
    conv_weigh(range(MICRO // 2, MICRO), True)
    if own_scatter:
        conv_scatter.start_core()
    back_one = reduce.finish_far()
    lines(back_one, scale_one, inverse_one, shift_one, line_one, rest_one, sums_one_out)
    if own_scatter:
        conv_scatter.core_to_dp()
        proj_scatter.finish()

    def end(i):
        micro = i // per_micro
        inner = pl.ds(pl.multiple_of(lax.rem(i, per_micro) * rows, rows), rows)
        reverse = meta[0, i]
        value = scale_one[micro] * grad_one[i] + line_one[micro] * moved[i].astype(F32) + rest_one[micro]
        value = chosen[micro, inner].astype(F32) + value
        grads[i] = value.astype(BF16)
        top, bottom = value[:LAST_EDGE].astype(BF16), value[rows - LAST_EDGE :].astype(BF16)
        last_left[i] = jnp.where(reverse > 0, bottom, top)
        last_right[i] = jnp.where(reverse > 0, top, bottom)

    stream.loop(seqs, end, BACK_PUMPS[7])
    last = Halo(place, last_left, last_right, last_from_left, last_from_right, last_sent, last_landed)
    last.start()
    stream.pump(BACK_PUMPS[8])
    if own_scatter:
        conv_scatter.dp_to_chip()
    last.finish()
    low_edge[...] = last_from_left[...]
    high_edge[...] = last_from_right[...]
    if own_scatter:
        conv_scatter.finish()
    for copy in out_relays:
        copy.wait()
    stream.finish()


def run_backward(dims, meta, counts, crossed, moved, conv, w, stats_one, params, totals_two, cot, cot_near, cot_far, out_stage):
    dp_count, bin_count, seqs, rows, chans, feats, base, relay = dims
    chips = bin_count // 2
    group = TAPS + 1
    quarter = chans // (dp_count * bin_count)
    own_scatter = scatters(dims)
    per_slot = rows // CHUNK
    held = seqs // MICRO * rows
    dma = pltpu.SemaphoreType.DMA
    wide = pltpu.VMEM((MICRO, 1, chans), F32)
    narrow = pltpu.VMEM((MICRO, 1, feats), F32)
    edge = jax.ShapeDtypeStruct((seqs, LAST_EDGE, chans), BF16)
    return pl.pallas_call(
        functools.partial(backward_kernel, dims),
        out_shape=(
            jax.ShapeDtypeStruct((seqs, rows, chans), BF16),
            edge,
            edge,
            jax.ShapeDtypeStruct((base * per_slot, CHUNK, chans), BF16),
            jax.ShapeDtypeStruct((4 * MICRO, feats), F32),
            jax.ShapeDtypeStruct((2 * MICRO, chans), F32),
            jax.ShapeDtypeStruct((group, quarter if own_scatter else chans, feats), F32),
            *([jax.ShapeDtypeStruct((relay, rows, chans), BF16)] if relay else ()),
        ),
        in_specs=[smem(), smem(), vmem(), *[anywhere()] * 3, *[vmem()] * 3, *[anywhere()] * 4],
        out_specs=(vmem(), vmem(), vmem(), anywhere(), vmem(), vmem(), vmem(), *([anywhere()] if relay else ())),
        scratch_shapes=[
            pltpu.VMEM((2 * seqs, rows, chans), BF16),
            pltpu.VMEM((seqs, rows, chans), BF16),
            pltpu.VMEM((seqs, rows, feats), F32),
            pltpu.VMEM((group, chans, feats), BF16),
            pltpu.VMEM((MICRO, held, chans), BF16),
            *[wide] * 4,
            *[narrow] * 4,
            pltpu.VMEM((seqs, rows, feats), F32),
            pltpu.VMEM((seqs, rows, chans), F32),
            pltpu.VMEM((MICRO, held, feats), BF16),
            pltpu.VMEM((MICRO, held, chans), BF16),
            pltpu.VMEM((MICRO, held, TAPS * feats), BF16),
            pltpu.VMEM((2 * MICRO, 8, feats), F32),
            pltpu.VMEM((2 * MICRO, 8, chans), F32),
            pltpu.VMEM((8, chans), F32),
            narrow,
            narrow,
            wide,
            wide,
            *[pltpu.VMEM((seqs, DILATION, feats), F32)] * 4,
            *[pltpu.VMEM((seqs, LAST_EDGE, chans), BF16)] * 4,
            *AllReduce.scratch(dp_count, bin_count, 4 * MICRO, feats),
            *AllReduce.scratch(dp_count, bin_count, 2 * MICRO, chans),
            dma((6,)),
            dma((2,)),
            dma((2,)),
            dma((2,)),
            dma((2,)),
            dma((base * per_slot,)),
            dma((base * per_slot,)),
            *(
                (
                    pltpu.VMEM((group, dp_count, chips, 2, quarter, feats), F32),
                    *Scatter.scratch(dims, 1),
                    *Scatter.scratch(dims, TAPS),
                )
                if own_scatter
                else ()
            ),
            *(
                [pltpu.VMEM((relay, rows, chans), BF16)]
                + [pltpu.VMEM((dp_count, relay, CHUNK, chans), BF16)] * 2
                + [dma((2,))]
                + [dma((dp_count,))] * 4
                if relay
                else ()
            ),
        ],
        compiler_params=pltpu.CompilerParams(
            collective_id=2, has_side_effects=True, vmem_limit_bytes=VMEM_LIMIT
        ),
        name="backward",
    )(meta, counts, crossed, moved, conv, w, stats_one, params, totals_two, cot, cot_near, cot_far, out_stage)


def last_kernel(dims, meta, back_one, back_two, *rest):
    dp_count, bin_count, seqs, rows, chans, feats, base, relay = dims
    own_scatter = scatters(dims)
    partial, rest = (rest[0], rest[1:]) if own_scatter else (None, rest)
    (grad, left, right, out, near), rest = rest[:5], rest[5:]
    relayed, rest = (rest[0], rest[1:]) if relay else (None, rest)
    (far, result_out, result_grad, gain_one, bias_one, gain_two, bias_two, bias_proj) = rest[:8]
    if own_scatter:
        conv_weight, proj_weight = rest[8:10]
        conv_weight[...] = partial[:TAPS]
        proj_weight[...] = partial[TAPS]
    (held, made, got, put) = rest[-4:]
    for i in range(seqs):
        reverse, slot = meta[0, i], meta[4, i]

        @pl.when(reverse == 0)
        def _():
            pltpu.make_async_copy(out.at[i], held.at[i], got.at[i]).start()

        @pl.when((reverse > 0) & (slot < base))
        def _():
            pltpu.make_async_copy(near.at[jnp.minimum(slot, base - 1)], held.at[i], got.at[i]).start()

        if relay:

            @pl.when((reverse > 0) & (slot >= base) & (slot < base + relay))
            def _():
                pltpu.make_async_copy(relayed.at[jnp.clip(slot - base, 0, relay - 1)], held.at[i], got.at[i]).start()

        @pl.when((reverse > 0) & (slot >= base + relay))
        def _():
            pltpu.make_async_copy(far.at[jnp.maximum(slot - base - relay, 0)], held.at[i], got.at[i]).start()

    across = rows + 2 * LAST_EDGE
    row = lax.broadcasted_iota(jnp.int32, (rows, across), 0)
    column = lax.broadcasted_iota(jnp.int32, (rows, across), 1)

    def step(i, carry):
        reverse, shift = meta[0, i], meta[1, i]
        low = jnp.where(reverse > 0, right[i], left[i])
        high = jnp.where(reverse > 0, left[i], right[i])
        source = jnp.concatenate([low, grad[i], high], axis=0)
        place = jnp.where(reverse > 0, rows - 1 - row - shift, row + shift) + LAST_EDGE
        pick = jnp.where(column == place, 1.0, 0.0).astype(BF16)
        made[i] = matmul(pick, source, 1, 0).astype(BF16)
        pltpu.make_async_copy(made.at[i], result_grad.at[i], put.at[0]).start()
        pltpu.make_async_copy(held.at[i], held.at[i], got.at[i]).wait()
        pltpu.make_async_copy(held.at[i], result_out.at[i], put.at[1]).start()
        return carry

    lax.fori_loop(0, seqs, step, 0)
    dp, bins = lax.axis_index("dp"), lax.axis_index("bins")

    def own(values, index, result):
        width, share = values.shape[1], result.shape[1]
        begin = index * share
        result[...] = pltpu.roll(values, lax.rem(width - begin, width), 1)[:, :share]

    def summed(back, begin):
        return jnp.sum(back[begin : begin + MICRO], axis=0, keepdims=True)

    wide, narrow = dp * bin_count + bins, bins
    own(summed(back_one, MICRO), wide, gain_one)
    own(summed(back_one, 0), wide, bias_one)
    own(summed(back_two, MICRO), narrow, gain_two)
    own(summed(back_two, 0), narrow, bias_two)
    bias = jnp.concatenate([back_two[2 * MICRO + k : 2 * MICRO + k + 1] for k in range(chans // feats)], axis=1)
    own(bias, wide, bias_proj)
    pltpu.make_async_copy(made, result_grad, put.at[0]).wait()
    pltpu.make_async_copy(held, result_out, put.at[1]).wait()


def run_last(dims, meta, back_one, back_two, partial, grad, left, right, out, near, relayed, far):
    dp_count, bin_count, seqs, rows, chans, feats, base, relay = dims
    own_scatter = scatters(dims)
    big = jax.ShapeDtypeStruct((seqs, rows, chans), BF16)
    quarter = chans // (dp_count * bin_count)
    wide = jax.ShapeDtypeStruct((1, quarter), F32)
    narrow = jax.ShapeDtypeStruct((1, feats // bin_count), F32)
    weights = (
        jax.ShapeDtypeStruct((TAPS, quarter, feats), F32),
        jax.ShapeDtypeStruct((quarter, feats), F32),
    )
    partials = [partial] if own_scatter else []
    return pl.pallas_call(
        functools.partial(last_kernel, dims),
        out_shape=(big, big, wide, wide, narrow, narrow, wide, *(weights if own_scatter else ())),
        in_specs=[
            smem(),
            *[vmem()] * (5 + len(partials)),
            *[anywhere()] * (3 + len(relayed)),
        ],
        out_specs=(anywhere(), anywhere(), *[vmem()] * (7 if own_scatter else 5)),
        scratch_shapes=[
            pltpu.VMEM(big.shape, BF16),
            pltpu.VMEM(big.shape, BF16),
            pltpu.SemaphoreType.DMA((seqs,)),
            pltpu.SemaphoreType.DMA((2,)),
        ],
        compiler_params=pltpu.CompilerParams(vmem_limit_bytes=VMEM_LIMIT),
        name="last",
    )(meta, back_one, back_two, *partials, grad, left, right, out, near, *relayed, far)


def local(
    activations,
    shift_bins,
    reverse_flags,
    gain_one,
    bias_one,
    conv_weight,
    gain_two,
    bias_two,
    proj_weight,
    proj_bias,
    cotangent,
):
    seqs, rows, chans = activations.shape
    feats = conv_weight.shape[2]
    dp_count, bin_count = lax.axis_size("dp"), lax.axis_size("bins")
    per_slot = rows // CHUNK
    base = BASE_SLOTS
    relay = RELAY_SLOTS if per_slot == dp_count else 0
    dims = (dp_count, bin_count, seqs, rows, chans, feats, base, relay)

    vectors = [vector[None] for vector in (gain_one, bias_one, proj_bias, gain_two, bias_two)]
    shard = jnp.concatenate([conv_weight, proj_weight.T[None]], axis=0)

    (
        moved,
        conv,
        out,
        out_stage,
        out_extra,
        cot_extra,
        cot_near,
        w,
        stats_one,
        params,
        totals_two,
        meta,
        *relays,
    ) = run_front(
        dims,
        reverse_flags,
        shift_bins,
        activations,
        cotangent.reshape(seqs * per_slot, CHUNK, chans),
        shard,
        vectors,
    )
    counts, choice, *packed = run_compact(dims, params, *relays)
    pairs = [(source, bin_count - 1 - source) for source in range(bin_count)]
    direct = seqs - base - relay
    pieces = 2 * dp_count * relay

    def crossing(relayed, slots, packed, pair):
        moving = [packed[: 2 * relayed]] * (relayed > 0)
        moving += [item[: slots * per_slot] for item in pair] * (slots > 0)
        if not moving:
            return packed, *pair
        got = lax.ppermute(jnp.concatenate(moving), "bins", pairs)
        put = lax.dynamic_update_slice_in_dim
        if relayed:
            packed = put(packed, got[: 2 * relayed], 0, 0)
        if slots:
            held = slots * per_slot
            rest = got[2 * relayed :]
            pair = tuple(put(item, rest[k * held : (k + 1) * held], 0, 0) for k, item in enumerate(pair))
        return packed, *pair

    every = pieces // 2
    branches = [functools.partial(crossing, held, 0) for held in range(every + 1)]
    for slots in range(1, direct + 1):
        branches += [functools.partial(crossing, held, slots) for held in (every // 2, every)]
    packed = packed[0] if relay else jnp.zeros((1, CHUNK, chans), BF16)
    crossed, cot_far, out_far = lax.switch(choice[0], branches, packed, (cot_extra, out_extra))

    slots_of = lambda item: item.reshape(-1, rows, chans)
    grads, low_edge, high_edge, out_near, back_two, back_one, partial, *landed = run_backward(
        dims,
        meta,
        counts,
        crossed,
        moved,
        conv,
        w,
        stats_one,
        params,
        totals_two,
        cotangent,
        slots_of(cot_near),
        slots_of(cot_far),
        out_stage,
    )
    output, grad_activations, gain_one, bias_one, gain_two, bias_two, bias_proj, *weights = run_last(
        dims,
        meta,
        back_one,
        back_two,
        partial,
        grads,
        low_edge,
        high_edge,
        out,
        slots_of(out_near),
        landed,
        slots_of(out_far),
    )
    if not weights:
        scattered = lax.psum_scatter(partial, ("dp", "bins"), scatter_dimension=1, tiled=True)
        weights = scattered[:TAPS], scattered[TAPS]
    return (
        output,
        grad_activations,
        gain_one[0],
        bias_one[0],
        weights[0],
        gain_two[0],
        bias_two[0],
        weights[1].T,
        bias_proj[0],
    )


def solution(mesh):
    placed = (
        P("dp", "bins", None),
        P("dp"),
        P("dp"),
        P("bins"),
        P("bins"),
        P(None, "bins", None),
        P("bins"),
        P("bins"),
        P(None, "bins"),
        P("bins"),
        P("dp", "bins", None),
    )
    return jax.shard_map(
        local,
        mesh=mesh,
        in_specs=placed,
        out_specs=(
            P("dp", "bins", None),
            P("dp", "bins", None),
            P(("dp", "bins")),
            P(("dp", "bins")),
            P(None, ("dp", "bins"), None),
            P("bins"),
            P("bins"),
            P(None, ("dp", "bins")),
            P(("dp", "bins")),
        ),
        check_vma=False,
    )
```

```python
import functools

import jax
import jax.numpy as jnp
from jax import lax
from jax.experimental import pallas as pl
from jax.experimental.pallas import tpu as pltpu
from jax.sharding import PartitionSpec as P

TAPS = 3
DILATION = 8
MICRO = 4
EPSILON = 1e-05
CHUNK = 32
EARLY = 8
BASE_SLOTS = 8
RELAY_SLOTS = 4
PUMPS = (0, 2, 10, 0, 3, 3, 0, 18, 0, 0)
BACK_PUMPS = (2, 1, 4, 6, 4, 1, 6, 2, 32, 2, 3)
WINDOW = 32
EDGE = 16
LAST_EDGE = 8
VMEM_LIMIT = 60 * 1024 * 1024
MESH = pl.DeviceIdType.MESH
F32 = jnp.float32
BF16 = jnp.bfloat16
ROOT = 0.7978845608028654
CUBE = 0.044715


def vmem():
    return pl.BlockSpec(memory_space=pltpu.VMEM)


def smem():
    return pl.BlockSpec(memory_space=pltpu.SMEM)


def anywhere():
    return pl.BlockSpec(memory_space=pl.ANY)


def matmul(a, b, ca, cb):
    return lax.dot_general(a, b, (((ca,), (cb,)), ((), ())), preferred_element_type=F32)


class Place:
    def __init__(self, dp_count, bin_count):
        self.dp_count, self.bin_count = dp_count, bin_count
        self.chip_count = bin_count // 2
        self.dp = lax.axis_index("dp")
        self.bin = lax.axis_index("bins")
        self.chip = self.bin // 2
        self.core = lax.rem(self.bin, 2)

    def greet(self):
        semaphore = pltpu.get_barrier_semaphore()
        for apart in range(1, self.bin_count):
            other = (self.dp, lax.rem(self.bin + apart, self.bin_count))
            pl.semaphore_signal(semaphore, inc=1, device_id=other, device_id_type=MESH)
        for apart in range(1, self.dp_count):
            for core in range(2):
                other = (lax.rem(self.dp + apart, self.dp_count), self.chip * 2 + core)
                pl.semaphore_signal(semaphore, inc=1, device_id=other, device_id_type=MESH)

    def meet(self):
        pl.semaphore_wait(
            pltpu.get_barrier_semaphore(), self.bin_count - 1 + 2 * (self.dp_count - 1)
        )


def remote(source, target, sent, landed, device):
    return pltpu.make_async_remote_copy(
        src_ref=source,
        dst_ref=target,
        send_sem=sent,
        recv_sem=landed,
        device_id=device,
        device_id_type=MESH,
    )


class Stream:
    def __init__(self, place, source, target, sent, landed, count):
        self.source, self.target, self.sent, self.landed = source, target, sent, landed
        self.count, self.next = count, 0
        self.device = (place.dp, place.bin_count - 1 - place.bin)

    def piece(self, index):
        return remote(
            self.source.at[index],
            self.target.at[index],
            self.sent.at[index],
            self.landed.at[index],
            self.device,
        )

    def pump(self, pieces=1):
        for _ in range(pieces):
            if self.next >= self.count:
                return
            if self.next >= WINDOW:
                self.piece(self.next - WINDOW).wait_send()
            self.piece(self.next).start()
            self.next += 1

    def loop(self, trips, body, pieces):
        pieces = max(0, min(pieces, self.count - self.next, trips))
        if pieces == 0 or self.next < WINDOW and self.next + pieces <= WINDOW:
            first, every = self.next, trips // max(pieces, 1)

            def plain(i, carry):
                body(i)
                done = lax.div(i, every)
                if pieces:

                    @pl.when((lax.rem(i, every) == 0) & (done < pieces))
                    def _():
                        self.piece(first + done).start()

                return carry

            lax.fori_loop(0, trips, plain, 0)
            self.next += pieces
            return
        if pieces == 0:
            lax.fori_loop(0, trips, lambda i, carry: (body(i), carry)[1], 0)
            return
        if self.next < WINDOW:
            self.pump(WINDOW - self.next)
            pieces = max(0, min(pieces, self.count - self.next))
        first = self.next
        every = trips // max(pieces, 1)

        def step(i, carry):
            body(i)
            done = lax.div(i, every)

            @pl.when((lax.rem(i, every) == 0) & (done < pieces))
            def _():
                self.piece(first + done - WINDOW).wait_send()
                self.piece(first + done).start()

            return carry

        lax.fori_loop(0, trips, step, 0)
        self.next = first + pieces

    def finish(self):
        self.pump(self.count)
        for index in range(max(0, self.count - WINDOW), self.count):
            self.piece(index).wait_send()
        for index in range(self.count):
            self.piece(index).wait_recv()


class AllReduce:
    def __init__(self, place, mine, near, far, near_sent, near_landed, far_sent, far_landed):
        self.place, self.mine, self.near, self.far = place, mine, near, far
        self.near_count = place.dp_count * 2
        self.me = place.dp * 2 + place.core
        self.near_copies = []
        for apart in range(1, self.near_count):
            to = lax.rem(self.me + apart, self.near_count)
            device = (to // 2, place.chip * 2 + lax.rem(to, 2))
            self.near_copies.append(
                remote(mine, near.at[apart - 1], near_sent.at[apart - 1], near_landed.at[apart - 1], device)
            )
        self.far_copies = []
        for apart in range(1, place.chip_count):
            to = lax.rem(place.chip + apart, place.chip_count)
            device = (place.dp, to * 2 + place.core)
            self.far_copies.append(
                remote(
                    near.at[self.near_count - 1],
                    far.at[apart - 1],
                    far_sent.at[apart - 1],
                    far_landed.at[apart - 1],
                    device,
                )
            )

    def start_near(self):
        for copy in self.near_copies:
            copy.start()

    def finish_near(self):
        for copy in self.near_copies:
            copy.wait()
        count = self.near_count

        total = None
        for member in range(count):
            apart = lax.rem(self.me - member + count, count)
            other = self.near[jnp.maximum(apart - 1, 0)]
            part = jnp.where(apart == 0, self.mine[...], other)
            total = part if total is None else total + part
        self.near[count - 1] = total

    def start_far(self):
        for copy in self.far_copies:
            copy.start()

    def finish_far(self):
        for copy in self.far_copies:
            copy.wait()
        count = self.place.chip_count
        total = None
        for member in range(count):
            apart = lax.rem(self.place.chip - member + count, count)
            part = jnp.where(
                apart == 0, self.near[self.near_count - 1], self.far[jnp.maximum(apart - 1, 0)]
            )
            total = part if total is None else total + part
        return total

    @staticmethod
    def scratch(dp_count, bin_count, rows, width):
        near, far = dp_count * 2, bin_count // 2
        return [
            pltpu.VMEM((rows, width), F32),
            pltpu.VMEM((near, rows, width), F32),
            pltpu.VMEM((far, rows, width), F32),
            pltpu.SemaphoreType.DMA((near,)),
            pltpu.SemaphoreType.DMA((near,)),
            pltpu.SemaphoreType.DMA((far,)),
            pltpu.SemaphoreType.DMA((far,)),
        ]


class Halo:
    def __init__(self, place, to_left, to_right, from_left, from_right, sent, landed):
        self.place, self.from_left, self.from_right = place, from_left, from_right
        count = place.bin_count
        self.right = remote(
            to_right, from_left, sent.at[0], landed.at[0], (place.dp, lax.rem(place.bin + 1, count))
        )
        self.left = remote(
            to_left, from_right, sent.at[1], landed.at[1], (place.dp, lax.rem(place.bin + count - 1, count))
        )
        self.first = place.bin == 0
        self.last = place.bin == count - 1

    def start(self):
        @pl.when(jnp.logical_not(self.last))
        def _():
            self.right.start()

        @pl.when(jnp.logical_not(self.first))
        def _():
            self.left.start()

        @pl.when(self.first)
        def _():
            self.from_left[...] = jnp.zeros_like(self.from_left)

        @pl.when(self.last)
        def _():
            self.from_right[...] = jnp.zeros_like(self.from_right)

    def finish(self):
        @pl.when(jnp.logical_not(self.last))
        def _():
            self.right.wait_send()
            self.left.wait_recv()

        @pl.when(jnp.logical_not(self.first))
        def _():
            self.left.wait_send()
            self.right.wait_recv()


def eighth(values):
    rows, width = values.shape
    return jnp.sum(values.reshape(rows // 8, 8, width), axis=0)


def norm_rows(totals, gains, count, scale_ref, offset_ref, inverse_ref, shift_ref):
    for micro in range(MICRO):
        mean = totals[micro : micro + 1] / count
        second = totals[MICRO + micro : MICRO + micro + 1] / count
        inverse = lax.rsqrt(second - mean * mean + EPSILON)
        scale = inverse * gains[0]
        scale_ref[micro] = scale
        offset_ref[micro] = gains[1] - mean * scale
        if inverse_ref is not None:
            inverse_ref[micro] = inverse
            shift_ref[micro] = -mean * inverse


def gelu(v):
    half = 0.5 * v
    return half + half * jnp.tanh(v * (ROOT + (ROOT * CUBE) * (v * v)))


def gelu_both(v):
    square = v * v
    p = 0.5 + 0.5 * jnp.tanh(v * (ROOT + (ROOT * CUBE) * square))
    value = v * p
    slope = p + value * (1.0 - p) * ((2.0 * ROOT) + (6.0 * ROOT * CUBE) * square)
    return value, slope


def to_columns(place, source, target, own, sent, landed):
    copies = []
    for apart in range(1, place.dp_count):
        to = lax.rem(place.dp + apart, place.dp_count)
        copies.append(
            remote(
                source.at[to], target(place.dp), sent.at[apart - 1], landed.at[apart - 1], (to, place.bin)
            )
        )
        copies[-1].start()
    copies.append(pltpu.make_async_copy(source.at[place.dp], target(place.dp), own))
    copies[-1].start()
    return copies


def front_kernel(dims, flags, shifts, x_in, cot_in, shard, *rest):
    dp_count, bin_count, seqs, rows, chans, feats, base, relay = dims
    vectors, rest = rest[:5], rest[5:]
    (moved_out, conv_out, out_out, out_stage, out_extra, cot_extra, landed_cot, weights_out) = rest[:8]
    (stats_out, params_out, totals_two) = rest[8:11]
    meta, rest = rest[11], rest[:11] + rest[12:]
    if relay:
        relay_cot, relay_out = rest[11:13]
        rest = rest[:11] + rest[13:]
    (x, x_low, x_high, hidden_all, moved, conv, out, w, stage) = rest[11:20]
    direct = direct_weights(dims)
    weights = w if direct else weights_out
    (sums_one, sums, scale_one, offset_one, scale_two, offset_two) = rest[20:26]
    reduce_first = rest[26:33]
    reduce_second = rest[33:40]
    (local, stores, halo_sent, halo_landed, one_sent, one_landed, two_sent, two_landed, three_sent, three_landed) = rest[40:50]
    cot_sent, cot_landed = rest[50:52]
    (line_out, lines, count_out, count_all, line_sent, line_landed, count_sent, count_landed) = rest[-9:-1]
    cot = rest[-1]
    place = Place(dp_count, bin_count)
    per_slot = rows // CHUNK
    per_micro = seqs // MICRO
    if relay:
        (over_cot, over_out, relay_own) = rest[52:55]
        (relay_cot_sent, relay_cot_landed, relay_out_sent, relay_out_landed) = rest[55:59]
    share = chans // bin_count
    group = TAPS + 1
    total_bins = rows * bin_count
    place.greet()
    load = pltpu.make_async_copy(x_in, x, local.at[0])
    load.start()
    load_cot = pltpu.make_async_copy(cot_in, cot, local.at[3])
    load_cot.start()
    tap = lax.rem(place.dp, group)
    home = pl.ds(pl.multiple_of(place.bin * share, 8), share)
    keep = pltpu.make_async_copy(shard.at[tap], weights.at[tap, home], local.at[1])
    keep.start()
    reversed_count = jnp.int32(0)
    origins = [jnp.int32(0)] * seqs
    for i in range(seqs):
        reverse = jnp.where(flags[i] > 0, 1, 0)
        meta[0, i] = reverse
        meta[1, i] = shifts[i]
        for slot in range(i + 1):
            origins[slot] = jnp.where((reverse > 0) & (reversed_count == slot), i, origins[slot])
        slot = reverse * reversed_count
        meta[3, i] = jnp.where(reverse > 0, seqs + slot, i)
        meta[4, i] = slot
        reversed_count += reverse
    for slot in range(seqs):
        meta[2, slot] = origins[slot]
    place.meet()

    ones = []
    for apart in range(1, place.chip_count):
        to = lax.rem(place.chip + apart, place.chip_count)
        ones.append(
            remote(
                shard.at[tap],
                weights.at[tap, home],
                one_sent.at[apart - 1],
                one_landed.at[apart - 1],
                (place.dp, to * 2 + place.core),
            )
        )
        ones[-1].start()
    pieces = [vector[...].astype(F32) for vector in vectors]
    wide = sum(piece.shape[1] for piece in pieces)
    if wide < chans:
        pieces.append(jnp.zeros((1, chans - wide), F32))
    line_out[...] = jnp.concatenate(pieces, axis=1)
    lines[place.bin] = line_out[...]
    count_out[...] = jnp.zeros_like(count_out) + reversed_count.astype(F32)
    count_all[place.dp] = count_out[...]
    smalls = []
    for apart in range(1, bin_count):
        to = lax.rem(place.bin + apart, bin_count)
        smalls.append(
            remote(line_out, lines.at[place.bin], line_sent.at[apart - 1], line_landed.at[apart - 1], (place.dp, to))
        )
    for apart in range(1, dp_count):
        to = lax.rem(place.dp + apart, dp_count)
        smalls.append(
            remote(
                count_out,
                count_all.at[place.dp],
                count_sent.at[apart - 1],
                count_landed.at[apart - 1],
                (to, place.bin),
            )
        )
    for copy in smalls:
        copy.start()
    halo = Halo(
        place, x_in.at[:, 0:EDGE], x_in.at[:, rows - EDGE : rows], x_low, x_high, halo_sent, halo_landed
    )
    halo.start()
    load_cot.wait()
    for slot in range(base):
        origin = meta[2, slot] * per_slot
        for piece in range(per_slot):
            stage[slot * per_slot + piece] = cot[origin + piece]
    stream = Stream(place, stage, landed_cot, cot_sent, cot_landed, base * per_slot)
    load.wait()

    sums_one[...] = jnp.zeros_like(sums_one)
    row = lax.broadcasted_iota(jnp.int32, (rows, 1), 0) + place.bin * rows

    def statistics(i):
        micro = i // per_micro
        target = row + meta[1, i]
        inside = jnp.where((target >= 0) & (target < total_bins), 1.0, 0.0).astype(F32)
        values = x[i].astype(F32) * inside
        sums_one[micro] += eighth(values)
        sums_one[MICRO + micro] += eighth(values * values)

    stream.loop(seqs, statistics, PUMPS[0])
    mine = reduce_first[0]
    mine[...] = jnp.sum(sums_one[...], axis=1)
    reduce = AllReduce(place, *reduce_first)
    reduce.start_near()
    keep.wait()
    for copy in ones:
        copy.wait()
    twos = []
    for apart in range(1, group):
        to = (place.dp // group) * group + lax.rem(tap + apart, group)
        for chip in range(place.chip_count):
            part = weights.at[tap, pl.ds(pl.multiple_of((chip * 2 + place.core) * share, 8), share)]
            index = (apart - 1) * place.chip_count + chip
            twos.append(remote(part, part, two_sent.at[index], two_landed.at[index], (to, place.bin)))
            twos[-1].start()
    stream.pump(PUMPS[1])
    for slot in range(base, seqs):
        origin = meta[2, slot] * per_slot
        for piece in range(per_slot):
            if slot < base + relay:
                over_cot[piece, slot - base] = cot[origin + piece]
            else:
                cot_extra[(slot - base - relay) * per_slot + piece] = cot[origin + piece]
    reduce.finish_near()
    reduce.start_far()
    stream.pump(PUMPS[2])
    relays = []
    if relay:
        relays += to_columns(
            place, over_cot, lambda own: relay_cot.at[own], relay_own.at[0], relay_cot_sent, relay_cot_landed
        )
    long_rows = rows + 2 * DILATION
    across = rows + 2 * EDGE
    local_row = lax.broadcasted_iota(jnp.int32, (long_rows, across), 0) - DILATION
    column = lax.broadcasted_iota(jnp.int32, (long_rows, across), 1)
    edge_row = lax.broadcasted_iota(jnp.int32, (DILATION, 1), 0)

    halo.finish()

    def shift_rows(i):
        reverse, shift = meta[0, i], meta[1, i]
        direction = 1 - 2 * reverse
        begin = reverse * (rows - 1)
        pick = jnp.where(column == local_row * direction + (begin - shift + EDGE), 1.0, 0.0).astype(BF16)
        source = jnp.concatenate([x_low[i], x[i], x_high[i]], axis=0)
        shifted = matmul(pick, source, 1, 0)
        hidden_all[i] = shifted.astype(BF16)
        moved[i] = shifted[DILATION : DILATION + rows].astype(BF16)
        pltpu.make_async_copy(moved.at[i], moved_out.at[i], stores.at[0]).start()

    lax.fori_loop(0, seqs, lambda i, carry: (shift_rows(i), carry)[1], 0)
    first = reduce.finish_far()
    stats_out[...] = first
    for copy in smalls:
        copy.wait()
    params_out[...] = jnp.zeros_like(params_out)
    begin = 0
    for index, (line, offset, width) in enumerate(
        ((0, 0, share), (1, 0, share), (2, 0, share), (3, 0, share // 2), (3, feats, share // 2))
    ):
        for member in range(bin_count):
            left = offset + member * width
            params_out[line : line + 1, left : left + width] = lines[member, :, begin : begin + width]
        begin += width
    lane = lax.broadcasted_iota(jnp.int32, (1, chans), 1)
    held = jnp.zeros((1, chans), F32)
    for column in range(dp_count):
        held = jnp.where(lane == feats + column, count_all[column, :, 0:1], held)
    params_out[4:5] = held
    count = float(per_micro * rows * dp_count * bin_count)
    params = params_out[...]
    norm_rows(first, (params[0:1], params[1:2]), count, scale_one, offset_one, None, None)
    proj_bias = params[2:3]
    sums[...] = jnp.zeros_like(sums)
    def up(i):
        micro = i // per_micro
        reverse = meta[0, i]
        direction = 1 - 2 * reverse
        begin = reverse * (rows - 1)
        hidden = gelu(hidden_all[i].astype(F32) * scale_one[micro] + offset_one[micro])
        parts = []
        for top, first_row in ((0, -DILATION), (DILATION + rows, rows)):
            where = place.bin * rows + begin + (edge_row + first_row) * direction
            parts.append(jnp.where((where >= 0) & (where < total_bins), hidden[top : top + DILATION], 0.0))
        hidden = jnp.concatenate([parts[0], hidden[DILATION : DILATION + rows], parts[1]], axis=0)
        hidden_all[i] = hidden.astype(BF16)

    half_way = seqs // 2
    stream.loop(half_way, up, PUMPS[4])
    for copy in twos:
        copy.wait()
    threes = []
    for line in range(group):
        for chip in range(place.chip_count):
            part = weights.at[line, pl.ds(pl.multiple_of((chip * 2 + place.core) * share, 8), share)]
            index = line * place.chip_count + chip
            threes.append(
                remote(
                    part,
                    part,
                    three_sent.at[index],
                    three_landed.at[index],
                    (place.dp, place.bin + 1 - 2 * place.core),
                )
            )
            threes[-1].start()
    stream.loop(half_way, lambda i: up(i + half_way), PUMPS[5])
    for copy in threes:
        copy.wait()
    if direct:
        pltpu.make_async_copy(w, weights_out, local.at[2]).start()
    else:
        pltpu.make_async_copy(weights_out, w, local.at[2]).start()
        pltpu.make_async_copy(weights_out, w, local.at[2]).wait()

    def across_taps(i):
        micro = i // per_micro
        hidden = hidden_all[i]
        result = None
        for tap in range(TAPS):
            term = matmul(hidden, w[tap], 1, 0)[tap * DILATION : tap * DILATION + rows]
            result = term if result is None else result + term
        conv[i] = result
        pltpu.make_async_copy(conv.at[i], conv_out.at[i], stores.at[1]).start()
        sums[micro] += eighth(result)
        sums[MICRO + micro] += eighth(result * result)

    stream.loop(seqs, across_taps, PUMPS[9])
    mine = reduce_second[0]
    mine[...] = jnp.sum(sums[...], axis=1)
    reduce = AllReduce(place, *reduce_second)
    reduce.start_near()
    stream.pump(PUMPS[6])
    reduce.finish_near()
    reduce.start_far()
    stream.pump(PUMPS[7])
    stats_two = reduce.finish_far()
    totals_two[...] = stats_two
    norm_rows(
        stats_two, (params[3:4, :feats], params[3:4, feats : 2 * feats]), count, scale_two, offset_two, None, None
    )

    def down(i):
        micro = i // per_micro
        hidden = gelu(conv[i] * scale_two[micro] + offset_two[micro]).astype(BF16)
        branch = matmul(hidden, w[TAPS], 1, 1) + proj_bias
        out[i] = (moved[i].astype(F32) + branch).astype(BF16)
        pltpu.make_async_copy(out.at[i], out_out.at[i], stores.at[2]).start()

    stream.loop(seqs - base, lambda i: down(i + base), 0)
    if relay:
        for slot in range(base, base + relay):
            for piece in range(per_slot):
                over_out[piece, slot - base] = out[meta[2, slot], piece * CHUNK : (piece + 1) * CHUNK]
        relays += to_columns(
            place, over_out, lambda own: relay_out.at[own], relay_own.at[1], relay_out_sent, relay_out_landed
        )
    stream.loop(base, down, PUMPS[8])
    for slot in (*range(base), *range(base + relay, seqs)):
        origin = meta[2, slot]
        for piece in range(per_slot):
            part = out[origin, piece * CHUNK : (piece + 1) * CHUNK]
            if slot < base:
                out_stage[slot * per_slot + piece] = part
            else:
                out_extra[(slot - base - relay) * per_slot + piece] = part
    if direct:
        pltpu.make_async_copy(w, weights_out, local.at[2]).wait()
    pltpu.make_async_copy(moved, moved_out, stores.at[0]).wait()
    pltpu.make_async_copy(conv, conv_out, stores.at[1]).wait()
    pltpu.make_async_copy(out, out_out, stores.at[2]).wait()
    for copy in relays:
        copy.wait()
    stream.finish()


def direct_weights(dims):
    return dims[4] // dims[1] % 16 == 0


def run_front(dims, flags, shifts, x, cot, shard, vectors):
    dp_count, bin_count, seqs, rows, chans, feats, base, relay = dims
    per_slot = rows // CHUNK
    chips = bin_count // 2
    group = TAPS + 1
    dma = pltpu.SemaphoreType.DMA
    big = (seqs, rows, chans)
    packed = jax.ShapeDtypeStruct((base * per_slot, CHUNK, chans), BF16)
    spare = jax.ShapeDtypeStruct(((seqs - base - relay) * per_slot, CHUNK, chans), BF16)
    columns = (dp_count, relay, CHUNK, chans)
    edge = pltpu.VMEM((seqs, EDGE, chans), BF16)
    return pl.pallas_call(
        functools.partial(front_kernel, dims),
        out_shape=(
            jax.ShapeDtypeStruct(big, BF16),
            jax.ShapeDtypeStruct((seqs, rows, feats), F32),
            jax.ShapeDtypeStruct(big, BF16),
            packed,
            spare,
            spare,
            packed,
            jax.ShapeDtypeStruct((group, chans, feats), BF16),
            jax.ShapeDtypeStruct((2 * MICRO, chans), F32),
            jax.ShapeDtypeStruct((8, chans), F32),
            jax.ShapeDtypeStruct((2 * MICRO, feats), F32),
            jax.ShapeDtypeStruct((5, seqs), jnp.int32),
            *([jax.ShapeDtypeStruct(columns, BF16)] * 2 if relay else ()),
        ),
        in_specs=[smem(), smem(), *[anywhere()] * 3, *[vmem()] * 5],
        out_specs=(
            *[anywhere()] * 3,
            *[vmem()] * 3,
            anywhere(),
            anywhere(),
            *[vmem()] * 3,
            smem(),
            *([anywhere()] * 2 if relay else ()),
        ),
        scratch_shapes=[
            pltpu.VMEM(big, BF16),
            edge,
            edge,
            pltpu.VMEM((seqs, rows + 2 * DILATION, chans), BF16),
            pltpu.VMEM(big, BF16),
            pltpu.VMEM((seqs, rows, feats), F32),
            pltpu.VMEM(big, BF16),
            pltpu.VMEM((group, chans, feats), BF16),
            pltpu.VMEM((base * per_slot, CHUNK, chans), BF16),
            pltpu.VMEM((2 * MICRO, 8, chans), F32),
            pltpu.VMEM((2 * MICRO, 8, feats), F32),
            pltpu.VMEM((MICRO, 1, chans), F32),
            pltpu.VMEM((MICRO, 1, chans), F32),
            pltpu.VMEM((MICRO, 1, feats), F32),
            pltpu.VMEM((MICRO, 1, feats), F32),
            *AllReduce.scratch(dp_count, bin_count, 2 * MICRO, chans),
            *AllReduce.scratch(dp_count, bin_count, 2 * MICRO, feats),
            dma((4,)),
            dma((3,)),
            dma((2,)),
            dma((2,)),
            dma((chips,)),
            dma((chips,)),
            dma((TAPS * chips,)),
            dma((TAPS * chips,)),
            dma((group * chips,)),
            dma((group * chips,)),
            dma((base * per_slot,)),
            dma((base * per_slot,)),
            *([pltpu.VMEM(columns, BF16)] * 2 + [dma((2,))] + [dma((dp_count,))] * 4 if relay else ()),
            pltpu.VMEM((1, chans), F32),
            pltpu.VMEM((bin_count, 1, chans), F32),
            pltpu.VMEM((1, 128), F32),
            pltpu.VMEM((dp_count, 1, 128), F32),
            *[dma((bin_count,))] * 2,
            *[dma((dp_count,))] * 2,
            pltpu.VMEM((seqs * per_slot, CHUNK, chans), BF16),
        ],
        compiler_params=pltpu.CompilerParams(
            collective_id=1, has_side_effects=True, vmem_limit_bytes=VMEM_LIMIT
        ),
        name="front",
    )(flags, shifts, x, cot, shard, *vectors)


def starts(counts, dims):
    base, relay = dims[6:8]
    begin, found = jnp.int32(0), []
    for column in range(dims[0]):
        held = jnp.clip(counts[column] - base, 0, relay)
        found.append((begin, held))
        begin = begin + held
    return found


def choose(dims, counts, choice):
    dp_count, seqs, base, relay = dims[0], dims[2], dims[6], dims[7]
    total, most = jnp.int32(0), jnp.int32(0)
    for column in range(dp_count):
        total = total + jnp.clip(counts[column] - base, 0, relay)
        most = jnp.maximum(most, counts[column])
    every = dp_count * relay
    beyond = jnp.maximum(most - base - relay - 1, 0) * 2 + jnp.where(total > every // 2, 1, 0)
    choice[0] = jnp.where(most > base + relay, every + 1 + beyond, total)


def compact_kernel(dims, params, *rest):
    dp_count, feats, relay = dims[0], dims[5], dims[7]
    (cot, out), rest = rest[: 2 * (relay > 0)] or (None, None), rest[2 * (relay > 0) :]
    counts, choice = rest[:2]
    for column in range(dp_count):
        counts[column] = params[4, feats + column].astype(jnp.int32)
    choose(dims, counts, choice)
    if not relay:
        return
    packed, ready = rest[2:]
    for wait in (False, True):
        for column, (begin, held) in enumerate(starts(counts, dims)):
            for slot in range(relay):

                @pl.when(slot < held)
                def _():
                    for side, source in enumerate((cot, out)):
                        copy = pltpu.make_async_copy(
                            source.at[column, slot],
                            packed.at[2 * jnp.minimum(begin + slot, dp_count * relay - 1) + side],
                            ready.at[(side * dp_count + column) * relay + slot],
                        )
                        copy.wait() if wait else copy.start()


def run_compact(dims, params, *relays):
    dp_count, chans, relay = dims[0], dims[4], dims[7]
    pieces = 2 * dp_count * relay
    return pl.pallas_call(
        functools.partial(compact_kernel, dims),
        out_shape=(
            jax.ShapeDtypeStruct((dp_count,), jnp.int32),
            jax.ShapeDtypeStruct((1,), jnp.int32),
            *([jax.ShapeDtypeStruct((pieces, CHUNK, chans), BF16)] if relay else ()),
        ),
        in_specs=[smem(), *[anywhere()] * len(relays)],
        out_specs=(smem(), smem(), *([vmem()] if relay else ())),
        scratch_shapes=[pltpu.SemaphoreType.DMA((pieces,))] if relay else [],
        name="compact",
    )(params, *relays)


class Scatter:
    def __init__(self, place, first, lines, partial, result, halves, dp_send, dp_got, chip_send, chip_got, *semaphores):
        self.place, self.lines = place, pl.ds(first, lines)
        self.partial, self.result, self.halves = partial, result, halves
        self.dp_send, self.dp_got, self.chip_send, self.chip_got = dp_send, dp_got, chip_send, chip_got
        core_sent, core_landed, dp_sent, dp_landed, chip_sent, chip_landed = semaphores
        self.core = remote(
            partial.at[self.lines, :, :, 1 - place.core],
            halves,
            core_sent.at[0],
            core_landed.at[0],
            (place.dp, place.bin + 1 - 2 * place.core),
        )
        self.dp_copies, self.chip_copies = [], []
        for apart in range(1, place.dp_count):
            to = lax.rem(place.dp + apart, place.dp_count)
            self.dp_copies.append(
                remote(
                    dp_send.at[to],
                    dp_got.at[apart - 1],
                    dp_sent.at[apart - 1],
                    dp_landed.at[apart - 1],
                    (to, place.bin),
                )
            )
        for apart in range(1, place.chip_count):
            to = lax.rem(place.chip + apart, place.chip_count)
            self.chip_copies.append(
                remote(
                    chip_send.at[to],
                    chip_got.at[apart - 1],
                    chip_sent.at[apart - 1],
                    chip_landed.at[apart - 1],
                    (place.dp, to * 2 + place.core),
                )
            )

    def start_core(self):
        self.core.start()

    def core_to_dp(self):
        self.core.wait()
        for target in range(self.place.dp_count):
            for chip in range(self.place.chip_count):
                both = self.partial[self.lines, target, chip, self.place.core] + self.halves[:, target, chip]
                self.halves[:, target, chip] = both
                self.dp_send[target, chip] = both.reshape(self.dp_send.shape[2:]).astype(BF16)
        for copy in self.dp_copies:
            copy.start()

    def dp_to_chip(self):
        for copy in self.dp_copies:
            copy.wait()
        for chip in range(self.place.chip_count):
            total = self.halves[:, self.place.dp, chip].reshape(self.dp_send.shape[2:])
            for apart in range(1, self.place.dp_count):
                total += self.dp_got[apart - 1, chip].astype(F32)
            self.halves[:, 0, chip] = total.reshape(self.halves[:, 0, chip].shape)
            self.chip_send[chip] = total.astype(BF16)
        for copy in self.chip_copies:
            copy.start()

    def finish(self):
        for copy in self.chip_copies:
            copy.wait()
        total = self.halves[:, 0, self.place.chip]
        for apart in range(1, self.place.chip_count):
            total += self.chip_got[apart - 1].astype(F32).reshape(total.shape)
        self.result[self.lines] = total

    @staticmethod
    def scratch(dims, lines):
        dp_count, bin_count, seqs, rows, chans, feats, base, relay = dims
        chips, dma = bin_count // 2, pltpu.SemaphoreType.DMA
        quarter = chans // (dp_count * bin_count)
        return [
            pltpu.VMEM((lines, dp_count, chips, quarter, feats), F32),
            pltpu.VMEM((dp_count, chips, lines * quarter, feats), BF16),
            pltpu.VMEM((dp_count, chips, lines * quarter, feats), BF16),
            pltpu.VMEM((chips, lines * quarter, feats), BF16),
            pltpu.VMEM((chips, lines * quarter, feats), BF16),
            dma((1,)),
            dma((1,)),
            dma((dp_count,)),
            dma((dp_count,)),
            dma((chips,)),
            dma((chips,)),
        ]


def scatters(dims):
    dp_count, bin_count, chans = dims[0], dims[1], dims[4]
    return chans % (dp_count * bin_count * 8) == 0


def backward_kernel(
    dims, meta, counts, crossed_in, moved_in, conv_in, w_in, stats_one, params_in, totals_two, cot, cot_near, cot_far, out_stage, *rest
):
    dp_count, bin_count, seqs, rows, chans, feats, base, relay = dims
    own_scatter = scatters(dims)
    (grads, low_edge, high_edge, landed_out, sums_two_out, sums_one_out, result) = rest[:7]
    if relay:
        landed_relay = rest[7]
        (crossed, relayed, home_cot, home_out, relay_own) = rest[-9:-4]
        (relay_cot_sent, relay_cot_landed, relay_out_sent, relay_out_landed) = rest[-4:]
        rest = rest[:7] + rest[8:-9]
    turned, rest = rest[7], rest[:7] + rest[8:]
    (cots, moved, conv, w, chosen) = rest[7:12]
    (scale_one, offset_one, inverse_one, shift_one, scale_two, offset_two, inverse_two, shift_two) = rest[12:20]
    (grad_two, grad_one, hidden_two, hidden_one, windows) = rest[20:25]
    (sums_two, sums_one, bias_sum, line_two, rest_two, line_one, rest_one) = rest[25:32]
    (send_left, send_right, from_left, from_right, last_left, last_right, last_from_left, last_from_right) = rest[32:40]
    reduce_two = rest[40:47]
    reduce_one = rest[47:54]
    (local, halo_sent, halo_landed, last_sent, last_landed, out_sent, out_landed) = rest[54:61]
    partial = result
    place = Place(dp_count, bin_count)
    per_slot = rows // CHUNK
    per_micro = seqs // MICRO
    place.greet()
    loads = [
        pltpu.make_async_copy(conv_in, conv, local.at[0]),
        pltpu.make_async_copy(w_in, w, local.at[1]),
        pltpu.make_async_copy(cot, cots.at[0:seqs], local.at[2]),
        pltpu.make_async_copy(cot_near, cots.at[seqs : seqs + base], local.at[3]),
        pltpu.make_async_copy(cot_far, cots.at[seqs + base + relay : 2 * seqs], local.at[4]),
        pltpu.make_async_copy(moved_in, moved, local.at[5]),
    ]
    if relay:
        load_crossed = pltpu.make_async_copy(crossed_in, crossed, local.at[6])
        load_crossed.start()
    for load in loads:
        load.start()
    if own_scatter:
        partial = rest[61]
        proj_scatter = Scatter(place, TAPS, 1, partial, result, *rest[62:73])
        conv_scatter = Scatter(place, 0, TAPS, partial, result, *rest[73:84])
    place.meet()
    stream = Stream(place, out_stage, landed_out, out_sent, out_landed, base * per_slot)
    stream.pump(BACK_PUMPS[10])
    cot_relays, out_relays = [], []
    if relay:
        load_crossed.wait()
        for column, (begin, held) in enumerate(starts(counts, dims)):
            for slot in range(relay):
                at = 2 * jnp.minimum(begin + slot, dp_count * relay - 1)
                home_cot[column, slot] = crossed[at]
                home_out[column, slot] = crossed[at + 1]
        spot = lambda own: pl.ds(pl.multiple_of(own * CHUNK, CHUNK), CHUNK)
        cot_relays = to_columns(
            place, home_cot, lambda own: relayed.at[:, spot(own)], relay_own.at[0], relay_cot_sent, relay_cot_landed
        )
    count = float(per_micro * rows * dp_count * bin_count)
    params = params_in[...]
    norm_rows(stats_one[...], (params[0:1], params[1:2]), count, scale_one, offset_one, inverse_one, shift_one)
    norm_rows(
        totals_two[...],
        (params[3:4, :feats], params[3:4, feats : 2 * feats]),
        count,
        scale_two,
        offset_two,
        inverse_two,
        shift_two,
    )
    sums_two[...] = jnp.zeros_like(sums_two)
    sums_one[...] = jnp.zeros_like(sums_one)
    bias_sum[...] = jnp.zeros_like(bias_sum)
    for load in loads[:5]:
        load.wait()

    def head(i, late):
        micro = i // per_micro
        inner = pl.ds(pl.multiple_of(lax.rem(i, per_micro) * rows, rows), rows)
        cotangent = cots[meta[3, i]]
        if late and relay:
            place_in = meta[4, i] - base
            other = relayed[jnp.clip(place_in, 0, relay - 1)]
            cotangent = jnp.where((meta[0, i] > 0) & (place_in >= 0) & (place_in < relay), other, cotangent)
        chosen[micro, inner] = cotangent
        bias_sum[...] += eighth(cotangent.astype(F32))
        values = conv[i]
        hidden, slope = gelu_both(values * scale_two[micro] + offset_two[micro])
        hidden_two[micro, inner] = hidden.astype(BF16)
        grad = matmul(cotangent, w[TAPS], 1, 0) * slope
        grad_two[i] = grad
        sums_two[micro] += eighth(grad)
        sums_two[MICRO + micro] += eighth(grad * values)

    stream.loop(base, lambda i: head(i, False), BACK_PUMPS[0])
    loads[5].wait()

    def slopes(i):
        micro = i // per_micro
        inner = pl.ds(pl.multiple_of(lax.rem(i, per_micro) * rows, rows), rows)
        hidden, slope = gelu_both(moved[i].astype(F32) * scale_one[micro] + offset_one[micro])
        hidden_one[micro, inner] = hidden.astype(BF16)
        grad_one[i] = slope

    lax.fori_loop(0, EARLY, lambda i, carry: (slopes(i), carry)[1], 0)
    for copy in cot_relays:
        copy.wait()
    stream.loop(seqs - base, lambda i: head(i + base, True), BACK_PUMPS[9])
    mine = reduce_two[0]
    mine[0 : 2 * MICRO] = jnp.sum(sums_two[...], axis=1)
    bias_row = jnp.sum(bias_sum[...], axis=0, keepdims=True)
    spare = jnp.zeros((1, feats), F32)
    for part in range(2 * MICRO):
        begin = part * feats
        mine[2 * MICRO + part : 2 * MICRO + part + 1] = bias_row[:, begin : begin + feats] if begin < chans else spare
    reduce = AllReduce(place, *reduce_two)
    reduce.start_near()
    stream.pump(BACK_PUMPS[1])

    def weigh(line, terms):
        total = None
        for left, right in terms:
            term = matmul(left, right, 0, 0)
            total = term if total is None else total + term
        partial[line] = total.reshape(partial.shape[1:])

    def proj_terms(micros):
        return [(chosen[micro], hidden_two[micro]) for micro in micros]

    lax.fori_loop(EARLY, seqs, lambda i, carry: (slopes(i), carry)[1], 0)
    reduce.finish_near()
    reduce.start_far()
    stream.pump(BACK_PUMPS[2])
    if relay:
        out_relays = to_columns(
            place, home_out, lambda own: landed_relay.at[:, spot(own)], relay_own.at[1], relay_out_sent, relay_out_landed
        )
    for tap in range(TAPS):
        turned[tap * feats : (tap + 1) * feats] = w[tap].T
    weigh(TAPS, proj_terms(range(MICRO)))
    if own_scatter:
        proj_scatter.start_core()
    back_two = reduce.finish_far()

    def lines(back, scale, inverse, shift, line, remainder, out):
        for micro in range(MICRO):
            plain = back[micro : micro + 1]
            centred = inverse[micro] * back[MICRO + micro : MICRO + micro + 1] + shift[micro] * plain
            out[micro : micro + 1] = plain
            out[MICRO + micro : MICRO + micro + 1] = centred
            line[micro] = -scale[micro] * inverse[micro] * (centred / count)
            remainder[micro] = -scale[micro] * (plain / count + shift[micro] * (centred / count))

    lines(back_two, scale_two, inverse_two, shift_two, line_two, rest_two, sums_two_out)
    sums_two_out[2 * MICRO :] = back_two[2 * MICRO :]

    def conv_gradient(i, begin, size):
        micro = i // per_micro
        span = slice(begin, begin + size)
        value = scale_two[micro] * grad_two[i, span] + line_two[micro] * conv[i, span] + rest_two[micro]
        return value.astype(BF16).astype(F32)

    def edges(i):
        reverse = meta[0, i]
        top, bottom = conv_gradient(i, 0, DILATION), conv_gradient(i, rows - DILATION, DILATION)
        send_left[i] = jnp.where(reverse > 0, bottom, top).astype(BF16)
        send_right[i] = jnp.where(reverse > 0, top, bottom).astype(BF16)

    lax.fori_loop(0, seqs, lambda i, carry: (edges(i), carry)[1], 0)
    halo = Halo(place, send_left, send_right, from_left, from_right, halo_sent, halo_landed)
    halo.start()
    stream.pump(BACK_PUMPS[3])
    if own_scatter:
        proj_scatter.core_to_dp()
    halo.finish()

    def tail(i):
        micro = i // per_micro
        inner = pl.ds(pl.multiple_of(lax.rem(i, per_micro) * rows, rows), rows)
        reverse = meta[0, i]
        left, right = from_left[i].astype(F32), from_right[i].astype(F32)
        low = jnp.where(reverse > 0, right, left)
        high = jnp.where(reverse > 0, left, right)
        full = jnp.concatenate([low, conv_gradient(i, 0, rows), high], axis=0)
        for tap in range(TAPS):
            begin = (TAPS - 1 - tap) * DILATION
            window = full[begin : begin + rows].astype(BF16)
            windows[micro, inner, tap * feats : (tap + 1) * feats] = window
        grad = matmul(windows[micro, inner], turned[...], 1, 0)
        values = moved[i].astype(F32)
        grad = grad * grad_one[i]
        grad_one[i] = grad
        sums_one[micro] += eighth(grad)
        sums_one[MICRO + micro] += eighth(grad * values)

    stream.loop(seqs, tail, BACK_PUMPS[4])
    mine = reduce_one[0]
    mine[...] = jnp.sum(sums_one[...], axis=1)
    reduce = AllReduce(place, *reduce_one)
    reduce.start_near()
    if own_scatter:
        proj_scatter.dp_to_chip()
    stream.pump(BACK_PUMPS[5])

    def conv_weigh(micros, add):
        total = None
        for micro in micros:
            term = matmul(hidden_one[micro], windows[micro], 0, 0)
            total = term if total is None else total + term
        for tap in range(TAPS):
            part = total[:, tap * feats : (tap + 1) * feats].reshape(partial.shape[1:])
            partial[tap] = partial[tap] + part if add else part

    conv_weigh(range(MICRO // 2), False)
    reduce.finish_near()
    reduce.start_far()
    stream.pump(BACK_PUMPS[6])
    conv_weigh(range(MICRO // 2, MICRO), True)
    if own_scatter:
        conv_scatter.start_core()
    back_one = reduce.finish_far()
    lines(back_one, scale_one, inverse_one, shift_one, line_one, rest_one, sums_one_out)
    if own_scatter:
        conv_scatter.core_to_dp()
        proj_scatter.finish()

    def end(i):
        micro = i // per_micro
        inner = pl.ds(pl.multiple_of(lax.rem(i, per_micro) * rows, rows), rows)
        reverse = meta[0, i]
        value = scale_one[micro] * grad_one[i] + line_one[micro] * moved[i].astype(F32) + rest_one[micro]
        value = chosen[micro, inner].astype(F32) + value
        grads[i] = value.astype(BF16)
        top, bottom = value[:LAST_EDGE].astype(BF16), value[rows - LAST_EDGE :].astype(BF16)
        last_left[i] = jnp.where(reverse > 0, bottom, top)
        last_right[i] = jnp.where(reverse > 0, top, bottom)

    stream.loop(seqs, end, BACK_PUMPS[7])
    last = Halo(place, last_left, last_right, last_from_left, last_from_right, last_sent, last_landed)
    last.start()
    stream.pump(BACK_PUMPS[8])
    if own_scatter:
        conv_scatter.dp_to_chip()
    last.finish()
    low_edge[...] = last_from_left[...]
    high_edge[...] = last_from_right[...]
    if own_scatter:
        conv_scatter.finish()
    for copy in out_relays:
        copy.wait()
    stream.finish()


def run_backward(dims, meta, counts, crossed, moved, conv, w, stats_one, params, totals_two, cot, cot_near, cot_far, out_stage):
    dp_count, bin_count, seqs, rows, chans, feats, base, relay = dims
    chips = bin_count // 2
    group = TAPS + 1
    quarter = chans // (dp_count * bin_count)
    own_scatter = scatters(dims)
    per_slot = rows // CHUNK
    held = seqs // MICRO * rows
    dma = pltpu.SemaphoreType.DMA
    wide = pltpu.VMEM((MICRO, 1, chans), F32)
    narrow = pltpu.VMEM((MICRO, 1, feats), F32)
    edge = jax.ShapeDtypeStruct((seqs, LAST_EDGE, chans), BF16)
    return pl.pallas_call(
        functools.partial(backward_kernel, dims),
        out_shape=(
            jax.ShapeDtypeStruct((seqs, rows, chans), BF16),
            edge,
            edge,
            jax.ShapeDtypeStruct((base * per_slot, CHUNK, chans), BF16),
            jax.ShapeDtypeStruct((4 * MICRO, feats), F32),
            jax.ShapeDtypeStruct((2 * MICRO, chans), F32),
            jax.ShapeDtypeStruct((group, quarter if own_scatter else chans, feats), F32),
            *([jax.ShapeDtypeStruct((relay, rows, chans), BF16)] if relay else ()),
        ),
        in_specs=[smem(), smem(), *[anywhere()] * 4, *[vmem()] * 3, *[anywhere()] * 4],
        out_specs=(vmem(), vmem(), vmem(), anywhere(), vmem(), vmem(), vmem(), *([anywhere()] if relay else ())),
        scratch_shapes=[
            pltpu.VMEM((TAPS * feats, chans), BF16),
            pltpu.VMEM((2 * seqs, rows, chans), BF16),
            pltpu.VMEM((seqs, rows, chans), BF16),
            pltpu.VMEM((seqs, rows, feats), F32),
            pltpu.VMEM((group, chans, feats), BF16),
            pltpu.VMEM((MICRO, held, chans), BF16),
            *[wide] * 4,
            *[narrow] * 4,
            pltpu.VMEM((seqs, rows, feats), F32),
            pltpu.VMEM((seqs, rows, chans), F32),
            pltpu.VMEM((MICRO, held, feats), BF16),
            pltpu.VMEM((MICRO, held, chans), BF16),
            pltpu.VMEM((MICRO, held, TAPS * feats), BF16),
            pltpu.VMEM((2 * MICRO, 8, feats), F32),
            pltpu.VMEM((2 * MICRO, 8, chans), F32),
            pltpu.VMEM((8, chans), F32),
            narrow,
            narrow,
            wide,
            wide,
            *[pltpu.VMEM((seqs, DILATION, feats), BF16)] * 4,
            *[pltpu.VMEM((seqs, LAST_EDGE, chans), BF16)] * 4,
            *AllReduce.scratch(dp_count, bin_count, 4 * MICRO, feats),
            *AllReduce.scratch(dp_count, bin_count, 2 * MICRO, chans),
            dma((7,)),
            dma((2,)),
            dma((2,)),
            dma((2,)),
            dma((2,)),
            dma((base * per_slot,)),
            dma((base * per_slot,)),
            *(
                (
                    pltpu.VMEM((group, dp_count, chips, 2, quarter, feats), F32),
                    *Scatter.scratch(dims, 1),
                    *Scatter.scratch(dims, TAPS),
                )
                if own_scatter
                else ()
            ),
            *(
                [pltpu.VMEM((2 * dp_count * relay, CHUNK, chans), BF16), pltpu.VMEM((relay, rows, chans), BF16)]
                + [pltpu.VMEM((dp_count, relay, CHUNK, chans), BF16)] * 2
                + [dma((2,))]
                + [dma((dp_count,))] * 4
                if relay
                else ()
            ),
        ],
        compiler_params=pltpu.CompilerParams(
            collective_id=2, has_side_effects=True, vmem_limit_bytes=VMEM_LIMIT
        ),
        name="backward",
    )(meta, counts, crossed, moved, conv, w, stats_one, params, totals_two, cot, cot_near, cot_far, out_stage)


def last_kernel(dims, meta, back_one, back_two, *rest):
    dp_count, bin_count, seqs, rows, chans, feats, base, relay = dims
    own_scatter = scatters(dims)
    partial, rest = (rest[0], rest[1:]) if own_scatter else (None, rest)
    (grad, left, right, out, near), rest = rest[:5], rest[5:]
    relayed, rest = (rest[0], rest[1:]) if relay else (None, rest)
    (far, result_out, result_grad, gain_one, bias_one, gain_two, bias_two, bias_proj) = rest[:8]
    if own_scatter:
        conv_weight, proj_weight = rest[8:10]
        conv_weight[...] = partial[:TAPS]
        proj_weight[...] = partial[TAPS]
    (held, made, got, put) = rest[-4:]
    for i in range(seqs):
        reverse, slot = meta[0, i], meta[4, i]

        @pl.when(reverse == 0)
        def _():
            pltpu.make_async_copy(out.at[i], held.at[i], got.at[i]).start()

        @pl.when((reverse > 0) & (slot < base))
        def _():
            pltpu.make_async_copy(near.at[jnp.minimum(slot, base - 1)], held.at[i], got.at[i]).start()

        if relay:

            @pl.when((reverse > 0) & (slot >= base) & (slot < base + relay))
            def _():
                pltpu.make_async_copy(relayed.at[jnp.clip(slot - base, 0, relay - 1)], held.at[i], got.at[i]).start()

        @pl.when((reverse > 0) & (slot >= base + relay))
        def _():
            pltpu.make_async_copy(far.at[jnp.maximum(slot - base - relay, 0)], held.at[i], got.at[i]).start()

    across = rows + 2 * LAST_EDGE
    row = lax.broadcasted_iota(jnp.int32, (rows, across), 0)
    column = lax.broadcasted_iota(jnp.int32, (rows, across), 1)

    def step(i, carry):
        reverse, shift = meta[0, i], meta[1, i]
        low = jnp.where(reverse > 0, right[i], left[i])
        high = jnp.where(reverse > 0, left[i], right[i])
        source = jnp.concatenate([low, grad[i], high], axis=0)
        place = jnp.where(reverse > 0, rows - 1 - row - shift, row + shift) + LAST_EDGE
        pick = jnp.where(column == place, 1.0, 0.0).astype(BF16)
        made[i] = matmul(pick, source, 1, 0).astype(BF16)
        pltpu.make_async_copy(made.at[i], result_grad.at[i], put.at[0]).start()
        pltpu.make_async_copy(held.at[i], held.at[i], got.at[i]).wait()
        pltpu.make_async_copy(held.at[i], result_out.at[i], put.at[1]).start()
        return carry

    lax.fori_loop(0, seqs, step, 0)
    dp, bins = lax.axis_index("dp"), lax.axis_index("bins")

    def own(values, index, result):
        width, share = values.shape[1], result.shape[1]
        begin = index * share
        result[...] = pltpu.roll(values, lax.rem(width - begin, width), 1)[:, :share]

    def summed(back, begin):
        return jnp.sum(back[begin : begin + MICRO], axis=0, keepdims=True)

    wide, narrow = dp * bin_count + bins, bins
    own(summed(back_one, MICRO), wide, gain_one)
    own(summed(back_one, 0), wide, bias_one)
    own(summed(back_two, MICRO), narrow, gain_two)
    own(summed(back_two, 0), narrow, bias_two)
    bias = jnp.concatenate([back_two[2 * MICRO + k : 2 * MICRO + k + 1] for k in range(chans // feats)], axis=1)
    own(bias, wide, bias_proj)
    pltpu.make_async_copy(made, result_grad, put.at[0]).wait()
    pltpu.make_async_copy(held, result_out, put.at[1]).wait()


def run_last(dims, meta, back_one, back_two, partial, grad, left, right, out, near, relayed, far):
    dp_count, bin_count, seqs, rows, chans, feats, base, relay = dims
    own_scatter = scatters(dims)
    big = jax.ShapeDtypeStruct((seqs, rows, chans), BF16)
    quarter = chans // (dp_count * bin_count)
    wide = jax.ShapeDtypeStruct((1, quarter), F32)
    narrow = jax.ShapeDtypeStruct((1, feats // bin_count), F32)
    weights = (
        jax.ShapeDtypeStruct((TAPS, quarter, feats), F32),
        jax.ShapeDtypeStruct((quarter, feats), F32),
    )
    partials = [partial] if own_scatter else []
    return pl.pallas_call(
        functools.partial(last_kernel, dims),
        out_shape=(big, big, wide, wide, narrow, narrow, wide, *(weights if own_scatter else ())),
        in_specs=[
            smem(),
            *[vmem()] * (5 + len(partials)),
            *[anywhere()] * (3 + len(relayed)),
        ],
        out_specs=(anywhere(), anywhere(), *[vmem()] * (7 if own_scatter else 5)),
        scratch_shapes=[
            pltpu.VMEM(big.shape, BF16),
            pltpu.VMEM(big.shape, BF16),
            pltpu.SemaphoreType.DMA((seqs,)),
            pltpu.SemaphoreType.DMA((2,)),
        ],
        compiler_params=pltpu.CompilerParams(vmem_limit_bytes=VMEM_LIMIT),
        name="last",
    )(meta, back_one, back_two, *partials, grad, left, right, out, near, *relayed, far)


def local(
    activations,
    shift_bins,
    reverse_flags,
    gain_one,
    bias_one,
    conv_weight,
    gain_two,
    bias_two,
    proj_weight,
    proj_bias,
    cotangent,
):
    seqs, rows, chans = activations.shape
    feats = conv_weight.shape[2]
    dp_count, bin_count = lax.axis_size("dp"), lax.axis_size("bins")
    per_slot = rows // CHUNK
    base = BASE_SLOTS
    relay = RELAY_SLOTS if per_slot == dp_count else 0
    dims = (dp_count, bin_count, seqs, rows, chans, feats, base, relay)

    vectors = [vector[None] for vector in (gain_one, bias_one, proj_bias, gain_two, bias_two)]
    shard = jnp.concatenate([conv_weight, proj_weight.T[None]], axis=0)

    (
        moved,
        conv,
        out,
        out_stage,
        out_extra,
        cot_extra,
        cot_near,
        w,
        stats_one,
        params,
        totals_two,
        meta,
        *relays,
    ) = run_front(
        dims,
        reverse_flags,
        shift_bins,
        activations,
        cotangent.reshape(seqs * per_slot, CHUNK, chans),
        shard,
        vectors,
    )
    counts, choice, *packed = run_compact(dims, params, *relays)
    pairs = [(source, bin_count - 1 - source) for source in range(bin_count)]
    direct = seqs - base - relay
    pieces = 2 * dp_count * relay

    def crossing(relayed, slots, packed, pair):
        moving = [packed[: 2 * relayed]] * (relayed > 0)
        moving += [item[: slots * per_slot] for item in pair] * (slots > 0)
        if not moving:
            return packed, *pair
        got = lax.ppermute(jnp.concatenate(moving), "bins", pairs)
        put = lax.dynamic_update_slice_in_dim
        if relayed:
            packed = put(packed, got[: 2 * relayed], 0, 0)
        if slots:
            held = slots * per_slot
            rest = got[2 * relayed :]
            pair = tuple(put(item, rest[k * held : (k + 1) * held], 0, 0) for k, item in enumerate(pair))
        return packed, *pair

    every = pieces // 2
    branches = [functools.partial(crossing, held, 0) for held in range(every + 1)]
    for slots in range(1, direct + 1):
        branches += [functools.partial(crossing, held, slots) for held in (every // 2, every)]
    packed = packed[0] if relay else jnp.zeros((1, CHUNK, chans), BF16)
    crossed, cot_far, out_far = lax.switch(choice[0], branches, packed, (cot_extra, out_extra))

    slots_of = lambda item: item.reshape(-1, rows, chans)
    grads, low_edge, high_edge, out_near, back_two, back_one, partial, *landed = run_backward(
        dims,
        meta,
        counts,
        crossed,
        moved,
        conv,
        w,
        stats_one,
        params,
        totals_two,
        cotangent,
        slots_of(cot_near),
        slots_of(cot_far),
        out_stage,
    )
    output, grad_activations, gain_one, bias_one, gain_two, bias_two, bias_proj, *weights = run_last(
        dims,
        meta,
        back_one,
        back_two,
        partial,
        grads,
        low_edge,
        high_edge,
        out,
        slots_of(out_near),
        landed,
        slots_of(out_far),
    )
    if not weights:
        scattered = lax.psum_scatter(partial, ("dp", "bins"), scatter_dimension=1, tiled=True)
        weights = scattered[:TAPS], scattered[TAPS]
    return (
        output,
        grad_activations,
        gain_one[0],
        bias_one[0],
        weights[0],
        gain_two[0],
        bias_two[0],
        weights[1].T,
        bias_proj[0],
    )


def solution(mesh):
    placed = (
        P("dp", "bins", None),
        P("dp"),
        P("dp"),
        P("bins"),
        P("bins"),
        P(None, "bins", None),
        P("bins"),
        P("bins"),
        P(None, "bins"),
        P("bins"),
        P("dp", "bins", None),
    )
    return jax.shard_map(
        local,
        mesh=mesh,
        in_specs=placed,
        out_specs=(
            P("dp", "bins", None),
            P("dp", "bins", None),
            P(("dp", "bins")),
            P(("dp", "bins")),
            P(None, ("dp", "bins"), None),
            P("bins"),
            P("bins"),
            P(None, ("dp", "bins")),
            P(("dp", "bins")),
        ),
        check_vma=False,
    )
```
